256 devices in a mesh: fsdp: 256 (over z, y, x, core).
Axes of the slice: x: 4, y: 4, z: 8, core: 2. Of those that a mesh axis runs over, the one named last changes fastest.
Arguments:
- x: bfloat16 [512, 512, 512], P('fsdp')
- lengths: int32 [512], P('fsdp')
- d_y: bfloat16 [512, 512, 512], P('fsdp')
- w_attn: bfloat16 [2, 4, 512, 512], P(None, None, 'fsdp')
- b_attn: bfloat16 [2, 4, 512], P(None, None, 'fsdp')
- ln_par: bfloat16 [2, 4, 512], P(None, None, 'fsdp')
- w_up: bfloat16 [2, 512, 2048], P(None, 'fsdp')
- b_up: bfloat16 [2, 2048], P(None, 'fsdp')
- w_down: bfloat16 [2, 2048, 512], P(None, 'fsdp')
- b_down: bfloat16 [2, 512], P(None, 'fsdp')
Outputs:
- output 1: bfloat16 [512, 512, 512], P('fsdp')
- output 2: float32 [2, 4, 512, 512], P(None, None, 'fsdp')
- output 3: float32 [2, 4, 512], P(None, None, 'fsdp')
- output 4: float32 [2, 4, 512], P(None, None, 'fsdp')
- output 5: float32 [2, 512, 2048], P(None, 'fsdp')
- output 6: float32 [2, 2048], P(None, 'fsdp')
- output 7: float32 [2, 2048, 512], P(None, 'fsdp')
- output 8: float32 [2, 512], P(None, 'fsdp')
All inputs are finite; a program needn't handle non-finite values.
Results may differ from the reference program's by a relative error of at most 0.0133472.
Values are sent between devices in bfloat16 or wider.
A program may use at most 768 MiB of HBM per device.

```python
import jax
import jax.numpy as jnp
from jax import lax

MODEL_DIM = 512
FFN_DIM = 2048
HEAD_DIM = 64
NUM_LAYERS = 2
SEQ_LEN = 512
SEQ_DEV = 2
GROUP_SIZE = 256
EPS = 1e-5
THETA = 10000.0
NUM_HEADS = MODEL_DIM // HEAD_DIM
BATCH = SEQ_DEV * GROUP_SIZE
MIN_LEN = SEQ_LEN // 8


def setup_inputs(seed: int = 0) -> dict:
    key_list = jax.random.split(jax.random.key(seed), 10)
    seq_index = jnp.arange(BATCH)
    drawn_len = jax.random.randint(key_list[1], (BATCH,), MIN_LEN, SEQ_LEN + 1)
    lengths = jnp.where(seq_index == 0, SEQ_LEN, jnp.where(seq_index == 1, MIN_LEN, drawn_len)).astype(jnp.int32)
    act_shape = (BATCH, SEQ_LEN, MODEL_DIM)
    dy_scale = float(BATCH * SEQ_LEN) ** -0.25
    ln_base = jnp.array([1.0, 0.0, 1.0, 0.0], dtype=jnp.float32)[None, :, None]
    return {
        'x': jax.random.normal(key_list[0], act_shape, jnp.float32).astype(jnp.bfloat16),
        'lengths': lengths,
        'd_y': (dy_scale * jax.random.normal(key_list[2], act_shape, jnp.float32)).astype(jnp.bfloat16),
        'w_attn': (MODEL_DIM ** -0.5 * jax.random.normal(key_list[3], (NUM_LAYERS, 4, MODEL_DIM, MODEL_DIM), jnp.float32)).astype(jnp.bfloat16),
        'b_attn': (0.3 * jax.random.normal(key_list[4], (NUM_LAYERS, 4, MODEL_DIM), jnp.float32)).astype(jnp.bfloat16),
        'ln_par': (ln_base + 0.2 * jax.random.normal(key_list[5], (NUM_LAYERS, 4, MODEL_DIM), jnp.float32)).astype(jnp.bfloat16),
        'w_up': (MODEL_DIM ** -0.5 * jax.random.normal(key_list[6], (NUM_LAYERS, MODEL_DIM, FFN_DIM), jnp.float32)).astype(jnp.bfloat16),
        'b_up': (0.5 * jax.random.normal(key_list[7], (NUM_LAYERS, FFN_DIM), jnp.float32)).astype(jnp.bfloat16),
        'w_down': (FFN_DIM ** -0.5 * jax.random.normal(key_list[8], (NUM_LAYERS, FFN_DIM, MODEL_DIM), jnp.float32)).astype(jnp.bfloat16),
        'b_down': (0.3 * jax.random.normal(key_list[9], (NUM_LAYERS, MODEL_DIM), jnp.float32)).astype(jnp.bfloat16),
    }


def to_bf16(tensor):
    return tensor.astype(jnp.bfloat16).astype(jnp.float32)


def norm_fwd(x_in, gain, shift):
    row_mean = jnp.mean(x_in, axis=-1, keepdims=True)
    centered = x_in - row_mean
    variance = jnp.mean(centered * centered, axis=-1, keepdims=True)
    return centered * lax.rsqrt(variance + EPS) * gain + shift


def rotary_tables():
    half_dim = HEAD_DIM // 2
    inv_freq = 1.0 / (THETA ** (jnp.arange(half_dim, dtype=jnp.float32) * (2.0 / HEAD_DIM)))
    angles = jnp.arange(SEQ_LEN, dtype=jnp.float32)[:, None] * inv_freq[None, :]
    return jnp.cos(angles)[:, None, :], jnp.sin(angles)[:, None, :]


def rotate(tensor, cos_tab, sin_tab):
    half_dim = HEAD_DIM // 2
    first_half = tensor[..., :half_dim]
    second_half = tensor[..., half_dim:]
    return jnp.concatenate([first_half * cos_tab - second_half * sin_tab, second_half * cos_tab + first_half * sin_tab], axis=-1)


def layer_fwd(x, weights, lengths, tables):
    w_attn, b_attn, ln_par, w_up, b_up, w_down, b_down = weights
    cos_tab, sin_tab = tables
    num_seq = x.shape[0]
    h_one = to_bf16(norm_fwd(x, ln_par[0], ln_par[1]))
    projected = jnp.einsum('bld,kde->kble', h_one, w_attn[:3]) + b_attn[:3, None, None, :]
    projected = projected.reshape(3, num_seq, SEQ_LEN, NUM_HEADS, HEAD_DIM)
    query_rot = to_bf16(rotate(projected[0] * (HEAD_DIM ** -0.5), cos_tab, sin_tab))
    key_rot = to_bf16(rotate(projected[1], cos_tab, sin_tab))
    values = to_bf16(projected[2])
    scores = jnp.einsum('bqhd,bkhd->bhqk', query_rot, key_rot)
    key_valid = jnp.arange(SEQ_LEN)[None, None, None, :] < lengths[:, None, None, None]
    attn_probs = to_bf16(jax.nn.softmax(jnp.where(key_valid, scores, -1e30), axis=-1))
    context = to_bf16(jnp.einsum('bhqk,bkhd->bqhd', attn_probs, values)).reshape(num_seq, SEQ_LEN, MODEL_DIM)
    x_mid = to_bf16(x + jnp.einsum('bld,de->ble', context, w_attn[3]) + b_attn[3])
    h_two = to_bf16(norm_fwd(x_mid, ln_par[2], ln_par[3]))
    act_out = to_bf16(jax.nn.gelu(jnp.einsum('bld,df->blf', h_two, w_up) + b_up, approximate=False))
    return to_bf16(x_mid + jnp.einsum('blf,fd->bld', act_out, w_down) + b_down)


def reference(x, lengths, d_y, w_attn, b_attn, ln_par, w_up, b_up, w_down, b_down):
    params = tuple(tensor.astype(jnp.float32) for tensor in (w_attn, b_attn, ln_par, w_up, b_up, w_down, b_down))
    tables = rotary_tables()

    def stack_fwd(x_block, param_set, len_block):
        hidden = x_block
        for layer_idx in range(NUM_LAYERS):
            hidden = layer_fwd(hidden, tuple(tensor[layer_idx] for tensor in param_set), len_block, tables)
        return hidden

    def block_step(grad_acc, block_in):
        x_block, len_block, dy_block = block_in

        def block_fwd(x_local, param_local):
            return stack_fwd(x_local, param_local, len_block)

        _, pull_back = jax.vjp(block_fwd, x_block.astype(jnp.float32), params)
        d_x_block, d_params = pull_back(dy_block.astype(jnp.float32))
        return jax.tree.map(jnp.add, grad_acc, d_params), d_x_block.astype(jnp.bfloat16)

    grad_zero = jax.tree.map(jnp.zeros_like, params)
    blocks_in = (x.reshape(GROUP_SIZE, SEQ_DEV, SEQ_LEN, MODEL_DIM), lengths.reshape(GROUP_SIZE, SEQ_DEV), d_y.reshape(GROUP_SIZE, SEQ_DEV, SEQ_LEN, MODEL_DIM))
    grad_sum, d_x = lax.scan(block_step, grad_zero, blocks_in)
    return (d_x.reshape(BATCH, SEQ_LEN, MODEL_DIM), grad_sum[0], grad_sum[1], grad_sum[2], grad_sum[3], grad_sum[4], grad_sum[5], grad_sum[6])
```

```python
import functools
import math
import jax
import jax.numpy as jnp
import numpy as np
from jax import lax
from jax.experimental import pallas as pl
from jax.experimental.pallas import tpu as pltpu
from jax.sharding import Mesh, PartitionSpec as P

F32, BF = jnp.float32, jnp.bfloat16
AXES = ('z', 'y', 'x', 'c')
SIZES = dict(z=8, y=4, x=4, c=2, k=2, h=2, l=2, r=2)
TILE = (8, 128)
TILED = dict(attn='kzyht', up='zyht', down='zyxct')
FINE = dict(attn='kzyhtlcr', up='zyhtlcr', down='zyxct')
LANE_TILES = dict(attn=4, up=8, down=2)
HALVED = dict(attn='k', up='t', down='t')
ALL = slice(None)


class Place:
    def __init__(self, send, recv):
        self.me = {a: lax.axis_index(a) for a in AXES}
        self.send, self.recv, self.used = send, recv, 0

    def shifted(self, axis, s):
        at = dict(self.me)
        if axis:
            at[axis] = lax.rem(at[axis] + s, SIZES[axis])
        return at

    def peers(self, axis):
        n = SIZES[axis]
        return sorted(range(1, n), key=lambda s: min(s, n - s))

    def greet(self, axes):
        bar = pltpu.get_barrier_semaphore()
        everyone = [(a, s) for a in axes for s in self.peers(a)]
        for a, s in everyone:
            pl.semaphore_signal(bar, inc=1, device_id=self.device(a, s), device_id_type=pl.DeviceIdType.MESH)
        pl.semaphore_wait(bar, len(everyone))

    def device(self, axis, s):
        at = self.shifted(axis, s)
        return tuple(at[a] for a in AXES)

    def copy(self, axis, s, refs):
        i, self.used = self.used, self.used + 1

        def build():
            src, dst = refs()
            return pltpu.make_async_remote_copy(src, dst, self.send.at[i], self.recv.at[i], device_id=self.device(axis, s), device_id_type=pl.DeviceIdType.MESH)
        build().start()
        return lambda: build().wait()

    def local(self, refs):
        i, self.used = self.used, self.used + 1

        def build():
            return pltpu.make_async_copy(*refs(), self.send.at[i])
        build().start()
        return lambda: build().wait()


def spot(at):
    return dict(at, h=lax.div(at['x'], SIZES['l']), l=lax.rem(at['x'], SIZES['l']))


def half(kind, core):
    n = SIZES['k'] if HALVED[kind] == 'k' else LANE_TILES[kind]
    return {HALVED[kind]: pl.ds(core * n, n)}


def view(ref, names, pick):
    return ref.at[tuple(pick.get(n, ALL) for n in names)]


def only(at, names):
    return {n: v for n, v in spot(at).items() if n in names}


OWNER = dict(x='xhl', y='y', z='z')


def gather_unit(place, kind, full, shard, order):
    names = FINE[kind]
    mine = [n for n in names if n not in 'tkr']

    def block(core, fixed, at):
        return view(full, names, dict(half(kind, core(at)), **only(at, fixed)))
    own, other = (lambda at: at['c']), (lambda at: 1 - at['c'])
    rows = [n for n in names if n in 'tk'] + ['r'] * 2

    def piece(core):
        return view(shard, rows, half(kind, core(place.me)))
    waits = [place.local(lambda: (piece(own), block(own, mine, place.me))),
             place.copy('c', 1, lambda: (piece(other), block(other, mine, place.me)))]
    yield
    for w in waits:
        w()
    left = list(order)
    while left:
        fixed = ''.join(OWNER[a] for a in left)
        axis = left.pop(0)
        same = lambda fixed=fixed: (block(own, fixed, place.me),) * 2
        waits = [(s, place.copy(axis, s, same)) for s in place.peers(axis)]
        if left:
            yield
            for _, w in waits:
                w()
    last = [place.copy('c', 1, same)]
    for s, w in waits:
        yield
        w()
        came = lambda s=s: (block(own, fixed, place.shifted(axis, SIZES[axis] - s)),) * 2
        last.append(place.copy('c', 1, came))
    yield
    for w in last:
        w()


def unravel(i, shape):
    idx = []
    for n in reversed(shape):
        idx.append(lax.rem(i, n))
        i = lax.div(i, n)
    return tuple(reversed(idx))


def each(shape, body):
    def step(i, carry):
        body(unravel(i, shape))
        return carry
    lax.fori_loop(0, math.prod(shape), step, 0)


def sizes(kind, names):
    return tuple(LANE_TILES[kind] if n == 't' else SIZES[n] for n in names) + TILE


def phases(kind, order):
    names = TILED[kind]
    for a in order:
        d = a if a in names else 'h'
        yield a, d, names, names.replace(d, '')
        names = names.replace(d, '')


def scatter_buffers(kind, order):
    shapes = [sizes(kind, TILED[kind])] * 2
    for a, _, _, after in phases(kind, order):
        shapes += [(SIZES[a] - 1,) + sizes(kind, after), sizes(kind, after)]
    shapes.append(sizes(kind, after.replace('c', '')))
    return [pltpu.VMEM(s, F32) for s in shapes]


def scatter_unit(place, kind, order, grad, out, bufs):
    me = place.me
    own, got, *bufs = bufs
    names = TILED[kind]
    waits = [place.copy('c', 1, lambda: (view(grad, names, half(kind, 1 - me['c'])), got)),
             place.local(lambda: (view(grad, names, half(kind, me['c'])), own))]
    yield
    for w in waits:
        w()

    def add(idx):
        own[idx] = own[idx] + got[idx]
    each(own.shape[:-4], add)
    src = own
    for a, d, before, after in phases(kind, order):
        slots, total, *bufs = bufs
        at = before.index(d)
        waits = [place.copy(a, s, lambda s=s, src=src: (view(src, before, only(place.shifted(a, s), d)), slots.at[s - 1])) for s in place.peers(a)]
        yield
        for w in waits:
            w()
        lead = total.shape[:-4]

        def reduce(idx):
            loop = dict(zip(after, idx))
            v = src[tuple(spot(me)[n] if n == d else loop.get(n, ALL) for n in before)]
            for s in range(SIZES[a] - 1):
                v = v + slots[(s,) + idx]
            total[idx if idx else ...] = v
        each(lead, reduce) if lead else reduce(())
        src = total
    other, = bufs
    mine = lambda core: view(src, after, dict(c=core)) if 'c' in after else src
    wait = place.copy('c', 1, lambda: (mine(1 - me['c']), other))
    yield
    wait()
    for core, ref in ((me['c'], mine(me['c'])), (1 - me['c'], other)):
        rows = ALL if kind == 'down' else pl.ds((spot(me)['l'] * 2 + me['c']) * 2, 2)
        out[half(kind, core)[HALVED[kind]]] = ref[..., rows, :]


def total_unit(place, value, out, slots):
    me = place.me
    keep, *slots = slots
    wait = place.copy('c', 1, lambda: (value.at[1 - me['c']], slots[0].at[0]))
    yield
    wait()
    keep[...] = value[me['c']] + slots[0][0]
    for axis, slot in zip('xyz', slots[1:]):
        slot[SIZES[axis] - 1] = keep[...]
        waits = [place.copy(axis, s, lambda s=s: (slot.at[SIZES[axis] - 1], slot.at[s - 1])) for s in place.peers(axis)]
        yield
        for w in waits:
            w()
        v = slot[0]
        for s in range(1, SIZES[axis]):
            v = v + slot[s]
        keep[...] = v
    out[me['c']] = keep[...]
    wait = place.copy('c', 1, lambda: (keep, out.at[me['c']]))
    yield
    wait()


def total_buffers(n):
    return [pltpu.VMEM((n, 512), F32)] + [pltpu.VMEM((SIZES[a], n, 512), F32) for a in 'cxyz']


def run(units):
    units = list(units)
    while units:
        units = [u for u in units if next(u, units) is not units]


def semaphores(n):
    return [pltpu.SemaphoreType.DMA((n,))] * 2


def any_space(n):
    return [pl.BlockSpec(memory_space=pl.ANY)] * n


def in_vmem(n):
    return [pl.BlockSpec(memory_space=pltpu.VMEM)] * n


SD = jax.ShapeDtypeStruct
GATHER_ORDER = dict(attn='xzy', up='xzy', down='yzx')
SCATTER_ORDER = dict(attn='yzx', up='yzx', down='xzy')
KINDS = tuple(TILED)


def gather_kernel(*refs):
    n = 2 * len(KINDS)
    shards, small, full, total, slots, sems = refs[:n], refs[n], refs[n + 1:2 * n + 1], refs[2 * n + 1], refs[2 * n + 2:-2], refs[-2:]
    place = Place(*sems)
    place.greet(AXES)
    run([total_unit(place, small, total, slots)] + [gather_unit(place, kind, f, s, GATHER_ORDER[kind]) for kind, f, s in zip(KINDS * 2, full, shards)])


def fine_shape(kind):
    n = 2 * LANE_TILES[kind] if HALVED[kind] == 't' else LANE_TILES[kind]
    dims = dict(SIZES, t=n, k=4)
    tail = (128,) if 'r' in FINE[kind] else TILE
    return tuple(dims[d] for d in FINE[kind]) + tail


def gather(attn, up, down, small):
    shards = []
    for l in range(2):
        shards += [attn[l].reshape(4, 2, 4, 128).swapaxes(1, 2), up[l].reshape(2, 16, 128).swapaxes(0, 1), down[l].reshape(8, 4, 128).swapaxes(0, 1)]
    *full, total = pl.pallas_call(
        gather_kernel, name='gather',
        in_specs=in_vmem(len(shards) + 1), out_specs=any_space(len(shards)) + in_vmem(1),
        out_shape=[SD(fine_shape(k), BF) for k in KINDS * 2] + [SD(small.shape, F32)],
        scratch_shapes=total_buffers(16) + semaphores(180),
        compiler_params=pltpu.CompilerParams(collective_id=1, has_side_effects=True),
    )(*shards, small)
    whole = []
    for l in range(2):
        a, u, d = full[3 * l:3 * l + 3]
        whole.append((tiles_to_rows(a.reshape(4, 64, 4, *TILE)), tiles_to_rows(u.reshape(64, 16, *TILE)), tiles_to_rows(d.reshape(256, 4, *TILE))))
    return whole, total


def tiles_to_rows(t):
    *lead, r, n, s, w = t.shape
    return t.swapaxes(-3, -2).reshape(*lead, r * s, n * w)


def rows_to_tiles(g):
    *lead, r, w = g.shape
    return g.reshape(*lead, r // TILE[0], TILE[0], w // TILE[1], TILE[1]).swapaxes(-3, -2)


def tiled_shape(kind):
    return fine_shape(kind)[:-3 if kind != 'down' else -2][:len(TILED[kind])] + TILE


def scatter_kernel(*refs):
    n = 2 * len(KINDS)
    grads, small, outs, total = refs[:n], refs[n:n + 4], refs[n + 4:2 * n + 4], refs[2 * n + 4]
    scratch = list(refs[2 * n + 5:-2])
    value, *scratch = scratch
    for i in range(4):
        value[i // 2, pl.ds(8 * (i % 2), 8)] = small[i][...]
    place = Place(*refs[-2:])
    place.greet(AXES)
    count = len(total_buffers(16))
    units = [total_unit(place, value, total, scratch[:count])]
    scratch = scratch[count:]
    for kind, g, o in zip(KINDS * 2, grads, outs):
        count = len(scatter_buffers(kind, SCATTER_ORDER[kind]))
        units.append(scatter_unit(place, kind, SCATTER_ORDER[kind], g, o, scratch[:count]))
        scratch = scratch[count:]
    run(units)


def scatter(grads, small):
    tiled = [rows_to_tiles(g).reshape(tiled_shape(k)) for k, g in zip(KINDS * 2, grads)]
    out = dict(attn=(4, 4, 2, 128), up=(16, 2, 128), down=(4, 8, 128))
    bufs = [b for k in KINDS * 2 for b in scatter_buffers(k, SCATTER_ORDER[k])]
    *res, total = pl.pallas_call(
        scatter_kernel, name='scatter',
        in_specs=any_space(len(tiled)) + in_vmem(4), out_specs=in_vmem(len(tiled) + 1),
        out_shape=[SD(out[k], F32) for k in KINDS * 2] + [SD((2, 16, 512), F32)],
        scratch_shapes=[pltpu.VMEM((2, 16, 512), F32)] + total_buffers(16) + bufs + semaphores(180),
        compiler_params=pltpu.CompilerParams(collective_id=2, has_side_effects=True, vmem_limit_bytes=63 << 20),
    )(*tiled, *small)
    stack = lambda i: jnp.stack([tiles_to_rows(res[j][..., None, :, :, :]) for j in (i, i + 3)])
    return stack(0), stack(1), stack(2), total


HEAD_DIM = 64
EPS = 1e-5
THETA = 10000.0
NEG_BIG = -1e30
SEQ, DIM, FFN, TOKENS, CHUNK, BLOCK, WIDE = 512, 512, 2048, 1024, 512, 256, 128


def blocks(n):
    return range(0, n, BLOCK)


def dot(a, b, ca=1, cb=0):
    return lax.dot_general(a, b, (((ca,), (cb,)), ((), ())), preferred_element_type=F32)


def rotary_tables():
    half = HEAD_DIM // 2
    inv = (1.0 / (THETA ** (np.arange(half, dtype=np.float32) * np.float32(2.0 / HEAD_DIM)))).astype(np.float32)
    ang = np.arange(SEQ, dtype=np.float32)[:, None] * inv[None, :]
    cos, sin = np.cos(ang), np.sin(ang)
    return np.tile(cos, (1, 4)).astype(np.float32), np.concatenate([-sin, sin, -sin, sin], axis=1).astype(np.float32)


def swap_halves(t):
    lane = lax.broadcasted_iota(jnp.int32, t.shape, 1)
    return jnp.where(lax.rem(lane, HEAD_DIM) < HEAD_DIM // 2, pltpu.roll(t, 128 - HEAD_DIM // 2, 1), pltpu.roll(t, HEAD_DIM // 2, 1))


def normed(t):
    mean = jnp.mean(t, axis=-1, keepdims=True)
    cent = t - mean
    var = jnp.mean(cent * cent, axis=-1, keepdims=True)
    rstd = lax.rsqrt(var + EPS)
    return cent * rstd, rstd


def norm_back(dh, gain, xhat, rstd):
    dn = dh * gain
    return rstd * (dn - jnp.mean(dn, axis=-1, keepdims=True) - xhat * jnp.mean(dn * xhat, axis=-1, keepdims=True))


def half_mask(shape, axis, h):
    i = lax.broadcasted_iota(jnp.int32, shape, axis)
    return (i < HEAD_DIM) if h == 0 else (i >= HEAD_DIM)


def attn_fwd_kernel(len_ref, x_ref, w_ref, s_ref, cos_ref, sin_ref, h_ref, q_ref, k_ref, v_ref, p_ref, ctx_ref, x1_ref):
    seq = pl.program_id(0)
    limit = len_ref[seq]
    for r in blocks(SEQ):
        rows = pl.ds(r, BLOCK)
        xhat, _ = normed(x_ref[0, rows].astype(F32))
        h_ref[0, rows] = (xhat * s_ref[0, 4:5] + s_ref[0, 5:6]).astype(BF)
        h = h_ref[0, rows]
        cos, sin = cos_ref[rows], sin_ref[rows]
        for j in range(2):
            cols = slice(BLOCK * j, BLOCK * j + BLOCK)
            for kind, dst in enumerate((q_ref, k_ref, v_ref)):
                t = dot(h, w_ref[kind, :, cols]) + s_ref[0, kind:kind + 1, cols]
                if kind == 0:
                    t = t * (HEAD_DIM ** -0.5)
                for i in range(2):
                    u = t[:, WIDE * i:WIDE * i + WIDE]
                    if kind < 2:
                        u = u * cos + swap_halves(u) * sin
                    dst[0, rows, BLOCK * j + WIDE * i:BLOCK * j + WIDE * i + WIDE] = u.astype(BF)
    valid = lax.broadcasted_iota(jnp.int32, (1, SEQ), 1) < limit

    def pair(j, _):
        lanes = pl.ds(pl.multiple_of(j * WIDE, WIDE), WIDE)
        k, v = k_ref[0, :, lanes], v_ref[0, :, lanes]
        for r in blocks(SEQ):
            rows = pl.ds(r, BLOCK)
            q = q_ref[0, rows, lanes]
            ctx = None
            for h in range(2):
                m = half_mask((SEQ, WIDE), 1, h)
                kh, vh = jnp.where(m, k, 0), jnp.where(m, v, 0)
                s = jnp.where(valid, dot(q, kh, 1, 1), NEG_BIG)
                e = jnp.exp(s - jnp.max(s, axis=-1, keepdims=True))
                p = (e * (1.0 / jnp.sum(e, axis=-1, keepdims=True))).astype(BF)
                p_ref[0, 2 * j + h, rows] = p
                part = dot(p, vh)
                ctx = part if ctx is None else ctx + part
            ctx_ref[0, rows, lanes] = ctx.astype(BF)
        return 0

    lax.fori_loop(0, 4, pair, 0)
    for r in blocks(SEQ):
        rows = pl.ds(r, BLOCK)
        out = dot(ctx_ref[0, rows], w_ref[3])
        x1_ref[0, rows] = (x_ref[0, rows].astype(F32) + out + s_ref[0, 3:4]).astype(BF)


def mlp_fwd_kernel(x_ref, w1_ref, w2_ref, s_ref, h_ref, a_ref, g_ref, y_ref):
    x = x_ref[0].astype(F32)
    xhat, _ = normed(x)
    h = (xhat * s_ref[0, 6:7] + s_ref[0, 7:8]).astype(BF)
    h_ref[0] = h
    acc = x + s_ref[0, 12:13]
    for j in range(4):
        cols = slice(CHUNK * j, CHUNK * j + CHUNK)
        pre = dot(h, w1_ref[:, cols]) + s_ref[0, 8 + j:9 + j]
        cdf = 0.5 * (1.0 + lax.erf(pre * (1.0 / math.sqrt(2.0))))
        pdf = jnp.exp(-0.5 * pre * pre) * (1.0 / math.sqrt(2.0 * math.pi))
        g_ref[0, :, cols] = cdf + pre * pdf
        a = (pre * cdf).astype(BF)
        a_ref[0, :, cols] = a
        acc = acc + dot(a, w2_ref[cols, :])
    y_ref[0] = acc.astype(BF)


def mlp_bwd_kernel(dy_ref, a_ref, g_ref, h_ref, x1_ref, w1_ref, w2_ref, s_ref, gw1_ref, gw2_ref, dmid_ref, gs_ref, acc_ref):
    j = pl.program_id(0)
    dy = dy_ref[...]
    gw2_ref[...] = dot(a_ref[...], dy, 0, 0)
    bias = jnp.zeros((1, DIM), F32)
    for r in blocks(TOKENS):
        rows = pl.ds(r, BLOCK)
        dpre = dot(dy_ref[rows], w2_ref[...], 1, 1) * g_ref[rows]
        bias = bias + jnp.sum(dpre, axis=0, keepdims=True)
        a_ref[rows] = dpre.astype(BF)
        part = dot(a_ref[rows], w1_ref[...], 1, 1)

        @pl.when(j == 0)
        def _():
            acc_ref[rows] = part

        @pl.when(j > 0)
        def _():
            acc_ref[rows] = acc_ref[rows] + part
    gs_ref[pl.ds(4 + j, 1)] = bias
    gw1_ref[...] = dot(h_ref[...], a_ref[...], 0, 0)

    @pl.when(j == 3)
    def _():
        sums = [jnp.zeros((1, DIM), F32) for _ in range(4)]
        for r in blocks(TOKENS):
            rows = pl.ds(r, BLOCK)
            dh = acc_ref[rows]
            xhat, rstd = normed(x1_ref[rows].astype(F32))
            d = dy_ref[rows].astype(F32)
            dmid = (d + norm_back(dh, s_ref[0, 6:7], xhat, rstd)).astype(BF)
            dmid_ref[rows] = dmid
            for i, t in enumerate((d, dh * xhat, dh, dmid.astype(F32))):
                sums[i] = sums[i] + jnp.sum(t, axis=0, keepdims=True)
        for i in range(4):
            gs_ref[i:i + 1] = sums[i]


def attn_bwd_kernel(dmid_ref, x_ref, h_ref, q_ref, k_ref, v_ref, p_ref, ctx_ref, w_ref, s_ref, cos_ref, sin_ref,
                    gw_ref, dx_ref, gs_ref, dctx_ref, dproj_ref):
    seq = pl.program_id(0)

    def put(dst, value):
        @pl.when(seq == 0)
        def _():
            dst[...] = value

        @pl.when(seq > 0)
        def _():
            dst[...] = dst[...] + value

    dmid = dmid_ref[0]
    for r in blocks(SEQ):
        rows = pl.ds(r, BLOCK)
        dctx_ref[rows] = dot(dmid_ref[0, rows], w_ref[3], 1, 1).astype(BF)
    put(gw_ref.at[3], dot(ctx_ref[0], dmid, 0, 0))

    def pair(j, _):
        lanes = pl.ds(pl.multiple_of(j * WIDE, WIDE), WIDE)
        q, k, v, dc = q_ref[0, :, lanes], k_ref[0, :, lanes], v_ref[0, :, lanes], dctx_ref[:, lanes]
        qt, dct = q.T, dc.T
        dq, dkt, dvt = None, None, None
        for h in range(2):
            m = half_mask((SEQ, WIDE), 1, h)
            mt = half_mask((WIDE, SEQ), 0, h)
            kh, vh = jnp.where(m, k, 0), jnp.where(m, v, 0)
            qh, dch = jnp.where(mt, qt, 0), jnp.where(mt, dct, 0)
            p = p_ref[0, 2 * j + h]
            part = dot(dch, p)
            dvt = part if dvt is None else dvt + part
            ds = []
            for r in blocks(SEQ):
                pf = p[r:r + BLOCK].astype(F32)
                dp = dot(dc[r:r + BLOCK], vh, 1, 1)
                ds.append((pf * (dp - jnp.sum(dp * pf, axis=-1, keepdims=True))).astype(BF))
            ds = jnp.concatenate(ds, axis=0)
            part = dot(ds, kh)
            dq = part if dq is None else dq + part
            part = dot(qh, ds)
            dkt = part if dkt is None else dkt + part
        cos, sin = cos_ref[...], sin_ref[...]
        dq = (dq * cos - swap_halves(dq) * sin) * (HEAD_DIM ** -0.5)
        dk = dkt.T
        dk = dk * cos - swap_halves(dk) * sin
        dv = dvt.T
        for i, t in enumerate((dq, dk, dv)):
            t = t.astype(BF)
            dproj_ref[i, :, lanes] = t
        return 0

    lax.fori_loop(0, 4, pair, 0)
    dh = None
    rowsums = []
    for i in range(3):
        d = dproj_ref[i]
        put(gw_ref.at[i], dot(h_ref[0], d, 0, 0))
        rowsums.append(jnp.sum(d.astype(F32), axis=0, keepdims=True))
        part = dot(d, w_ref[i], 1, 1)
        dh = part if dh is None else dh + part
    xhat, rstd = normed(x_ref[0].astype(F32))
    dx_ref[0] = (dmid.astype(F32) + norm_back(dh, s_ref[0, 4:5], xhat, rstd)).astype(BF)
    rowsums.append(jnp.sum(dh * xhat, axis=0, keepdims=True))
    rowsums.append(jnp.sum(dh, axis=0, keepdims=True))
    put(gs_ref, jnp.concatenate(rowsums + [jnp.zeros((3, DIM), F32)], axis=0))


VM = 56 * 2 ** 20


def whole(shape):
    n = len(shape)
    return pl.BlockSpec(shape, lambda *_: (0,) * n)


def per_seq(shape):
    n = len(shape)
    return pl.BlockSpec((1,) + shape, lambda i: (i,) + (0,) * n)


def at_layer(layer, shape):
    n = len(shape)
    return pl.BlockSpec((1,) + shape, lambda *_: (layer,) + (0,) * n)


def attn_fwd(layer, lengths, x, w, s, cos, sin):
    t = per_seq((SEQ, DIM))
    b = SD((2, SEQ, DIM), BF)
    return pl.pallas_call(
        attn_fwd_kernel, grid=(2,), name='attn_fwd',
        in_specs=[pl.BlockSpec(memory_space=pltpu.SMEM), t, whole((4, DIM, DIM)), at_layer(layer, (16, DIM)), whole((SEQ, WIDE)), whole((SEQ, WIDE))],
        out_specs=[t, t, t, t, per_seq((8, SEQ, SEQ)), t, t],
        out_shape=[b, b, b, b, SD((2, 8, SEQ, SEQ), BF), b, b],
        compiler_params=pltpu.CompilerParams(vmem_limit_bytes=VM),
    )(lengths, x, w, s, cos, sin)


def mlp_fwd(layer, x1, w1, w2, s):
    R = 256
    row = lambda n: pl.BlockSpec((1, R, n), lambda i: (i // 2, i % 2, 0))
    return pl.pallas_call(
        mlp_fwd_kernel, grid=(4,), name='mlp_fwd',
        in_specs=[row(DIM), whole((DIM, FFN)), whole((FFN, DIM)), at_layer(layer, (16, DIM))],
        out_specs=[row(DIM), row(FFN), row(FFN), row(DIM)],
        out_shape=[SD((2, SEQ, DIM), BF), SD((2, SEQ, FFN), BF), SD((2, SEQ, FFN), F32), SD((2, SEQ, DIM), BF)],
        compiler_params=pltpu.CompilerParams(vmem_limit_bytes=VM),
    )(x1, w1, w2, s)


def mlp_bwd(layer, dy, a, g, h, x1, w1, w2, s):
    flat = lambda t: t.reshape(TOKENS, t.shape[-1])
    full = whole((TOKENS, DIM))
    return pl.pallas_call(
        mlp_bwd_kernel, grid=(4,), name='mlp_bwd',
        in_specs=[full, pl.BlockSpec((TOKENS, CHUNK), lambda j: (0, j)), pl.BlockSpec((TOKENS, CHUNK), lambda j: (0, j)), full, full,
                  pl.BlockSpec((DIM, CHUNK), lambda j: (0, j)), pl.BlockSpec((CHUNK, DIM), lambda j: (j, 0)), at_layer(layer, (16, DIM))],
        out_specs=[pl.BlockSpec((DIM, CHUNK), lambda j: (0, j)), pl.BlockSpec((CHUNK, DIM), lambda j: (j, 0)), full, whole((8, DIM))],
        out_shape=[SD((DIM, FFN), F32), SD((FFN, DIM), F32), SD((TOKENS, DIM), BF), SD((8, DIM), F32)],
        scratch_shapes=[pltpu.VMEM((TOKENS, DIM), F32)],
        compiler_params=pltpu.CompilerParams(vmem_limit_bytes=VM),
    )(flat(dy), flat(a), flat(g), flat(h), flat(x1), w1, w2, s)


def attn_bwd(layer, dmid, x, h, q, k, v, p, ctx, w, s, cos, sin):
    t = per_seq((SEQ, DIM))
    return pl.pallas_call(
        attn_bwd_kernel, grid=(2,), name='attn_bwd',
        in_specs=[t, t, t, t, t, t, per_seq((8, SEQ, SEQ)), t, whole((4, DIM, DIM)), at_layer(layer, (16, DIM)), whole((SEQ, WIDE)), whole((SEQ, WIDE))],
        out_specs=[whole((4, DIM, DIM)), t, whole((8, DIM))],
        out_shape=[SD((4, DIM, DIM), F32), SD((2, SEQ, DIM), BF), SD((8, DIM), F32)],
        scratch_shapes=[pltpu.VMEM((SEQ, DIM), BF), pltpu.VMEM((3, SEQ, DIM), BF)],
        compiler_params=pltpu.CompilerParams(vmem_limit_bytes=VM),
    )(dmid.reshape(2, SEQ, DIM), x, h, q, k, v, p, ctx, w, s, cos, sin)


def compute(x, lengths, d_y, whole_wts, small):
    cos, sin = (jnp.asarray(t) for t in rotary_tables())
    saved, y = [], x
    for l in range(2):
        fa, fu, fd = whole_wts[l]
        h1, q, k, v, p, ctx, x1 = attn_fwd(l, lengths, y, fa, small, cos, sin)
        h2, a, g, y2 = mlp_fwd(l, x1, fu, fd, small)
        saved.append((y, h1, q, k, v, p, ctx, x1, h2, a, g))
        y = y2
    d, grads = d_y, [None, None]
    for l in (1, 0):
        x_in, h1, q, k, v, p, ctx, x1, h2, a, g = saved[l]
        fa, fu, fd = whole_wts[l]
        gu, gd, dmid, s_mlp = mlp_bwd(l, d, a, g, h2, x1, fu, fd, small)
        ga, d, s_attn = attn_bwd(l, dmid, x_in, h1, q, k, v, p, ctx, fa, small, cos, sin)
        grads[l] = (ga, gu, gd, s_mlp, s_attn)
    return d, grads


def pack_small(b_attn, ln_par, b_up, b_down, index):
    rows = jnp.concatenate([b_attn, ln_par, b_down[:, None]], axis=1).astype(F32)
    rows = lax.dynamic_update_slice(jnp.zeros((2, 9, DIM), F32), rows, (0, 0, 2 * index))
    ups = lax.dynamic_update_slice(jnp.zeros((2, FFN), F32), b_up.astype(F32), (0, 8 * index))
    return jnp.concatenate([rows[:, :8], ups.reshape(2, 4, DIM), rows[:, 8:], jnp.zeros((2, 3, DIM), F32)], axis=1)


def solution(mesh):
    grid = Mesh(mesh.devices.reshape([SIZES[a] for a in AXES]), AXES)
    first, second, third = P(AXES), P(None, AXES), P(None, None, AXES)
    weight_specs = (third, third, third, second, second, second, second)

    def device_step(x, lengths, d_y, w_attn, b_attn, ln_par, w_up, b_up, w_down, b_down):
        index = lax.axis_index(AXES)
        whole_wts, small = gather(w_attn, w_up, w_down, pack_small(b_attn, ln_par, b_up, b_down, index))
        d_x, grads = compute(x, lengths, d_y, whole_wts, small)
        o_attn, o_up, o_down, sums = scatter([g for layer in grads for g in layer[:3]], [s for layer in grads for s in layer[3:]])
        pick = lax.dynamic_slice(sums, (0, 0, 2 * index), (2, 16, 2))
        ups = lax.dynamic_slice(sums[:, 4:8].reshape(2, FFN), (0, 8 * index), (2, 8))
        rows = lambda *ids: jnp.stack([pick[:, i] for i in ids], axis=1)
        return d_x, o_attn, rows(8, 9, 10, 3), rows(11, 12, 1, 2), o_up, ups, o_down, pick[:, 0]

    return jax.shard_map(device_step, mesh=grid, in_specs=(first,) * 3 + weight_specs, out_specs=(first,) + weight_specs, check_vma=False)
```

```python
import math
import jax
import jax.numpy as jnp
import numpy as np
from jax import lax
from jax.experimental import pallas as pl
from jax.experimental.pallas import tpu as pltpu
from jax.sharding import Mesh, PartitionSpec as P

HEAD_DIM, EPS, THETA, NEG_BIG = 64, 1e-5, 10000.0, -1e30
SEQ, DIM, FFN, TOKENS, CHUNK, BLOCK, WIDE = 512, 512, 2048, 1024, 512, 256, 128
LAYERS = CORES = SEQS = PAIR = 2
MATRICES = CHUNKS = QUAD = 4
HEADS = OCT = 8
SMALL = 16
F32, BF = jnp.float32, jnp.bfloat16
SD = jax.ShapeDtypeStruct
AXES = ('z', 'y', 'x', 'c')
SIZES = dict(z=OCT, y=QUAD, x=QUAD, c=PAIR, k=PAIR, h=PAIR, l=PAIR, r=PAIR)
TILE = (OCT, WIDE)
ALL = slice(None)
BIAS_OUT, GAIN1, SHIFT1, GAIN2, SHIFT2, BIAS_UP, BIAS_DOWN = 3, 4, 5, 6, 7, 8, 12
TILED = dict(part='kzyht', slim='zyht', pair='zyht', up='zyht', down='zyxct')
FINE = dict(attn='kzyhtlcr', up='zyhtlcr', down='zyxct')
LANE_TILES = dict(attn=QUAD, part=PAIR, slim=PAIR, pair=PAIR, up=OCT, down=PAIR)
OWNER = dict(x='xhl', y='y', z='z')
UNITS = dict(up='yzx', down='xyz', part='hyzl', slim='yzx', pair='hyzl')
MLP_STEPS, ATTN_STEPS = CHUNKS, 8
LAYER_STEPS = MLP_STEPS + ATTN_STEPS
STEPS = LAYERS * LAYER_STEPS
SETS = (('up', 'up', ('t', PAIR, CHUNKS)), ('down', 'down', ('z', PAIR, CHUNKS)), ('first', 'part', ('z', OCT, 1)), ('second', 'slim', ('z', OCT, 1)), ('third', 'pair', ('z', OCT, 1)))
SCHEDULE = {(1, 'up'): 'ABCDEKNOP', (1, 'down'): 'ABCDEKNOP', (1, 'first'): 'HLNOPTU', (1, 'second'): 'LMPQSV', (1, 'third'): 'LMPQSTV',
            (0, 'up'): 'MNOPQVcd', (0, 'down'): 'MNOPQVcd', (0, 'first'): 'TUX', (0, 'second'): 'Xa', (0, 'third'): 'Xa'}
ENDING = 'mstfmudstfmstfmstftmm'
VM = 56 << 20


def spot(at):
    return dict(at, h=lax.div(at['x'], SIZES['l']), l=lax.rem(at['x'], SIZES['l']))


def only(at, names):
    return {n: at[n] for n in names if n in at}


def view(ref, names, pick):
    return ref.at[tuple(pick.get(n, ALL) for n in names)]


class Place:
    def __init__(self, send, recv):
        self.me = spot({a: lax.axis_index(a) for a in AXES})
        self.send, self.recv, self.used = send, recv, 0

    def shifted(self, axis, s):
        at = dict(self.me, **{axis: lax.rem(self.me[axis] + s, SIZES[axis])})
        if axis in 'hl':
            at['x'] = SIZES['l'] * at['h'] + at['l']
        return spot(at)

    def device(self, axis, s):
        at = self.shifted(axis, s)
        return tuple(at[a] for a in AXES)

    def peers(self, axis):
        n = SIZES[axis]
        return sorted(range(1, n), key=lambda s: min(s, n - s))

    def signal(self, sem, axis, s):
        pl.semaphore_signal(sem, inc=1, device_id=self.device(axis, s), device_id_type=pl.DeviceIdType.MESH)

    def greet(self):
        bar = pltpu.get_barrier_semaphore()
        everyone = [(a, s) for a in AXES for s in self.peers(a)]
        for a, s in everyone:
            self.signal(bar, a, s)
        pl.semaphore_wait(bar, len(everyone))

    def begin(self, build):
        self.used += 1
        assert self.used <= self.send.shape[0]
        build().start()
        return lambda: build().wait()

    def copy(self, axis, s, refs):
        i = self.used

        def build():
            src, dst = refs()
            return pltpu.make_async_remote_copy(src, dst, self.send.at[i], self.recv.at[i], device_id=self.device(axis, s), device_id_type=pl.DeviceIdType.MESH)
        return self.begin(build)

    def local(self, refs):
        i = self.used
        return self.begin(lambda: pltpu.make_async_copy(*refs(), self.send.at[i]))


def half(kind, core, part):
    if kind == 'attn':
        return dict(k=pl.ds(core * CORES + part, 1))
    return dict(t=pl.ds(core * LANE_TILES[kind], LANE_TILES[kind]))


def gathered(kind, full, part):
    names = FINE[kind]
    return lambda core, fixed, at: view(full, names, dict(half(kind, core(at), part), **only(at, fixed)))


def own(at):
    return at['c']


def other(at):
    return 1 - at['c']


def gather_early(place, kind, part, order, full, shard):
    block = gathered(kind, full, part)
    names = FINE[kind]
    mine = [n for n in names if n not in 'tkr']
    rows = [n for n in names if n in 'tk'] + ['r', 'r']

    def piece(core):
        return view(shard, rows, half(kind, core(place.me), part))
    waits = [place.local(lambda: (piece(own), block(own, mine, place.me))),
             place.copy('c', 1, lambda: (piece(other), block(other, mine, place.me)))]
    for i in range(len(order) - 1):
        yield
        for w in waits:
            w()
        fixed = ''.join(OWNER[a] for a in order[i:])
        waits = [place.copy(order[i], s, lambda: (block(own, fixed, place.me),) * PAIR) for s in place.peers(order[i])]
    yield
    for w in waits:
        w()


def gather_late(place, kind, part, order, full):
    block = gathered(kind, full, part)
    axis = order[-1]
    fixed = OWNER[axis]
    same = lambda at: (block(own, fixed, at),) * PAIR
    waits = [(s, place.copy(axis, s, lambda: same(place.me))) for s in place.peers(axis)]
    last = [place.copy('c', 1, lambda: same(place.me))]
    for s, w in waits:
        yield
        w()
        last.append(place.copy('c', 1, lambda s=s: same(place.shifted(axis, SIZES[axis] - s))))
    yield
    for w in last:
        w()


def gather_whole(*args):
    yield from gather_early(*args)
    yield from gather_late(*args[:-1])


def unravel(i, shape):
    idx = []
    for n in reversed(shape):
        idx.append(lax.rem(i, n))
        i = lax.div(i, n)
    return tuple(reversed(idx))


def each(shape, body):
    def step(i, carry):
        body(unravel(i, shape))
        return carry
    lax.fori_loop(0, math.prod(shape), step, 0)


def total_unit(place, value, out, slots):
    me = place.me
    keep, slot, *slots = slots
    wait = place.copy('c', 1, lambda: (value.at[other(me)], slot.at[0]))
    yield
    wait()
    keep[...] = value[me['c']] + slot[0]
    for axis, slot in zip('xyz', slots):
        last = SIZES[axis] - 1
        slot[last] = keep[...]
        waits = [place.copy(axis, s, lambda s=s: (slot.at[last], slot.at[s - 1])) for s in place.peers(axis)]
        yield
        for w in waits:
            w()
        v = slot[0]
        for s in range(1, SIZES[axis]):
            v = v + slot[s]
        keep[...] = v
    out[me['c']] = keep[...]
    wait = place.copy('c', 1, lambda: (keep, out.at[me['c']]))
    yield
    wait()


def total_buffers():
    return [pltpu.VMEM((SMALL, DIM), F32)] + [pltpu.VMEM((SIZES[a], SMALL, DIM), F32) for a in 'cxyz']


def run(units):
    units = list(units)
    while units:
        units = [u for u in units if next(u, units) is not units]


def free_sizes(kind, names):
    return tuple(LANE_TILES[kind] if n == 't' else SIZES[n] for n in names) + TILE


def plan(kind):
    left = TILED[kind]
    for axis in UNITS[kind]:
        d = axis if axis in left else 'h' if axis == 'x' else ''
        left = left.replace(d, '')
        yield axis, d, left


def unit_buffers(kind, layers):
    slots = [pltpu.VMEM((SIZES[axis] - 1,) + free_sizes(kind, left), F32) for axis, _, left in plan(kind)]
    *_, (_, _, left) = plan(kind)
    _, _, first = next(plan(kind))
    shapes = [(PAIR,) + free_sizes(kind, TILED[kind]), free_sizes(kind, TILED[kind]), free_sizes(kind, first)]
    return [pltpu.VMEM(s, F32) for s in shapes] + slots[:1] + (slots[1:] + [pltpu.VMEM(free_sizes(kind, left.replace('c', '')), F32)]) * layers


def reduce_unit(place, kind, bufs, finish, pieces, give, take):
    grad, got, first, slots, *rest = bufs
    me = place.me
    whole_grad, whole_names = grad, 'g' + TILED[kind]
    names, pick = whole_names, dict(g=me['c'])
    dim, size, count = pieces

    def cut(i, n=1):
        return {dim: pl.ds(size * i, size * n)}

    def accumulate(terms, fixed, into, piece=None):
        left = [n for n in names if n not in fixed]
        lead = left[:-3]
        sizes_of = dict(SIZES, t=LANE_TILES[kind])
        if piece is not None:
            sizes_of[dim] = size

        def body(idx):
            loop = dict(zip(lead, idx))
            if piece is not None:
                loop[dim] = loop[dim] + size * piece if dim in loop else pl.ds(size * piece, size)
            mine = tuple(fixed.get(n, loop.get(n, ALL)) for n in names)
            at = tuple(loop.get(n, ALL) for n in left)
            v = grad[mine]
            for ref in terms:
                v = v + ref[at]
            into[mine if into is grad else at] = v
        if lead:
            each([sizes_of[n] for n in lead], body)
        else:
            body(())

    (axis, d, left), *later = plan(kind)
    arrived, waits = [], []

    def begin(start, n):
        if not waits:
            take(1)
        for i in range(start, start + n):
            arrived[i]()
            accumulate([got], pick, grad, i)
        for s in place.peers(axis):
            waits.append(place.copy(axis, s, lambda s=s: (view(whole_grad, whole_names, dict(only(place.shifted(axis, s), d), g=me['c'], **cut(start, n))),
                                                          view(slots, 's' + TILED[kind].replace(d, ''), dict(cut(start, n), s=s - 1)))))
    take(0)
    for i in range(count):
        arrived.append(place.copy('c', 1, lambda i=i: (view(whole_grad, whole_names, dict(cut(i), g=other(me))), view(got, TILED[kind], cut(i)))))
        if i and count == PAIR * i:
            begin(0, i)
        yield
    begin(count // PAIR, count - count // PAIR)
    give(0)
    yield
    for w in waits:
        w()
    pick = dict(pick, **only(me, d))
    accumulate([slots.at[s] for s in range(SIZES[axis] - 1)], pick, first)
    give(1)
    grad, names, pick = first, left, {}
    for axis, d, left in later:
        slots, *rest = rest
        waits = [place.copy(axis, s, lambda s=s: (view(first, names, dict(pick, **only(place.shifted(axis, s), d))), slots.at[s - 1])) for s in place.peers(axis)]
        yield
        for w in waits:
            w()
        pick = dict(pick, **only(me, d))
        accumulate([slots.at[s] for s in range(SIZES[axis] - 1)], pick, first)
    away, = rest
    last = (lambda core: dict(pick, c=core(me))) if 'c' in left else (lambda core: pick)
    wait = place.copy('c', 1, lambda: (view(first, names, last(other)), away))
    yield
    wait()
    rows = ALL if kind == 'down' else pl.ds((me['l'] * PAIR + me['c']) * PAIR, PAIR)
    finish(own(me), first[tuple(last(own).get(n, ALL) for n in names) + (rows,)])
    finish(other(me), away[..., rows, :])


def blocks(n):
    return range(0, n, BLOCK)


def lane(i):
    return slice(WIDE * i, WIDE * i + WIDE)


def dot(a, b, ca=1, cb=0):
    return lax.dot_general(a, b, (((ca,), (cb,)), ((), ())), preferred_element_type=F32)


def rotary_tables():
    half_dim = HEAD_DIM // PAIR
    inv = (1.0 / (THETA ** (np.arange(half_dim, dtype=np.float32) * np.float32(2.0 / HEAD_DIM)))).astype(np.float32)
    ang = np.arange(SEQ, dtype=np.float32)[:, None] * inv[None, :]
    cos, sin = np.cos(ang), np.sin(ang)
    return np.tile(cos, (1, QUAD)), np.concatenate([-sin, sin] * PAIR, axis=1)


def swap_halves(t):
    n = HEAD_DIM // PAIR
    lanes = lax.broadcasted_iota(jnp.int32, t.shape, 1)
    return jnp.where(lax.rem(lanes, HEAD_DIM) < n, pltpu.roll(t, WIDE - n, 1), pltpu.roll(t, n, 1))


def normed(t):
    cent = t - jnp.mean(t, axis=-1, keepdims=True)
    rstd = lax.rsqrt(jnp.mean(cent * cent, axis=-1, keepdims=True) + EPS)
    return cent * rstd, rstd


def norm_back(dh, gain, xhat, rstd):
    dn = dh * gain
    return rstd * (dn - jnp.mean(dn, axis=-1, keepdims=True) - xhat * jnp.mean(dn * xhat, axis=-1, keepdims=True))


def row(ref, i):
    return ref[i:i + 1]


def half_mask(shape, axis, h):
    i = lax.broadcasted_iota(jnp.int32, shape, axis)
    return i >= HEAD_DIM if h else i < HEAD_DIM


def any_space(n):
    return [pl.BlockSpec(memory_space=pl.ANY)] * n


def in_vmem(n):
    return [pl.BlockSpec(memory_space=pltpu.VMEM)] * n


def semaphores(n):
    return [pltpu.SemaphoreType.DMA((n,))] * PAIR


def whole(shape, **kw):
    return pl.BlockSpec(shape, lambda *_: (0,) * len(shape), **kw)


def tiles_to_rows(t):
    *lead, r, n, s, w = t.shape
    return t.swapaxes(-3, -2).reshape(*lead, r * s, n * w)


def natural(kind, full):
    n = full.shape[FINE[kind].index('t')]
    lead = (MATRICES,) if kind == 'attn' else ()
    return tiles_to_rows(full.reshape(*lead, -1, n, *TILE))


def fine_shape(kind):
    n = LANE_TILES[kind] if kind == 'attn' else PAIR * LANE_TILES[kind]
    dims = dict(SIZES, t=n, k=MATRICES)
    return tuple(dims[d] for d in FINE[kind]) + ((WIDE,) if 'r' in FINE[kind] else TILE)


GATHERS = (('attn', 0, 0, 'zxy'), ('attn', 0, 1, 'zyx'), ('up', 0, 0, 'zxy'), ('down', 0, 0, 'zyx'),
           ('attn', 1, 0, 'zxy'), ('attn', 1, 1, 'zyx'), ('up', 1, 0, 'zxy'), ('down', 1, 0, 'zyx'))
LATE = (GATHERS[2:6], GATHERS[6:])
KINDS = tuple(FINE)


def gather_kernel(sa, su, sd, b_attn, ln, b_up, b_down, *refs):
    n = LAYERS * len(KINDS)
    full, total, value, slots, sems = refs[:n], refs[n], refs[n + 1], refs[n + 2:-2], refs[-2:]
    place = Place(*sems)
    place.greet()
    shards, full = dict(zip(KINDS, (sa, su, sd))), dict(zip([(k, l) for l in range(LAYERS) for k in KINDS], full))
    me = place.me
    index = ((me['z'] * SIZES['y'] + me['y']) * SIZES['x'] + me['x']) * CORES + me['c']

    def spread(v, rows):
        n = v.shape[1]
        at = lax.broadcasted_iota(jnp.int32, (rows, DIM), 1) - n * index
        if v.shape[0] < rows:
            at = at + DIM * lax.broadcasted_iota(jnp.int32, (rows, DIM), 0)
        return sum(jnp.where(at == i, v[:, i:i + 1], 0.0) for i in range(n))
    value[...] = jnp.zeros_like(value)
    for l in range(LAYERS):
        value[l, :GAIN1] = spread(b_attn[l].astype(F32), QUAD)
        value[l, GAIN1:BIAS_UP] = spread(ln[l].astype(F32), QUAD)
        value[l, BIAS_UP:BIAS_DOWN] = spread(b_up[l:l + 1].astype(F32), QUAD)
        value[l, BIAS_DOWN:BIAS_DOWN + 1] = spread(b_down[l:l + 1].astype(F32), 1)
    units = [(gather_early if g in sum(LATE, ()) else gather_whole)(place, g[0], *g[2:], full[g[:2]], shards[g[0]].at[g[1]]) for g in GATHERS]
    run([units[0], units[1], total_unit(place, value, total, slots)] + units[2:])


def gather(attn, up, down, *small):
    shards = [attn.reshape(LAYERS, MATRICES, PAIR, -1, WIDE).swapaxes(-3, -2), up.reshape(LAYERS, PAIR, -1, WIDE).swapaxes(-3, -2),
              down.reshape(LAYERS, OCT, -1, WIDE).swapaxes(-3, -2)]
    keys = [(k, l) for l in range(LAYERS) for k in KINDS]
    *full, total = pl.pallas_call(
        gather_kernel, name='gather',
        in_specs=in_vmem(len(shards) + len(small)), out_specs=any_space(len(keys)) + in_vmem(1),
        out_shape=[SD(fine_shape(k), BF) for k, _ in keys] + [SD((LAYERS, SMALL, DIM), F32)],
        scratch_shapes=[pltpu.VMEM((LAYERS, SMALL, DIM), F32)] + total_buffers() + semaphores(200),
        compiler_params=pltpu.CompilerParams(collective_id=1, has_side_effects=True),
    )(*shards, *small)
    return dict(zip(keys, full)), total


def attn_fwd_kernel(late, len_ref, x_ref, w_ref, s_ref, cos_ref, sin_ref, *refs):
    h_ref, q_ref, k_ref, v_ref, ctx_ref, x1_ref, p_ref, *full = refs[:-2]
    t = pl.program_id(0)
    seq, j = lax.div(t, QUAD), lax.rem(t, QUAD)
    place = Place(*refs[-2:])
    full = dict(zip(sorted({g[:2] for g in late}), full))
    gens = []

    @pl.when(t == 0)
    def _():
        place.greet()
        for g in late:
            gens.append(gather_late(place, g[0], *g[2:], full[g[:2]]))
            next(gens[-1])

    @pl.when(j == 0)
    def _():
        for r in blocks(SEQ):
            rows = pl.ds(r, BLOCK)
            xhat, _ = normed(x_ref[0, rows].astype(F32))
            h_ref[0, rows] = (xhat * row(s_ref, GAIN1) + row(s_ref, SHIFT1)).astype(BF)
            h = h_ref[0, rows]
            cos, sin = cos_ref[rows], sin_ref[rows]
            for c in blocks(DIM):
                cols = slice(c, c + BLOCK)
                for kind, dst in enumerate((q_ref, k_ref, v_ref)):
                    u = dot(h, w_ref[kind, :, cols]) + s_ref[kind:kind + 1, cols]
                    if dst is q_ref:
                        u = u * (HEAD_DIM ** -0.5)
                    for i in range(PAIR):
                        e = u[:, lane(i)]
                        if dst is not v_ref:
                            e = e * cos + swap_halves(e) * sin
                        dst[0, rows, c + WIDE * i:c + WIDE * i + WIDE] = e.astype(BF)

    valid = lax.broadcasted_iota(jnp.int32, (1, SEQ), 1) < len_ref[seq]
    lanes = pl.ds(pl.multiple_of(j * WIDE, WIDE), WIDE)
    masks = [half_mask((SEQ, WIDE), 1, h) for h in range(PAIR)]
    ks = [jnp.where(m, k_ref[0, :, lanes], 0) for m in masks]
    vs = [jnp.where(m, v_ref[0, :, lanes], 0) for m in masks]
    chains = [(r, h) for r in blocks(SEQ) for h in range(PAIR)]

    def score(r, h):
        return dot(q_ref[0, pl.ds(r, BLOCK), lanes], ks[h], 1, 1)
    ahead, ctx = score(*chains[0]), 0
    for i, (r, h) in enumerate(chains):
        s = jnp.where(valid, ahead, NEG_BIG)
        if i + 1 < len(chains):
            ahead = score(*chains[i + 1])
        e = jnp.exp(s - jnp.max(s, axis=-1, keepdims=True))
        p = (e * (1.0 / jnp.sum(e, axis=-1, keepdims=True))).astype(BF)
        p_ref[0, h, pl.ds(r, BLOCK)] = p
        ctx = ctx + dot(p, vs[h]) if h else dot(p, vs[h])
        if h:
            ctx_ref[0, pl.ds(r, BLOCK), lanes] = ctx.astype(BF)

    @pl.when(j == QUAD - 1)
    def _():
        for r in blocks(SEQ):
            rows = pl.ds(r, BLOCK)
            x1_ref[0, rows] = (x_ref[0, rows].astype(F32) + dot(ctx_ref[0, rows], w_ref[BIAS_OUT]) + row(s_ref, BIAS_OUT)).astype(BF)

    for step, count in ((4, PAIR), (6, 1), (7, OCT)):
        @pl.when(t == step)
        def _():
            for gen in gens if step == 7 else gens[:PAIR]:
                for _ in range(count):
                    next(gen, 0)


def mlp_fwd_kernel(x_ref, w1_ref, w2_ref, s_ref, h_ref, a_ref, g_ref, *y_ref):
    x = x_ref[0].astype(F32)
    xhat, _ = normed(x)
    h = (xhat * row(s_ref, GAIN2) + row(s_ref, SHIFT2)).astype(BF)
    h_ref[0] = h
    acc = x + row(s_ref, BIAS_DOWN)
    for j in range(CHUNKS):
        cols = slice(CHUNK * j, CHUNK * j + CHUNK)
        pre = dot(h, w1_ref[:, cols]) + row(s_ref, BIAS_UP + j)
        cdf = 0.5 * (1.0 + lax.erf(pre * (1.0 / math.sqrt(2.0))))
        pdf = jnp.exp(-0.5 * pre * pre) * (1.0 / math.sqrt(2.0 * math.pi))
        g_ref[0, :, cols] = cdf + pre * pdf
        a = (pre * cdf).astype(BF)
        a_ref[0, :, cols] = a
        if y_ref:
            acc = acc + dot(a, w2_ref[cols, :])
    for ref in y_ref:
        ref[0] = acc.astype(BF)


def layer_small(layer):
    return pl.BlockSpec((None, SMALL, DIM), lambda *_: (layer, 0, 0))


def attn_fwd(layer, lengths, x, w, s, cos, sin, prev, late):
    seq = lambda t: (lax.div(t, QUAD), 0, 0)
    t = pl.BlockSpec((1, SEQ, DIM), seq)
    saved = [pl.BlockSpec((None, 1, SEQ, DIM), lambda t: (layer,) + seq(t))] * 6
    saved.append(pl.BlockSpec((None, 1, PAIR, SEQ, SEQ), lambda t: (layer, lax.div(t, QUAD), lax.rem(t, QUAD), 0, 0)))
    inputs = [lengths, x, w, s, cos, sin]
    n, m = len(inputs), len(prev)

    def body(*refs):
        attn_fwd_kernel(LATE[layer], *refs[:n], *refs[n + m + len(late):])
    res = pl.pallas_call(
        body, name='attn_fwd', grid=(OCT,),
        in_specs=[pl.BlockSpec(memory_space=pltpu.SMEM), t, whole((MATRICES, DIM, DIM)), layer_small(layer), whole((SEQ, WIDE)), whole((SEQ, WIDE))] + any_space(m + len(late)),
        out_specs=saved + any_space(len(late)),
        out_shape=[SD((LAYERS, SEQS, SEQ, DIM), BF)] * 6 + [SD((LAYERS, SEQS, HEADS, SEQ, SEQ), BF)] + [SD(e.shape, BF) for e in late],
        input_output_aliases=dict([(n + i, i) for i in range(m)] + [(n + m + i, len(saved) + i) for i in range(len(late))]),
        scratch_shapes=semaphores(40),
        compiler_params=pltpu.CompilerParams(collective_id=2 + layer, has_side_effects=True, vmem_limit_bytes=VM),
    )(*inputs, *prev, *late)
    return res[:len(saved)], res[len(saved):]


def mlp_fwd(layer, x1, w1, w2, s, prev):
    place = lambda t: (layer, lax.div(t, PAIR), lax.rem(t, PAIR), 0)
    block = lambda n: pl.BlockSpec((None, 1, BLOCK, n), place)
    widths = [(DIM, BF), (FFN, BF), (FFN, F32)]
    outs = [block(w) for w, _ in widths] + [pl.BlockSpec((1, BLOCK, DIM), lambda t: place(t)[1:])] * (1 - layer)
    shapes = [SD((LAYERS, SEQS, SEQ, w), d) for w, d in widths] + [SD((SEQS, SEQ, DIM), BF)] * (1 - layer)
    inputs = [x1, w1, w2, s]
    n, m = len(inputs), len(prev)
    return pl.pallas_call(
        lambda *refs: mlp_fwd_kernel(*refs[:n], *refs[n + m:]), name='mlp_fwd', grid=(QUAD,),
        in_specs=[block(DIM), whole((DIM, FFN)), whole((FFN, DIM)), layer_small(layer)] + any_space(m),
        out_specs=outs, out_shape=shapes,
        input_output_aliases={n + i: i for i in range(m)},
        compiler_params=pltpu.CompilerParams(vmem_limit_bytes=VM),
    )(*inputs, *prev)


def backward_kernel(dy, a, g, q, k, v, p, s, cos_ref, sin_ref, h2, x1, h1, ctx, x0, y0, w1_0, w1_1, w2_0, w2_1, wa_0, wa_1,
                    d_x, g_attn, g_up, g_down, gb_attn, g_ln, gb_up, gb_down, dx, dmid, dproj, dpre, acc, value, total, w1, w2, wa, h2s, h1s, late, *refs):
    credits, fetched, *sems = refs[-4:]
    t = pl.program_id(0)
    layer, r = 1 - lax.div(t, LAYER_STEPS), lax.rem(t, LAYER_STEPS)
    place = Place(*sems)
    me = place.me
    slots, refs = refs[:len(total_buffers())], refs[len(total_buffers()):-4]

    def finish_of(name, l):
        def finish(core, part):
            if name == 'down':
                for i in range(PAIR):
                    g_down[l, :, pl.ds(pl.multiple_of((PAIR * core + i) * WIDE, WIDE), WIDE)] = part[i]
            elif name == 'up':
                for i in range(OCT):
                    at = i // PAIR * QUAD + PAIR * core + i % PAIR
                    g_up[l, :, pl.ds(pl.multiple_of(at * WIDE, WIDE), WIDE)] = part[i]
            elif name == 'first':
                for i in range(QUAD):
                    g_attn[l, PAIR * core + i // PAIR, :, lane(i % PAIR)] = part[i // PAIR, i % PAIR]
            else:
                for i in range(PAIR):
                    g_attn[l, PAIR * core + (name == 'third'), :, lane(PAIR + i)] = part[i]
        return finish

    gens, grads = {}, {}
    for i, (name, kind, pieces) in enumerate(SETS):
        m = len(unit_buffers(kind, 1)) - QUAD
        shared, later, refs = refs[:QUAD], refs[QUAD:QUAD + LAYERS * m], refs[QUAD + LAYERS * m:]
        grads[name] = shared[0]
        axis = UNITS[kind][0]
        groups = [[('c', 1)], [(axis, e) for e in place.peers(axis)]]

        def give(which, groups=groups, i=i):
            for e in groups[which]:
                place.signal(credits.at[PAIR * i + which], *e)

        def take(which, groups=groups, i=i):
            pl.semaphore_wait(credits.at[PAIR * i + which], len(groups[which]))
        nothing = lambda which: None
        for l in (1, 0):
            gens[l, name] = reduce_unit(place, kind, [*shared, *later[m * l:m * l + m]], finish_of(name, l), pieces, give if l else nothing, nothing if l else take)

    loads = dict(w2=(w2_0, w2_1, w2), w1=(w1_0, w1_1, w1), h2=(h2.at[0], h2.at[1], h2s), x1=(x1.at[0], x1.at[1], late), h1=(h1.at[0], h1.at[1], h1s),
                 wa=(wa_0, wa_1, wa), ctx=(ctx.at[0], ctx.at[1], late), xin=(x0, y0, late))
    starts = {(1, 'w2'): 'A', (1, 'w1'): 'A', (1, 'h2'): 'A', (1, 'x1'): 'A', (1, 'h1'): 'B', (1, 'wa'): 'B', (1, 'ctx'): 'E', (1, 'xin'): 'I',
              (0, 'w2'): 'E', (0, 'w1'): 'E', (0, 'h2'): 'E', (0, 'x1'): 'M', (0, 'h1'): 'M', (0, 'wa'): 'M', (0, 'ctx'): 'Q', (0, 'xin'): 'U'}

    def load(name, l):
        return pltpu.make_async_copy(loads[name][l], loads[name][-1], fetched.at[list(loads).index(name)])

    @pl.when(t == 0)
    def _():
        place.greet()
        dx[...] = dy[...]
        value[...] = jnp.zeros_like(value)

    for step in range(STEPS):
        due = [key for key, letter in starts.items() if ord(letter) - ord('A') == step]
        if due:
            @pl.when(t == step)
            def _():
                for l, name in due:
                    load(name, l).start()

    def put(ref, where, part, shape):
        ref[where] = part.reshape(shape + TILE)

    def add_sums(rows, terms):
        for i, e in zip(rows, terms):
            value[layer, i:i + 1] += jnp.sum(e, axis=0, keepdims=True)

    @pl.when(r == 0)
    def _():
        for name in ('w2', 'w1', 'h2'):
            load(name, 0).wait()

    @pl.when(r < MLP_STEPS)
    def _():
        gw = dot(a[...], dx[...], 0, 0)
        for i in range(QUAD):
            put(grads['down'], (i // PAIR, pl.ds(PAIR * r, PAIR), ALL, ALL, ALL, i % PAIR), gw[:, lane(i)], (PAIR, QUAD, QUAD, CORES))
        chunk = pl.ds(pl.multiple_of(r * CHUNK, CHUNK), CHUNK)
        bias = jnp.zeros((1, DIM), F32)
        for e in blocks(TOKENS):
            rows = pl.ds(e, BLOCK)
            d = dot(dx[rows], w2[chunk], 1, 1) * g[rows]
            bias = bias + jnp.sum(d, axis=0, keepdims=True)
            dpre[rows] = d.astype(BF)
            part = dot(dpre[rows], w1[:, chunk], 1, 1)

            @pl.when(r == 0)
            def _():
                acc[rows] = part

            @pl.when(r > 0)
            def _():
                acc[rows] = acc[rows] + part
        value[layer, pl.ds(BIAS_UP + r, 1)] = bias
        gw = dot(h2s[...], dpre[...], 0, 0)
        for i in range(QUAD):
            put(grads['up'], (i // PAIR, ALL, ALL, ALL, PAIR * r + i % PAIR), gw[:, lane(i)], (OCT, QUAD, PAIR))

    @pl.when(r == MLP_STEPS - 1)
    def _():
        load('x1', 0).wait()
        for e in blocks(TOKENS):
            rows = pl.ds(e, BLOCK)
            dh = acc[rows]
            xhat, rstd = normed(late[rows].astype(F32))
            d = dx[rows].astype(F32)
            dmid[rows] = (d + norm_back(dh, row(s, GAIN2), xhat, rstd)).astype(BF)
            add_sums((BIAS_DOWN, GAIN2, SHIFT2, BIAS_OUT), (d, dh * xhat, dh, dmid[rows].astype(F32)))

    @pl.when(r == MLP_STEPS)
    def _():
        load('wa', 0).wait()

    @pl.when(r >= MLP_STEPS)
    def _():
        e = r - MLP_STEPS
        rows = pl.ds(pl.multiple_of(lax.rem(e, SEQS) * SEQ, SEQ), SEQ)
        lanes = pl.ds(pl.multiple_of(lax.div(e, SEQS) * WIDE, WIDE), WIDE)
        qv, kv, vv = q[...], k[...], v[...]
        dc = dot(dmid[rows], wa[BIAS_OUT, lanes], 1, 1).astype(BF)
        qt, dct = qv.T, dc.T
        dq, dkt, dvt = 0, 0, 0
        for h in range(PAIR):
            m = half_mask((SEQ, WIDE), 1, h)
            mt = half_mask((WIDE, SEQ), 0, h)
            kh, vh = jnp.where(m, kv, 0), jnp.where(m, vv, 0)
            dvt = dvt + dot(jnp.where(mt, dct, 0), p[h])
            ds = []
            for b in blocks(SEQ):
                pf = p[h, pl.ds(b, BLOCK)].astype(F32)
                dp = dot(dc[b:b + BLOCK], vh, 1, 1)
                ds.append((pf * (dp - jnp.sum(dp * pf, axis=-1, keepdims=True))).astype(BF))
            ds = jnp.concatenate(ds, axis=0)
            dq = dq + dot(ds, kh)
            dkt = dkt + dot(jnp.where(mt, qt, 0), ds)
        cos, sin = cos_ref[...], sin_ref[...]
        dk = dkt.T
        dproj[0, rows, lanes] = ((dq * cos - swap_halves(dq) * sin) * (HEAD_DIM ** -0.5)).astype(BF)
        dproj[1, rows, lanes] = (dk * cos - swap_halves(dk) * sin).astype(BF)
        dproj[PAIR, rows, lanes] = dvt.T.astype(BF)

    for which in range(PAIR):
        @pl.when(r == MLP_STEPS + ATTN_STEPS // PAIR * (1 + which) - 1)
        def _():
            if which == 0:
                load('h1', 0).wait()
                load('ctx', 0).wait()
                gw_out = dot(late[...], dmid[...], 0, 0)
                for j in range(QUAD):
                    name, at = (('third', (1, ALL, ALL, ALL, j % PAIR)) if j >= PAIR else ('first', (1, 1, ALL, ALL, ALL, j)))
                    put(grads[name], at, gw_out[:, lane(j)], (OCT, QUAD, PAIR))
            cols = slice(BLOCK * which, BLOCK * which + BLOCK)
            for i in range(MATRICES - 1):
                gw = dot(h1s[...], dproj[i, :, cols], 0, 0)
                for j in range(PAIR):
                    name, at = (('second', 'third')[i % PAIR], (i // PAIR,)) if which else ('first', (i // PAIR, i % PAIR))
                    put(grads[name], at + (ALL, ALL, ALL, j), gw[:, lane(j)], (OCT, QUAD, PAIR))

    def advance(when, cond):
        for l in (1, 0):
            due = [gens[l, name] for (n, name), letters in SCHEDULE.items() if n == l and when in letters]
            if due:
                @pl.when(cond)
                def _():
                    for gen in due:
                        next(gen, 0)

    for step in range(STEPS):
        advance(chr(ord('A') + step), t == step)

    def result(i):
        e = pl.ds(i * BLOCK, BLOCK)
        return pltpu.make_async_copy(dx.at[e], d_x.at[e], fetched.at[len(loads) + i])

    @pl.when(r == LAYER_STEPS - 1)
    def _():
        load('xin', 0).wait()
        for i, e in enumerate(blocks(TOKENS)):
            rows = pl.ds(e, BLOCK)
            parts = [dproj[j, rows] for j in range(MATRICES - 1)]
            dh = sum(dot(part, wa[j], 1, 1) for j, part in enumerate(parts))
            xhat, rstd = normed(late[rows].astype(F32))
            add_sums((0, 1, PAIR, GAIN1, SHIFT1), [part.astype(F32) for part in parts] + [dh * xhat, dh])
            dx[rows] = (dmid[rows].astype(F32) + norm_back(dh, row(s, GAIN1), xhat, rstd)).astype(BF)
            advance('abcd'[i], layer == 0)

    @pl.when(t == STEPS - 1)
    def _():
        for i in range(QUAD):
            result(i).start()
        left = {name[0]: gens[0, name] for name, _, _ in SETS}
        left['m'] = total_unit(place, value, total, slots)
        for letter in ENDING:
            next(left[letter], 0)
        run(left.values())
        index = ((me['z'] * SIZES['y'] + me['y']) * SIZES['x'] + me['x']) * CORES + me['c']
        lanes = lax.broadcasted_iota(jnp.int32, (QUAD, DIM), 1)
        flat = lanes + DIM * lax.broadcasted_iota(jnp.int32, (QUAD, DIM), 0)
        for l in range(LAYERS):
            for i in range(PAIR):
                here = lanes == PAIR * index + i
                pick = lambda e: jnp.sum(jnp.where(here[:e.shape[0]], e, 0.0), axis=-1, keepdims=True)
                gb_attn[l, :, i:i + 1] = pick(total[l, :GAIN1])
                g_ln[l, :, i:i + 1] = pick(total[l, GAIN1:BIAS_UP])
                gb_down[l:l + 1, i:i + 1] = pick(total[l, BIAS_DOWN:BIAS_DOWN + 1])
            for i in range(OCT):
                e = jnp.where(flat == OCT * index + i, total[l, BIAS_UP:BIAS_DOWN], 0.0)
                gb_up[l:l + 1, i:i + 1] = jnp.sum(jnp.sum(e, axis=0, keepdims=True), axis=-1, keepdims=True)
        for i in range(QUAD):
            result(i).wait()


def backward(dy, saved, x0, y0, wts, s, cos, sin):
    h1, q, k, v, ctx, x1, p, h2, a, g = saved
    once = dict(pipeline_mode=pl.Buffered(1))
    layer = lambda t: 1 - lax.div(t, LAYER_STEPS)
    chunk = lambda t: jnp.minimum(lax.rem(t, LAYER_STEPS), CHUNKS - 1)
    head_of = lambda t: jnp.maximum(lax.rem(t, LAYER_STEPS) - MLP_STEPS, 0)
    seq = lambda t: lax.rem(head_of(t), SEQS)
    pair = lambda t: lax.div(head_of(t), SEQS)
    flat = lambda e: e.reshape(*e.shape[:-3], TOKENS, e.shape[-1])
    cols = pl.BlockSpec((None, TOKENS, CHUNK), lambda t: (layer(t), 0, chunk(t)))
    head = pl.BlockSpec((None, None, SEQ, WIDE), lambda t: (layer(t), seq(t), 0, pair(t)))
    late = [flat(e) for e in (h2, x1, h1, ctx, x0, y0)] + [w for pair_of in wts for w in pair_of]
    act, small = pltpu.VMEM((TOKENS, DIM), BF), pltpu.VMEM((LAYERS, SMALL, DIM), F32)
    bufs = [e for _, kind, _ in SETS for e in unit_buffers(kind, LAYERS)]
    shapes = [(LAYERS, MATRICES, PAIR, DIM), (LAYERS, PAIR, FFN), (LAYERS, OCT, DIM), (LAYERS, QUAD, PAIR), (LAYERS, QUAD, PAIR), (LAYERS, OCT), (LAYERS, PAIR)]
    return pl.pallas_call(
        backward_kernel, name='backward', grid=(STEPS,),
        in_specs=[whole((TOKENS, DIM), **once), cols, cols, head, head, head,
                  pl.BlockSpec((None, None, PAIR, SEQ, SEQ), lambda t: (layer(t), seq(t), pair(t), 0, 0)),
                  pl.BlockSpec((None, SMALL, DIM), lambda t: (layer(t), 0, 0)), whole((SEQ, WIDE), **once), whole((SEQ, WIDE), **once)] + any_space(len(late)),
        out_specs=any_space(1) + in_vmem(len(shapes)),
        out_shape=[SD((TOKENS, DIM), BF)] + [SD(e, F32) for e in shapes],
        scratch_shapes=[act, act, pltpu.VMEM((MATRICES - 1, TOKENS, DIM), BF), act, pltpu.VMEM((TOKENS, DIM), F32), small, small,
                        pltpu.VMEM((DIM, FFN), BF), pltpu.VMEM((FFN, DIM), BF), pltpu.VMEM((MATRICES, DIM, DIM), BF), act, act, act]
        + total_buffers() + bufs + [pltpu.SemaphoreType.REGULAR((PAIR * len(SETS),)), pltpu.SemaphoreType.DMA((SMALL,))] + semaphores(200),
        compiler_params=pltpu.CompilerParams(collective_id=SMALL, has_side_effects=True, vmem_limit_bytes=67043328),
    )(flat(dy), flat(a), flat(g), q, k, v, p, s, cos, sin, *late)


def solution(mesh):
    grid = Mesh(mesh.devices.reshape([SIZES[a] for a in AXES]), AXES)
    first, second, third = P(AXES), P(None, AXES), P(None, None, AXES)
    weight_specs = (third, third, third, second, second, second, second)

    def device_step(x, lengths, d_y, w_attn, b_attn, ln_par, w_up, b_up, w_down, b_down):
        full, small = gather(w_attn, w_up, w_down, b_attn, ln_par, b_up, b_down)
        cos, sin = (jnp.asarray(t) for t in rotary_tables())
        attn_saved, mlp_saved, y, wts = [], [], x, {}
        for layer in range(LAYERS):
            inner = y
            late = sorted({g[:2] for g in LATE[layer]})
            wts['attn', layer] = natural('attn', full['attn', layer])
            attn_saved, done = attn_fwd(layer, lengths, inner, wts['attn', layer], small, cos, sin, attn_saved, [full[e] for e in late])
            full.update(zip(late, done))
            for kind in ('up', 'down'):
                wts[kind, layer] = natural(kind, full[kind, layer])
            *mlp_saved, y = list(mlp_fwd(layer, attn_saved[5], wts['up', layer], wts['down', layer], small, mlp_saved)) + [x] * layer
        by_layer = [[wts[kind, layer] for layer in range(LAYERS)] for kind in ('up', 'down', 'attn')]
        d_x, *grads = backward(d_y, list(attn_saved) + mlp_saved, x, inner, by_layer, small, cos, sin)
        g_attn, g_up, g_down, gb_attn, g_ln, gb_up, gb_down = grads
        return d_x.reshape(x.shape), g_attn, gb_attn, g_ln, g_up, gb_up, g_down, gb_down

    return jax.shard_map(device_step, mesh=grid, in_specs=(first,) * 3 + weight_specs, out_specs=(first,) + weight_specs, check_vma=False)
```

```python
import math
import jax
import jax.numpy as jnp
import numpy as np
from jax import lax
from jax.experimental import pallas as pl
from jax.experimental.pallas import tpu as pltpu
from jax.sharding import Mesh, PartitionSpec as P

HEAD_DIM, EPS, THETA, NEG_BIG = 64, 1e-5, 10000.0, -1e30
SEQ, DIM, FFN, TOKENS, CHUNK, BLOCK, WIDE = 512, 512, 2048, 1024, 512, 256, 128
LAYERS = CORES = SEQS = PAIR = 2
MATRICES = CHUNKS = QUAD = 4
HEADS = OCT = 8
SMALL = 16
F32, BF = jnp.float32, jnp.bfloat16
SD = jax.ShapeDtypeStruct
AXES = ('z', 'y', 'x', 'c')
SIZES = dict(z=OCT, y=QUAD, x=QUAD, c=PAIR, k=PAIR, h=PAIR, l=PAIR, r=PAIR)
TILE = (OCT, WIDE)
ALL = slice(None)
BIAS_OUT, GAIN1, SHIFT1, GAIN2, SHIFT2, BIAS_UP, BIAS_DOWN = 3, 4, 5, 6, 7, 8, 12
TILED = dict(part='kzyht', slim='zyht', pair='zyht', up='zyht', down='zyxct')
FINE = dict(attn='kzyhtlcr', up='zyhtlcr', down='zyxct')
LANE_TILES = dict(attn=QUAD, part=PAIR, slim=PAIR, pair=PAIR, up=OCT, down=PAIR)
OWNER = dict(x='xhl', y='y', z='z')
UNITS = dict(up=('yzx', 'yzx'), down=('xyz', 'xyz'), part=('hyzl', 'hzyl'), slim=('yzx', 'yzx'), pair=('hyzl', 'hzyl'))
MLP_STEPS, ATTN_STEPS = CHUNKS, 8
LAYER_STEPS = MLP_STEPS + ATTN_STEPS
STEPS = LAYERS * LAYER_STEPS
SETS = (('up', 'up', ('t', PAIR, CHUNKS)), ('down', 'down', ('z', PAIR, CHUNKS)), ('first', 'part', ('z', OCT, 1)), ('second', 'slim', ('z', OCT, 1)), ('third', 'pair', ('z', OCT, 1)))
SCHEDULE = {(1, 'small'): 'MNOPST', (1, 'second'): 'LMQUXb', (1, 'third'): 'LMPTWac', (1, 'first'): 'HJNSUWX', (1, 'up'): 'ABCDEJNQU', (1, 'down'): 'ABCDEJMOP',
            (0, 'up'): 'MNOPQVb', (0, 'down'): 'MNOPQVXc', (0, 'first'): 'TVb', (0, 'second'): 'Xa', (0, 'third'): 'Xa'}
ENDING = 'lsdltufsldtsfltsftlft'
VM = 56 << 20


def spot(at):
    return dict(at, h=lax.div(at['x'], SIZES['l']), l=lax.rem(at['x'], SIZES['l']))


def only(at, names):
    return {n: at[n] for n in names if n in at}


def view(ref, names, pick):
    return ref.at[tuple(pick.get(n, ALL) for n in names)]


class Place:
    def __init__(self, send, recv):
        self.me = spot({a: lax.axis_index(a) for a in AXES})
        self.send, self.recv, self.used = send, recv, 0

    def shifted(self, axis, s):
        at = dict(self.me, **{axis: lax.rem(self.me[axis] + s, SIZES[axis])})
        if axis in 'hl':
            at['x'] = SIZES['l'] * at['h'] + at['l']
        return spot(at)

    def device(self, axis, s):
        at = self.shifted(axis, s)
        return tuple(at[a] for a in AXES)

    def peers(self, axis):
        n = SIZES[axis]
        return sorted(range(1, n), key=lambda s: min(s, n - s))

    def signal(self, sem, axis, s):
        pl.semaphore_signal(sem, inc=1, device_id=self.device(axis, s), device_id_type=pl.DeviceIdType.MESH)

    def greet(self):
        bar = pltpu.get_barrier_semaphore()
        everyone = [(a, s) for a in AXES for s in self.peers(a)]
        for a, s in everyone:
            self.signal(bar, a, s)
        pl.semaphore_wait(bar, len(everyone))

    def begin(self, build):
        self.used += 1
        assert self.used <= self.send.shape[0]
        build().start()
        return lambda: build().wait()

    def copy(self, axis, s, refs):
        i = self.used

        def build():
            src, dst = refs()
            return pltpu.make_async_remote_copy(src, dst, self.send.at[i], self.recv.at[i], device_id=self.device(axis, s), device_id_type=pl.DeviceIdType.MESH)
        return self.begin(build)

    def local(self, refs):
        i = self.used
        return self.begin(lambda: pltpu.make_async_copy(*refs(), self.send.at[i]))


def half(kind, core, part):
    if kind == 'attn':
        return dict(k=pl.ds(core * CORES + part, 1))
    return dict(t=pl.ds(core * LANE_TILES[kind], LANE_TILES[kind]))


def gathered(kind, full, part):
    names = FINE[kind]
    return lambda core, fixed, at: view(full, names, dict(half(kind, core(at), part), **only(at, fixed)))


def own(at):
    return at['c']


def other(at):
    return 1 - at['c']


def gather_early(place, kind, part, order, full, shard):
    block = gathered(kind, full, part)
    names = FINE[kind]
    mine = [n for n in names if n not in 'tkr']
    rows = [n for n in names if n in 'tk'] + ['r', 'r']

    def piece(core):
        return view(shard, rows, half(kind, core(place.me), part))
    waits = [place.local(lambda: (piece(own), block(own, mine, place.me))),
             place.copy('c', 1, lambda: (piece(other), block(other, mine, place.me)))]
    for i in range(len(order) - 1):
        yield
        for w in waits:
            w()
        fixed = ''.join(OWNER[a] for a in order[i:])
        waits = [place.copy(order[i], s, lambda: (block(own, fixed, place.me),) * PAIR) for s in place.peers(order[i])]
    yield
    for w in waits:
        w()


def gather_late(place, kind, part, order, full):
    block = gathered(kind, full, part)
    axis = order[-1]
    fixed = OWNER[axis]
    same = lambda at: (block(own, fixed, at),) * PAIR
    waits = [(s, place.copy(axis, s, lambda: same(place.me))) for s in place.peers(axis)]
    last = [place.copy('c', 1, lambda: same(place.me))]
    for s, w in waits:
        yield
        w()
        last.append(place.copy('c', 1, lambda s=s: same(place.shifted(axis, SIZES[axis] - s))))
    yield
    for w in last:
        w()


def gather_whole(*args):
    yield from gather_early(*args)
    yield from gather_late(*args[:-1])


def unravel(i, shape):
    idx = []
    for n in reversed(shape):
        idx.append(lax.rem(i, n))
        i = lax.div(i, n)
    return tuple(reversed(idx))


def each(shape, body):
    def step(i, carry):
        body(unravel(i, shape))
        return carry
    lax.fori_loop(0, math.prod(shape), step, 0)


def total_unit(place, value, out, slots):
    me = place.me
    keep, slot, *slots = slots
    wait = place.copy('c', 1, lambda: (value.at[other(me)], slot.at[0]))
    yield
    wait()
    keep[...] = value[me['c']] + slot[0]
    for axis, slot in zip('xyz', slots):
        last = SIZES[axis] - 1
        slot[last] = keep[...]
        waits = [place.copy(axis, s, lambda s=s: (slot.at[last], slot.at[s - 1])) for s in place.peers(axis)]
        yield
        for w in waits:
            w()
        v = slot[0]
        for s in range(1, SIZES[axis]):
            v = v + slot[s]
        keep[...] = v
    out[me['c']] = keep[...]
    wait = place.copy('c', 1, lambda: (keep, out.at[me['c']]))
    yield
    wait()


def total_buffers(n):
    return [pltpu.VMEM((n, DIM), F32)] + [pltpu.VMEM((SIZES[a], n, DIM), F32) for a in 'cxyz']


def run(units):
    units = list(units)
    while units:
        units = [u for u in units if next(u, units) is not units]


def free_sizes(kind, names):
    return tuple(LANE_TILES[kind] if n == 't' else SIZES[n] for n in names) + TILE


def plan(kind, layer=0):
    left = TILED[kind]
    for axis in UNITS[kind][layer]:
        d = axis if axis in left else 'h' if axis == 'x' else ''
        left = left.replace(d, '')
        yield axis, d, left


def unit_buffers(kind):
    _, _, first = next(plan(kind))
    shapes = [(PAIR,) + free_sizes(kind, TILED[kind]), free_sizes(kind, TILED[kind]), free_sizes(kind, first)]
    later = []
    for layer in range(LAYERS):
        slots = [(SIZES[axis] - 1,) + free_sizes(kind, left) for axis, _, left in plan(kind, layer)]
        *_, (_, _, left) = plan(kind, layer)
        later.append([pltpu.VMEM(s, F32) for s in slots[1:] + [free_sizes(kind, left.replace('c', ''))]])
    return [pltpu.VMEM(s, F32) for s in shapes + slots[:1]], later


def reduce_unit(place, kind, layer, bufs, finish, pieces, give, take):
    grad, got, first, slots, *rest = bufs
    me = place.me
    whole_grad, whole_names = grad, 'g' + TILED[kind]
    names, pick = whole_names, dict(g=me['c'])
    dim, size, count = pieces

    def cut(i):
        return {dim: pl.ds(size * i, size)}

    def accumulate(terms, fixed, into, piece=None):
        left = [n for n in names if n not in fixed]
        lead = left[:-3]
        sizes_of = dict(SIZES, t=LANE_TILES[kind])
        if piece is not None:
            sizes_of[dim] = size

        def body(idx):
            loop = dict(zip(lead, idx))
            if piece is not None:
                loop[dim] = loop[dim] + size * piece if dim in loop else pl.ds(size * piece, size)
            mine = tuple(fixed.get(n, loop.get(n, ALL)) for n in names)
            at = tuple(loop.get(n, ALL) for n in left)
            v = grad[mine]
            for ref in terms:
                v = v + ref[at]
            into[mine if into is grad else at] = v
        if lead:
            each([sizes_of[n] for n in lead], body)
        else:
            body(())

    (axis, d, left), *later = plan(kind, layer)
    arrived, waits = [], []

    def begin(i):
        if i == 0:
            take(1)
        arrived[i]()
        accumulate([got], pick, grad, i)
        for s in place.peers(axis):
            waits.append(place.copy(axis, s, lambda s=s: (view(whole_grad, whole_names, dict(only(place.shifted(axis, s), d), g=me['c'], **cut(i))),
                                                          view(slots, 's' + TILED[kind].replace(d, ''), dict(cut(i), s=s - 1)))))
    take(0)
    for i in range(count):
        arrived.append(place.copy('c', 1, lambda i=i: (view(whole_grad, whole_names, dict(cut(i), g=other(me))), view(got, TILED[kind], cut(i)))))
        if i:
            begin(i - 1)
        yield
    begin(count - 1)
    give(0)
    yield
    for w in waits:
        w()
    pick = dict(pick, **only(me, d))
    accumulate([slots.at[s] for s in range(SIZES[axis] - 1)], pick, first)
    give(1)
    grad, names, pick = first, left, {}
    for axis, d, left in later:
        slots, *rest = rest
        waits = [place.copy(axis, s, lambda s=s: (view(first, names, dict(pick, **only(place.shifted(axis, s), d))), slots.at[s - 1])) for s in place.peers(axis)]
        yield
        for w in waits:
            w()
        pick = dict(pick, **only(me, d))
        accumulate([slots.at[s] for s in range(SIZES[axis] - 1)], pick, first)
    away, = rest
    last = (lambda core: dict(pick, c=core(me))) if 'c' in left else (lambda core: pick)
    wait = place.copy('c', 1, lambda: (view(first, names, last(other)), away))
    yield
    wait()
    rows = ALL if kind == 'down' else pl.ds((me['l'] * PAIR + me['c']) * PAIR, PAIR)
    finish(own(me), first[tuple(last(own).get(n, ALL) for n in names) + (rows,)])
    finish(other(me), away[..., rows, :])


def blocks(n):
    return range(0, n, BLOCK)


def lane(i):
    return slice(WIDE * i, WIDE * i + WIDE)


def dot(a, b, ca=1, cb=0):
    return lax.dot_general(a, b, (((ca,), (cb,)), ((), ())), preferred_element_type=F32)


def rotary_tables():
    half_dim = HEAD_DIM // PAIR
    inv = (1.0 / (THETA ** (np.arange(half_dim, dtype=np.float32) * np.float32(2.0 / HEAD_DIM)))).astype(np.float32)
    ang = np.arange(SEQ, dtype=np.float32)[:, None] * inv[None, :]
    cos, sin = np.cos(ang), np.sin(ang)
    return np.tile(cos, (1, QUAD)), np.concatenate([-sin, sin] * PAIR, axis=1)


def swap_halves(t):
    n = HEAD_DIM // PAIR
    lanes = lax.broadcasted_iota(jnp.int32, t.shape, 1)
    return jnp.where(lax.rem(lanes, HEAD_DIM) < n, pltpu.roll(t, WIDE - n, 1), pltpu.roll(t, n, 1))


def normed(t):
    cent = t - jnp.mean(t, axis=-1, keepdims=True)
    rstd = lax.rsqrt(jnp.mean(cent * cent, axis=-1, keepdims=True) + EPS)
    return cent * rstd, rstd


def norm_back(dh, gain, xhat, rstd):
    dn = dh * gain
    return rstd * (dn - jnp.mean(dn, axis=-1, keepdims=True) - xhat * jnp.mean(dn * xhat, axis=-1, keepdims=True))


def row(ref, i):
    return ref[i:i + 1]


def half_mask(shape, axis, h):
    i = lax.broadcasted_iota(jnp.int32, shape, axis)
    return i >= HEAD_DIM if h else i < HEAD_DIM


def any_space(n):
    return [pl.BlockSpec(memory_space=pl.ANY)] * n


def in_vmem(n):
    return [pl.BlockSpec(memory_space=pltpu.VMEM)] * n


def semaphores(n):
    return [pltpu.SemaphoreType.DMA((n,))] * PAIR


def whole(shape, **kw):
    return pl.BlockSpec(shape, lambda *_: (0,) * len(shape), **kw)


def tiles_to_rows(t):
    *lead, r, n, s, w = t.shape
    return t.swapaxes(-3, -2).reshape(*lead, r * s, n * w)


def natural(kind, full):
    n = full.shape[FINE[kind].index('t')]
    lead = (MATRICES,) if kind == 'attn' else ()
    return tiles_to_rows(full.reshape(*lead, -1, n, *TILE))


def fine_shape(kind):
    n = LANE_TILES[kind] if kind == 'attn' else PAIR * LANE_TILES[kind]
    dims = dict(SIZES, t=n, k=MATRICES)
    return tuple(dims[d] for d in FINE[kind]) + ((WIDE,) if 'r' in FINE[kind] else TILE)


ATTN0, ATTN1 = ((('attn', l, 0, 'zxy'), ('attn', l, 1, 'zyx')) for l in range(LAYERS))
MLP0, MLP1 = ((('up', l, 0, 'zxy'), ('down', l, 0, 'zyx')) for l in range(LAYERS))
JOBS = dict(gather=[(gather_whole, g) for g in ATTN0] + [(gather_early, g) for g in MLP0 + ATTN1 + MLP1],
            attn0=[(gather_late, g) for g in MLP0 + ATTN1], attn1=[(gather_late, g) for g in MLP1])
HOST_STEPS = dict(attn0=((5, '0101'), (6, '01')), attn1=((5, '0101'), (6, '01')))
KINDS = tuple(FINE)


def keys(name):
    return sorted({g[:2] for _, g in JOBS[name]})


def units_of(name, place, full, shards):
    units = []
    for make, (kind, layer, part, order) in JOBS[name]:
        args = [place, kind, part, order, full[kind, layer]]
        units.append(make(*args) if make is gather_late else make(*args, shards[kind, layer]))
    return units


def host(name, place, t, full, shards):
    units = []

    @pl.when(t == 0)
    def _():
        place.greet()
        units.extend(units_of(name, place, full, shards))
        for u in units:
            next(u)

    def proceed():
        for step, digits in HOST_STEPS[name]:
            @pl.when(t == step)
            def _():
                for i in digits:
                    next(units[int(i)], 0)

        @pl.when(t == pl.num_programs(0) - 1)
        def _():
            run(units)
    return proceed


def gather_kernel(sa, su, sd, b_attn, ln, b_up, b_down, *refs):
    n = len(keys('gather'))
    full, total, value, slots, sems = refs[:n], refs[n], refs[n + 1], refs[n + 2:-2], refs[-2:]
    place = Place(*sems)
    place.greet()
    shards = {(kind, l): ref.at[l] for kind, ref in zip(KINDS, (sa, su, sd)) for l in range(LAYERS)}
    me = place.me
    index = ((me['z'] * SIZES['y'] + me['y']) * SIZES['x'] + me['x']) * CORES + me['c']

    def spread(v, rows):
        n = v.shape[1]
        at = lax.broadcasted_iota(jnp.int32, (rows, DIM), 1) - n * index
        if v.shape[0] < rows:
            at = at + DIM * lax.broadcasted_iota(jnp.int32, (rows, DIM), 0)
        return sum(jnp.where(at == i, v[:, i:i + 1], 0.0) for i in range(n))
    value[...] = jnp.zeros_like(value)
    shape = (PAIR, DIM)
    two = (lax.broadcasted_iota(jnp.int32, shape, 1) == PAIR * index + lax.broadcasted_iota(jnp.int32, shape, 0)).astype(F32).astype(BF)
    for l in range(LAYERS):
        value[l, :GAIN1] = dot(b_attn[l], two, 0, 0)
        value[l, GAIN1:BIAS_UP] = dot(ln[l], two, 0, 0)
        value[l, BIAS_UP:BIAS_DOWN] = spread(b_up[l:l + 1].astype(F32), QUAD)
        value[l, BIAS_DOWN:BIAS_DOWN + 1] = spread(b_down[l:l + 1].astype(F32), 1)
    units = units_of('gather', place, dict(zip(keys('gather'), full)), shards)
    units.insert(PAIR, total_unit(place, value, total, slots))
    run(units)


def tiled_shards(attn, up, down):
    return (attn.reshape(LAYERS, MATRICES, PAIR, -1, WIDE).swapaxes(-3, -2), up.reshape(LAYERS, PAIR, -1, WIDE).swapaxes(-3, -2),
            down.reshape(LAYERS, OCT, -1, WIDE).swapaxes(-3, -2))


def gather(shards, *small):
    names = keys('gather')
    *full, total = pl.pallas_call(
        gather_kernel, name='gather',
        in_specs=in_vmem(len(shards) + len(small)), out_specs=any_space(len(names)) + in_vmem(1),
        out_shape=[SD(fine_shape(k), BF) for k, _ in names] + [SD((LAYERS, SMALL, DIM), F32)],
        scratch_shapes=[pltpu.VMEM((LAYERS, SMALL, DIM), F32)] + total_buffers(SMALL) + semaphores(200),
        compiler_params=pltpu.CompilerParams(collective_id=1, has_side_effects=True),
    )(*shards, *small)
    return dict(zip(names, full)), total


def attn_fwd_kernel(name, len_ref, x_ref, w_ref, s_ref, cos_ref, sin_ref, *refs):
    h_ref, q_ref, k_ref, v_ref, ctx_ref, x1_ref, p_ref, *full = refs[:-2]
    t = pl.program_id(0)
    seq, j = lax.div(t, QUAD), lax.rem(t, QUAD)
    proceed = host(name, Place(*refs[-2:]), t, dict(zip(keys(name), full)), {})

    @pl.when(j == 0)
    def _():
        for r in blocks(SEQ):
            rows = pl.ds(r, BLOCK)
            xhat, _ = normed(x_ref[0, rows].astype(F32))
            h_ref[0, rows] = (xhat * row(s_ref, GAIN1) + row(s_ref, SHIFT1)).astype(BF)
            h = h_ref[0, rows]
            cos, sin = cos_ref[rows], sin_ref[rows]
            for c in blocks(DIM):
                cols = slice(c, c + BLOCK)
                for kind, dst in enumerate((q_ref, k_ref, v_ref)):
                    u = dot(h, w_ref[kind, :, cols]) + s_ref[kind:kind + 1, cols]
                    if dst is q_ref:
                        u = u * (HEAD_DIM ** -0.5)
                    for i in range(PAIR):
                        e = u[:, lane(i)]
                        if dst is not v_ref:
                            e = e * cos + swap_halves(e) * sin
                        dst[0, rows, c + WIDE * i:c + WIDE * i + WIDE] = e.astype(BF)

    valid = lax.broadcasted_iota(jnp.int32, (1, SEQ), 1) < len_ref[seq]
    lanes = pl.ds(pl.multiple_of(j * WIDE, WIDE), WIDE)
    masks = [half_mask((SEQ, WIDE), 1, h) for h in range(PAIR)]
    ks = [jnp.where(m, k_ref[0, :, lanes], 0) for m in masks]
    vs = [jnp.where(m, v_ref[0, :, lanes], 0) for m in masks]
    chains = [(r, h) for r in blocks(SEQ) for h in range(PAIR)]

    def score(r, h):
        return dot(q_ref[0, pl.ds(r, BLOCK), lanes], ks[h], 1, 1)
    ahead, ctx = score(*chains[0]), 0
    for i, (r, h) in enumerate(chains):
        s = jnp.where(valid, ahead, NEG_BIG)
        if i + 1 < len(chains):
            ahead = score(*chains[i + 1])
        e = jnp.exp(s - jnp.max(s, axis=-1, keepdims=True))
        p = (e * (1.0 / jnp.sum(e, axis=-1, keepdims=True))).astype(BF)
        p_ref[0, h, pl.ds(r, BLOCK)] = p
        ctx = ctx + dot(p, vs[h]) if h else dot(p, vs[h])
        if h:
            ctx_ref[0, pl.ds(r, BLOCK), lanes] = ctx.astype(BF)

    @pl.when(j == QUAD - 1)
    def _():
        for r in blocks(SEQ):
            rows = pl.ds(r, BLOCK)
            x1_ref[0, rows] = (x_ref[0, rows].astype(F32) + dot(ctx_ref[0, rows], w_ref[BIAS_OUT]) + row(s_ref, BIAS_OUT)).astype(BF)

    proceed()


def mlp_fwd_kernel(x_ref, w1_ref, w2_ref, s_ref, h_ref, a_ref, g_ref, *y_ref):
    x = x_ref[0].astype(F32)
    xhat, _ = normed(x)
    h = (xhat * row(s_ref, GAIN2) + row(s_ref, SHIFT2)).astype(BF)
    h_ref[0] = h
    acc = x + row(s_ref, BIAS_DOWN)
    for j in range(CHUNKS):
        cols = slice(CHUNK * j, CHUNK * j + CHUNK)
        pre = dot(h, w1_ref[:, cols]) + row(s_ref, BIAS_UP + j)
        z = pre * math.sqrt(0.5)
        cdf = 0.5 + 0.5 * lax.erf(z)
        g_ref[0, :, cols] = cdf + pre * math.sqrt(0.5 / math.pi) * jnp.exp2(z * z * -math.log2(math.e))
        a = (pre * cdf).astype(BF)
        a_ref[0, :, cols] = a
        if y_ref:
            acc = acc + dot(a, w2_ref[cols, :])
    for ref in y_ref:
        ref[0] = acc.astype(BF)


def layer_small(layer):
    return pl.BlockSpec((None, SMALL, DIM), lambda *_: (layer, 0, 0))


def attn_fwd(layer, lengths, x, w, s, cos, sin, prev, late):
    seq = lambda t: (lax.div(t, QUAD), 0, 0)
    t = pl.BlockSpec((1, SEQ, DIM), seq)
    saved = [pl.BlockSpec((None, 1, SEQ, DIM), lambda t: (layer,) + seq(t))] * 6
    saved.append(pl.BlockSpec((None, 1, PAIR, SEQ, SEQ), lambda t: (layer, lax.div(t, QUAD), lax.rem(t, QUAD), 0, 0)))
    inputs = [lengths, x, w, s, cos, sin]
    n, m = len(inputs), len(prev)
    res = pl.pallas_call(
        lambda *refs: attn_fwd_kernel('attn%d' % layer, *refs[:n], *refs[n + m + len(late):]), name='attn_fwd', grid=(OCT,),
        in_specs=[pl.BlockSpec(memory_space=pltpu.SMEM), t, whole((MATRICES, DIM, DIM)), layer_small(layer), whole((SEQ, WIDE)), whole((SEQ, WIDE))] + any_space(m + len(late)),
        out_specs=saved + any_space(len(late)),
        out_shape=[SD((LAYERS, SEQS, SEQ, DIM), BF)] * 6 + [SD((LAYERS, SEQS, HEADS, SEQ, SEQ), BF)] + [SD(e.shape, BF) for e in late],
        input_output_aliases=dict([(n + i, i) for i in range(m)] + [(n + m + i, len(saved) + i) for i in range(len(late))]),
        scratch_shapes=semaphores(40),
        compiler_params=pltpu.CompilerParams(collective_id=PAIR + layer, has_side_effects=True, vmem_limit_bytes=VM),
    )(*inputs, *prev, *late)
    return res[:len(saved)], res[len(saved):]


def mlp_fwd(layer, x1, w1, w2, s, prev):
    place = lambda t: (layer, lax.div(t, PAIR), lax.rem(t, PAIR), 0)
    block = lambda n: pl.BlockSpec((None, 1, BLOCK, n), place)
    widths = [(DIM, BF), (FFN, BF), (FFN, F32)]
    outs = [block(w) for w, _ in widths] + [pl.BlockSpec((1, BLOCK, DIM), lambda t: place(t)[1:])] * (1 - layer)
    inputs = [x1, w1, w2, s]
    n, m = len(inputs), len(prev)
    return pl.pallas_call(
        lambda *refs: mlp_fwd_kernel(*refs[:n], *refs[n + m:]), name='mlp_fwd', grid=(QUAD,),
        in_specs=[block(DIM), whole((DIM, FFN)), whole((FFN, DIM)), layer_small(layer)] + any_space(m), out_specs=outs,
        out_shape=[SD((LAYERS, SEQS, SEQ, w), d) for w, d in widths] + [SD((SEQS, SEQ, DIM), BF)] * (1 - layer),
        input_output_aliases={n + i: i for i in range(m)},
        compiler_params=pltpu.CompilerParams(vmem_limit_bytes=VM),
    )(*inputs, *prev)


def backward_kernel(dy, a, g, q, k, v, p, s, cos_ref, sin_ref, h2, x1, h1, ctx, x0, y0, w1_0, w1_1, w2_0, w2_1, wa_0, wa_1,
                    d_x, g_attn, g_up, g_down, gb_attn, g_ln, gb_up, gb_down, dx, dmid, dproj, dpre, acc, value, total, w1, w2, wa, h2s, h1s, late, *refs):
    credits, fetched, *sems = refs[-4:]
    t = pl.program_id(0)
    layer, r = 1 - lax.div(t, LAYER_STEPS), lax.rem(t, LAYER_STEPS)
    place = Place(*sems)
    me = place.me
    n = len(total_buffers(1))
    slots, last_slots, refs = refs[:n], refs[n:n + n], refs[n + n:-4]

    def finish_of(name, l):
        def finish(core, part):
            if name == 'down':
                for i in range(PAIR):
                    g_down[l, :, pl.ds(pl.multiple_of((PAIR * core + i) * WIDE, WIDE), WIDE)] = part[i]
            elif name == 'up':
                for i in range(OCT):
                    at = i // PAIR * QUAD + PAIR * core + i % PAIR
                    g_up[l, :, pl.ds(pl.multiple_of(at * WIDE, WIDE), WIDE)] = part[i]
            elif name == 'first':
                for i in range(QUAD):
                    g_attn[l, PAIR * core + i // PAIR, :, lane(i % PAIR)] = part[i // PAIR, i % PAIR]
            else:
                for i in range(PAIR):
                    g_attn[l, PAIR * core + (name == 'third'), :, lane(PAIR + i)] = part[i]
        return finish

    gens, grads = {(1, 'small'): total_unit(place, value.at[1], total.at[1], slots)}, {}
    for i, (name, kind, pieces) in enumerate(SETS):
        shared, refs = refs[:QUAD], refs[QUAD:]
        m = len(unit_buffers(kind)[1][0])
        later, refs = (refs[:m], refs[m:m + m]), refs[m + m:]
        grads[name] = shared[0]
        axis = UNITS[kind][0][0]
        groups = [[('c', 1)], [(axis, e) for e in place.peers(axis)]]

        def give(which, groups=groups, i=i):
            for e in groups[which]:
                place.signal(credits.at[PAIR * i + which], *e)

        def take(which, groups=groups, i=i):
            pl.semaphore_wait(credits.at[PAIR * i + which], len(groups[which]))
        nothing = lambda which: None
        for l in (1, 0):
            gens[l, name] = reduce_unit(place, kind, l, [*shared, *later[l]], finish_of(name, l), pieces, give if l else nothing, nothing if l else take)

    loads = dict(w2=(w2_0, w2_1, w2), w1=(w1_0, w1_1, w1), h2=(h2.at[0], h2.at[1], h2s), x1=(x1.at[0], x1.at[1], late), h1=(h1.at[0], h1.at[1], h1s),
                 wa=(wa_0, wa_1, wa), ctx=(ctx.at[0], ctx.at[1], late), xin=(x0, y0, late))
    starts = {(1, 'w2'): 'A', (1, 'w1'): 'A', (1, 'h2'): 'A', (1, 'x1'): 'A', (1, 'h1'): 'B', (1, 'wa'): 'B', (1, 'ctx'): 'E', (1, 'xin'): 'I',
              (0, 'w2'): 'E', (0, 'w1'): 'E', (0, 'h2'): 'E', (0, 'x1'): 'M', (0, 'h1'): 'M', (0, 'wa'): 'M', (0, 'ctx'): 'Q', (0, 'xin'): 'U'}

    def load(name, l):
        return pltpu.make_async_copy(loads[name][l], loads[name][-1], fetched.at[list(loads).index(name)])

    @pl.when(t == 0)
    def _():
        place.greet()
        dx[...] = dy[...]
        value[...] = jnp.zeros_like(value)

    for step in range(STEPS):
        due = [key for key, letter in starts.items() if ord(letter) - ord('A') == step]
        if due:
            @pl.when(t == step)
            def _():
                for l, name in due:
                    load(name, l).start()

    def put(ref, where, part, shape):
        ref[where] = part.reshape(shape + TILE)

    def add_sums(rows, terms):
        for i, e in zip(rows, terms):
            value[layer, i // OCT, i % OCT:i % OCT + 1] += jnp.sum(e, axis=0, keepdims=True)

    @pl.when(r == 0)
    def _():
        for name in ('w2', 'w1', 'h2'):
            load(name, 0).wait()

    @pl.when(r < MLP_STEPS)
    def _():
        gw = dot(a[...], dx[...], 0, 0)
        for i in range(QUAD):
            put(grads['down'], (i // PAIR, pl.ds(PAIR * r, PAIR), ALL, ALL, ALL, i % PAIR), gw[:, lane(i)], (PAIR, QUAD, QUAD, CORES))
        chunk = pl.ds(pl.multiple_of(r * CHUNK, CHUNK), CHUNK)
        bias = jnp.zeros((1, DIM), F32)
        for e in blocks(TOKENS):
            rows = pl.ds(e, BLOCK)
            d = dot(dx[rows], w2[chunk], 1, 1) * g[rows]
            bias = bias + jnp.sum(d, axis=0, keepdims=True)
            dpre[rows] = d.astype(BF)
            part = dot(dpre[rows], w1[:, chunk], 1, 1)

            @pl.when(r == 0)
            def _():
                acc[rows] = part

            @pl.when(r > 0)
            def _():
                acc[rows] = acc[rows] + part
        value[layer, 1, pl.ds(r, 1)] = bias
        gw = dot(h2s[...], dpre[...], 0, 0)
        for i in range(QUAD):
            put(grads['up'], (i // PAIR, ALL, ALL, ALL, PAIR * r + i % PAIR), gw[:, lane(i)], (OCT, QUAD, PAIR))

    @pl.when(r == MLP_STEPS - 1)
    def _():
        load('x1', 0).wait()
        for e in blocks(TOKENS):
            rows = pl.ds(e, BLOCK)
            dh = acc[rows]
            xhat, rstd = normed(late[rows].astype(F32))
            d = dx[rows].astype(F32)
            dmid[rows] = (d + norm_back(dh, row(s, GAIN2), xhat, rstd)).astype(BF)
            add_sums((BIAS_DOWN, GAIN2, SHIFT2, BIAS_OUT), (d, dh * xhat, dh, dmid[rows].astype(F32)))

    @pl.when(r == MLP_STEPS)
    def _():
        load('wa', 0).wait()

    @pl.when(r >= MLP_STEPS)
    def _():
        e = r - MLP_STEPS
        rows = pl.ds(pl.multiple_of(lax.rem(e, SEQS) * SEQ, SEQ), SEQ)
        lanes = pl.ds(pl.multiple_of(lax.div(e, SEQS) * WIDE, WIDE), WIDE)
        qv, kv, vv = q[...], k[...], v[...]
        dc = dot(dmid[rows], wa[BIAS_OUT, lanes], 1, 1).astype(BF)
        qt, dct = qv.T, dc.T
        dq, dkt, dvt = 0, 0, 0
        for h in range(PAIR):
            m = half_mask((SEQ, WIDE), 1, h)
            mt = half_mask((WIDE, SEQ), 0, h)
            kh, vh = jnp.where(m, kv, 0), jnp.where(m, vv, 0)
            dvt = dvt + dot(jnp.where(mt, dct, 0), p[h])
            ds = []
            for b in blocks(SEQ):
                pf = p[h, pl.ds(b, BLOCK)].astype(F32)
                dp = dot(dc[b:b + BLOCK], vh, 1, 1)
                ds.append((pf * (dp - jnp.sum(dp * pf, axis=-1, keepdims=True))).astype(BF))
            ds = jnp.concatenate(ds, axis=0)
            dq = dq + dot(ds, kh)
            dkt = dkt + dot(jnp.where(mt, qt, 0), ds)
        cos, sin = cos_ref[...], sin_ref[...]
        dk = dkt.T
        dproj[0, rows, lanes] = ((dq * cos - swap_halves(dq) * sin) * (HEAD_DIM ** -0.5)).astype(BF)
        dproj[1, rows, lanes] = (dk * cos - swap_halves(dk) * sin).astype(BF)
        dproj[PAIR, rows, lanes] = dvt.T.astype(BF)

    for which in range(PAIR):
        @pl.when(r == MLP_STEPS + ATTN_STEPS // PAIR * (1 + which) - 1)
        def _():
            if which == 0:
                load('h1', 0).wait()
                load('ctx', 0).wait()
                gw_out = dot(late[...], dmid[...], 0, 0)
                for j in range(QUAD):
                    name, at = (('third', (1, ALL, ALL, ALL, j % PAIR)) if j >= PAIR else ('first', (1, 1, ALL, ALL, ALL, j)))
                    put(grads[name], at, gw_out[:, lane(j)], (OCT, QUAD, PAIR))
            cols = slice(BLOCK * which, BLOCK * which + BLOCK)
            for i in range(MATRICES - 1):
                gw = dot(h1s[...], dproj[i, :, cols], 0, 0)
                for j in range(PAIR):
                    name, at = (('second', 'third')[i % PAIR], (i // PAIR,)) if which else ('first', (i // PAIR, i % PAIR))
                    put(grads[name], at + (ALL, ALL, ALL, j), gw[:, lane(j)], (OCT, QUAD, PAIR))

    def advance(when, cond):
        due = [gens[key] for key, letters in SCHEDULE.items() if when in letters]
        if due:
            @pl.when(cond)
            def _():
                for gen in due:
                    next(gen, 0)

    for step in range(STEPS):
        advance(chr(ord('A') + step), t == step)

    def result(i):
        e = pl.ds(i * BLOCK, BLOCK)
        return pltpu.make_async_copy(dx.at[e], d_x.at[e], fetched.at[len(loads) + i])

    @pl.when(r == LAYER_STEPS - 1)
    def _():
        load('xin', 0).wait()
        for i, e in enumerate(blocks(TOKENS)):
            rows = pl.ds(e, BLOCK)
            parts = [dproj[j, rows] for j in range(MATRICES - 1)]
            dh = sum(dot(part, wa[j], 1, 1) for j, part in enumerate(parts))
            xhat, rstd = normed(late[rows].astype(F32))
            add_sums((0, 1, PAIR, GAIN1, SHIFT1), [part.astype(F32) for part in parts] + [dh * xhat, dh])
            dx[rows] = (dmid[rows].astype(F32) + norm_back(dh, row(s, GAIN1), xhat, rstd)).astype(BF)
            advance('abcd'[i], layer == 0)

    @pl.when(t == STEPS - 1)
    def _():
        for i in range(QUAD):
            result(i).start()
        left = {name[0]: gens[0, name] for name, _, _ in SETS}
        left['l'] = total_unit(place, value.at[0], total.at[0], last_slots)
        for letter in ENDING:
            next(left[letter], 0)
        run(left.values())
        index = ((me['z'] * SIZES['y'] + me['y']) * SIZES['x'] + me['x']) * CORES + me['c']
        shape = (OCT, DIM)
        lanes, rows = lax.broadcasted_iota(jnp.int32, shape, 1), lax.broadcasted_iota(jnp.int32, shape, 0)
        diagonal = lax.broadcasted_iota(jnp.int32, (OCT, OCT), 0) == lax.broadcasted_iota(jnp.int32, (OCT, OCT), 1)

        def across(e):
            return jnp.sum(jnp.where(diagonal, jnp.sum(e, axis=-1, keepdims=True), 0.0), axis=0, keepdims=True)
        for l in range(LAYERS):
            for i in range(PAIR):
                here = lanes == PAIR * index + i
                e = across(jnp.where(here, total[l, 0], 0.0))
                gb_attn[l, i:i + 1], g_ln[l, i:i + 1] = e[:, :QUAD], e[:, QUAD:]
                gb_down[l:l + 1, i:i + 1] = across(jnp.where(here, total[l, 1], 0.0))[:, QUAD:QUAD + 1]
            gb_up[l:l + 1] = across(sum(jnp.where(lanes + DIM * n == OCT * index + rows, total[l, 1, n:n + 1], 0.0) for n in range(QUAD)))
        for i in range(QUAD):
            result(i).wait()


def backward(dy, saved, x0, y0, wts, s, cos, sin):
    h1, q, k, v, ctx, x1, p, h2, a, g = saved
    once = dict(pipeline_mode=pl.Buffered(1))
    layer = lambda t: 1 - lax.div(t, LAYER_STEPS)
    chunk = lambda t: jnp.minimum(lax.rem(t, LAYER_STEPS), CHUNKS - 1)
    head_of = lambda t: jnp.maximum(lax.rem(t, LAYER_STEPS) - MLP_STEPS, 0)
    seq = lambda t: lax.rem(head_of(t), SEQS)
    pair = lambda t: lax.div(head_of(t), SEQS)
    flat = lambda e: e.reshape(*e.shape[:-3], TOKENS, e.shape[-1])
    cols = pl.BlockSpec((None, TOKENS, CHUNK), lambda t: (layer(t), 0, chunk(t)))
    head = pl.BlockSpec((None, None, SEQ, WIDE), lambda t: (layer(t), seq(t), 0, pair(t)))
    late = [flat(e) for e in (h2, x1, h1, ctx, x0, y0)] + [w for pair_of in wts for w in pair_of]
    act, small = pltpu.VMEM((TOKENS, DIM), BF), pltpu.VMEM((LAYERS, CORES, OCT, DIM), F32)
    bufs = [e for _, kind, _ in SETS for group in (unit_buffers(kind)[0], *unit_buffers(kind)[1]) for e in group]
    shapes = [(LAYERS, MATRICES, PAIR, DIM), (LAYERS, PAIR, FFN), (LAYERS, OCT, DIM), (LAYERS, PAIR, QUAD), (LAYERS, PAIR, QUAD), (LAYERS, OCT), (LAYERS, PAIR)]
    return pl.pallas_call(
        backward_kernel, name='backward', grid=(STEPS,),
        in_specs=[whole((TOKENS, DIM), **once), cols, cols, head, head, head,
                  pl.BlockSpec((None, None, PAIR, SEQ, SEQ), lambda t: (layer(t), seq(t), pair(t), 0, 0)),
                  pl.BlockSpec((None, SMALL, DIM), lambda t: (layer(t), 0, 0)), whole((SEQ, WIDE), **once), whole((SEQ, WIDE), **once)] + any_space(len(late)),
        out_specs=any_space(1) + in_vmem(len(shapes)),
        out_shape=[SD((TOKENS, DIM), BF)] + [SD(e, F32) for e in shapes],
        scratch_shapes=[act, act, pltpu.VMEM((MATRICES - 1, TOKENS, DIM), BF), act, pltpu.VMEM((TOKENS, DIM), F32), small, small,
                        pltpu.VMEM((DIM, FFN), BF), pltpu.VMEM((FFN, DIM), BF), pltpu.VMEM((MATRICES, DIM, DIM), BF), act, act, act]
        + total_buffers(OCT) * LAYERS + bufs + [pltpu.SemaphoreType.REGULAR((PAIR * len(SETS),)), pltpu.SemaphoreType.DMA((SMALL,))] + semaphores(240),
        compiler_params=pltpu.CompilerParams(collective_id=SMALL, has_side_effects=True, vmem_limit_bytes=67043328),
    )(flat(dy), flat(a), flat(g), q, k, v, p, s, cos, sin, *late)


def deliver(*results):
    n = len(results)

    def body(*refs):
        for src, dst in zip(refs[:n], refs[n:]):
            dst[...] = src[...]
    return pl.pallas_call(body, name='deliver', in_specs=in_vmem(n), out_specs=in_vmem(n), out_shape=[SD(e.shape, e.dtype) for e in results])(*results)


def solution(mesh):
    grid = Mesh(mesh.devices.reshape([SIZES[a] for a in AXES]), AXES)
    first, second, third = P(AXES), P(None, AXES), P(None, None, AXES)
    weight_specs = (third, third, third, second, second, second, second)

    def device_step(x, lengths, d_y, w_attn, b_attn, ln_par, w_up, b_up, w_down, b_down):
        shards = tiled_shards(w_attn, w_up, w_down)
        full, small = gather(shards, b_attn.swapaxes(1, PAIR), ln_par.swapaxes(1, PAIR), b_up, b_down)
        cos, sin = (jnp.asarray(t) for t in rotary_tables())
        attn_saved, mlp_saved, y, wts = [], [], x, {}
        for layer in range(LAYERS):
            inner = y
            late = keys('attn%d' % layer)
            wts['attn', layer] = natural('attn', full['attn', layer])
            attn_saved, done = attn_fwd(layer, lengths, inner, wts['attn', layer], small, cos, sin, attn_saved, [full[e] for e in late])
            full.update(zip(late, done))
            for kind in ('up', 'down'):
                wts[kind, layer] = natural(kind, full[kind, layer])
            *mlp_saved, y = list(mlp_fwd(layer, attn_saved[5], wts['up', layer], wts['down', layer], small, mlp_saved)) + [x] * layer
        by_layer = [[wts[kind, layer] for layer in range(LAYERS)] for kind in ('up', 'down', 'attn')]
        d_x, *grads = backward(d_y, list(attn_saved) + mlp_saved, x, inner, by_layer, small, cos, sin)
        d_x, g_attn, g_up, g_down, gb_attn, g_ln, gb_up, gb_down = deliver(d_x, *grads)
        return d_x.reshape(x.shape), g_attn, gb_attn.swapaxes(1, PAIR), g_ln.swapaxes(1, PAIR), g_up, gb_up, g_down, gb_down

    return jax.shard_map(device_step, mesh=grid, in_specs=(first,) * 3 + weight_specs, out_specs=(first,) + weight_specs, check_vma=False)
```

```python
import math
import jax
import jax.numpy as jnp
import numpy as np
from jax import lax
from jax.experimental import pallas as pl
from jax.experimental.pallas import tpu as pltpu
from jax.sharding import Mesh, PartitionSpec as P

HEAD_DIM, EPS, THETA, NEG_BIG = 64, 1e-5, 10000.0, -1e30
SEQ, DIM, FFN, TOKENS, CHUNK, BLOCK, WIDE = 512, 512, 2048, 1024, 512, 256, 128
LAYERS = CORES = SEQS = PAIR = 2
MATRICES = CHUNKS = QUAD = 4
HEADS = OCT = 8
SMALL = 16
F32, BF = jnp.float32, jnp.bfloat16
SD = jax.ShapeDtypeStruct
AXES = ('z', 'y', 'x', 'c')
SIZES = dict(z=OCT, y=QUAD, x=QUAD, c=PAIR, k=PAIR, h=PAIR, l=PAIR, r=PAIR)
TILE = (OCT, WIDE)
ALL = slice(None)
BIAS_OUT, GAIN1, SHIFT1, GAIN2, SHIFT2, BIAS_UP, BIAS_DOWN = 3, 4, 5, 6, 7, 8, 12
TILED = dict(part='kzyht', slim='zyht', pair='zyht', up='zyht', down='zyxct')
FINE = dict(attn='kzyhtlcr', up='zyhtlcr', down='zyxct')
LANE_TILES = dict(attn=QUAD, part=PAIR, slim=PAIR, pair=PAIR, up=OCT, down=PAIR)
OWNER = dict(x='xhl', y='y', z='z')
UNITS = dict(up=('yzx', 'yzx'), down=('xyz', 'xyz'), part=('hyzl', 'hzyl'), slim=('yzx', 'yzx'), pair=('hyzl', 'hzyl'))
MLP_STEPS, ATTN_STEPS = CHUNKS, 8
LAYER_STEPS = MLP_STEPS + ATTN_STEPS
STEPS = LAYERS * LAYER_STEPS
SETS = (('up', 'up', ('t', PAIR, CHUNKS)), ('down', 'down', ('z', PAIR, CHUNKS)), ('first', 'part', ('z', OCT, 1)), ('second', 'slim', ('z', OCT, 1)), ('third', 'pair', ('z', OCT, 1)))
SCHEDULE = {(1, 'small'): 'MNOPTU', (1, 'second'): 'LMQUb', (1, 'third'): 'LMPUXd', (1, 'first'): 'HJNSUX', (1, 'up'): 'ABCDEJNU', (1, 'down'): 'ABCDEJMOP',
            (0, 'up'): 'MNOPQV', (0, 'down'): 'MNOPQVa', (0, 'first'): 'TV', (0, 'second'): 'Xa', (0, 'third'): 'Xa'}
ENDING = 'lulsftldtusfltdsftlftl'
VM = 56 << 20


def spot(at):
    return dict(at, h=lax.div(at['x'], SIZES['l']), l=lax.rem(at['x'], SIZES['l']))


def only(at, names):
    return {n: at[n] for n in names if n in at}


def view(ref, names, pick):
    return ref.at[tuple(pick.get(n, ALL) for n in names)]


class Place:
    def __init__(self, send, recv):
        self.me = spot({a: lax.axis_index(a) for a in AXES})
        self.send, self.recv, self.used = send, recv, 0

    def shifted(self, axis, s):
        at = dict(self.me, **{axis: lax.rem(self.me[axis] + s, SIZES[axis])})
        if axis in 'hl':
            at['x'] = SIZES['l'] * at['h'] + at['l']
        return spot(at)

    def device(self, axis, s, core=0):
        at = self.shifted(axis, s)
        if core:
            at['c'] = other(at)
        return tuple(at[a] for a in AXES)

    def peers(self, axis):
        n = SIZES[axis]
        return sorted(range(1, n), key=lambda s: min(s, n - s))

    def signal(self, sem, *to):
        pl.semaphore_signal(sem, inc=1, device_id=self.device(*to), device_id_type=pl.DeviceIdType.MESH)

    def hello(self, partners=()):
        everyone = [(a, s, 0) for a in AXES for s in self.peers(a)] + [(a, s, 1) for a in partners for s in self.peers(a)]
        for e in everyone:
            self.signal(pltpu.get_barrier_semaphore(), *e)
        return len(everyone)

    def greet(self, said=None):
        n = self.hello() if said is None else said
        pl.semaphore_wait(pltpu.get_barrier_semaphore(), n)

    def begin(self, build):
        self.used += 1
        assert self.used <= self.send.shape[0]
        build().start()
        return lambda: build().wait()

    def copy(self, axis, s, refs, core=0):
        i = self.used

        def build():
            src, dst = refs()
            return pltpu.make_async_remote_copy(src, dst, self.send.at[i], self.recv.at[i], device_id=self.device(axis, s, core), device_id_type=pl.DeviceIdType.MESH)
        return self.begin(build)

    def local(self, refs):
        i = self.used
        return self.begin(lambda: pltpu.make_async_copy(*refs(), self.send.at[i]))


def half(kind, core, part):
    if kind == 'attn':
        return dict(k=pl.ds(core * CORES + part, 1))
    return dict(t=pl.ds(core * LANE_TILES[kind], LANE_TILES[kind]))


def gathered(kind, full, part):
    names = FINE[kind]
    return lambda core, fixed, at: view(full, names, dict(half(kind, core(at), part), **only(at, fixed)))


def own(at):
    return at['c']


def other(at):
    return 1 - at['c']


def gather_early(place, kind, part, order, full, shard):
    block = gathered(kind, full, part)
    names = FINE[kind]
    mine = [n for n in names if n not in 'tkr']
    rows = [n for n in names if n in 'tk'] + ['r', 'r']

    def piece(core):
        return view(shard, rows, half(kind, core(place.me), part))
    waits = [place.local(lambda: (piece(own), block(own, mine, place.me))),
             place.copy('c', 1, lambda: (piece(other), block(other, mine, place.me)))]
    for i in range(len(order) - 1):
        yield
        for w in waits:
            w()
        fixed = ''.join(OWNER[a] for a in order[i:])
        waits = [place.copy(order[i], s, lambda: (block(own, fixed, place.me),) * PAIR) for s in place.peers(order[i])]
    yield
    for w in waits:
        w()


def gather_late(place, kind, part, order, full):
    block = gathered(kind, full, part)
    axis = order[-1]
    fixed = OWNER[axis]
    same = lambda at: (block(own, fixed, at),) * PAIR
    waits = [(s, place.copy(axis, s, lambda: same(place.me))) for s in place.peers(axis)]
    last = [place.copy('c', 1, lambda: same(place.me))]
    for s, w in waits:
        yield
        w()
        last.append(place.copy('c', 1, lambda s=s: same(place.shifted(axis, SIZES[axis] - s))))
    yield
    for w in last:
        w()


def gather_whole(*args):
    yield from gather_early(*args)
    yield from gather_late(*args[:-1])


def unravel(i, shape):
    idx = []
    for n in reversed(shape):
        idx.append(lax.rem(i, n))
        i = lax.div(i, n)
    return tuple(reversed(idx))


def each(shape, body):
    def step(i, carry):
        body(unravel(i, shape))
        return carry
    lax.fori_loop(0, math.prod(shape), step, 0)


def total_unit(place, value, out, slots, axes='xyz'):
    me = place.me
    keep, slot, *slots = slots
    wait = place.copy('c', 1, lambda: (value.at[other(me)], slot.at[0]))
    yield
    wait()
    keep[...] = value[me['c']] + slot[0]
    for axis, slot in zip(axes, slots):
        last = SIZES[axis] - 1
        slot[last] = keep[...]
        waits = [place.copy(axis, s, lambda s=s: (slot.at[last], slot.at[s - 1])) for s in place.peers(axis)]
        yield
        for w in waits:
            w()
        v = slot[0]
        for s in range(1, SIZES[axis]):
            v = v + slot[s]
        keep[...] = v
    out[me['c']] = keep[...]
    wait = place.copy('c', 1, lambda: (keep, out.at[me['c']]))
    yield
    wait()


def total_buffers(n):
    return [pltpu.VMEM((n, DIM), F32)] + [pltpu.VMEM((OCT, n, DIM), F32)] * QUAD


def run(units):
    units = list(units)
    while units:
        units = [u for u in units if next(u, units) is not units]


def free_sizes(kind, names):
    return tuple(LANE_TILES[kind] if n == 't' else SIZES[n] for n in names) + TILE


def plan(kind, layer=0):
    left = TILED[kind]
    for axis in UNITS[kind][layer]:
        d = axis if axis in left else 'h' if axis == 'x' else ''
        left = left.replace(d, '')
        yield axis, d, left


def unit_buffers(kind):
    _, _, first = next(plan(kind))
    shapes = [(PAIR,) + free_sizes(kind, TILED[kind]), free_sizes(kind, TILED[kind]), free_sizes(kind, first)]
    later = []
    for layer in range(LAYERS):
        slots = [(SIZES[axis] - 1,) + free_sizes(kind, left) for axis, _, left in plan(kind, layer)]
        *_, (axis, _, left) = plan(kind, layer)
        if kind == 'down':
            slots.append(free_sizes(kind, left.replace('c', '')))
        else:
            slots[-1] = (PAIR * SIZES[axis],) + free_sizes(kind, left)
        later.append([pltpu.VMEM(s, F32) for s in slots[1:]])
    return [pltpu.VMEM(s, F32) for s in shapes + slots[:1]], later


def reduce_unit(place, kind, layer, bufs, finish, pieces, give, take):
    grad, got, first, slots, *rest = bufs
    me = place.me
    whole_grad, whole_names = grad, 'g' + TILED[kind]
    names, pick = whole_names, dict(g=me['c'])
    dim, size, count = pieces

    def cut(i):
        return {dim: pl.ds(size * i, size)}

    def accumulate(terms, fixed, into, piece=None):
        left = [n for n in names if n not in fixed]
        lead = left[:-3]
        sizes_of = dict(SIZES, t=LANE_TILES[kind])
        if piece is not None:
            sizes_of[dim] = size

        def body(idx):
            loop = dict(zip(lead, idx))
            if piece is not None:
                loop[dim] = loop[dim] + size * piece if dim in loop else pl.ds(size * piece, size)
            mine = tuple(fixed.get(n, loop.get(n, ALL)) for n in names)
            at = tuple(loop.get(n, ALL) for n in left)
            v = grad[mine]
            for ref in terms:
                v = v + ref[at]
            into[mine if into is grad else at] = v
        if lead:
            each([sizes_of[n] for n in lead], body)
        else:
            body(())

    (axis, d, left), *later = plan(kind, layer)
    arrived, waits = [], []

    def begin(i):
        if i == 0:
            take(1)
        arrived[i]()
        accumulate([got], pick, grad, i)
        for s in place.peers(axis):
            waits.append(place.copy(axis, s, lambda s=s: (view(whole_grad, whole_names, dict(only(place.shifted(axis, s), d), g=me['c'], **cut(i))),
                                                          view(slots, 's' + TILED[kind].replace(d, ''), dict(cut(i), s=s - 1)))))
    take(0)
    for i in range(count):
        arrived.append(place.copy('c', 1, lambda i=i: (view(whole_grad, whole_names, dict(cut(i), g=other(me))), view(got, TILED[kind], cut(i)))))
        if i:
            begin(i - 1)
        yield
    begin(count - 1)
    give(0)
    yield
    for w in waits:
        w()
    pick = dict(pick, **only(me, d))
    accumulate([slots.at[s] for s in range(SIZES[axis] - 1)], pick, first)
    give(1)
    grad, names, pick = first, left, {}
    for axis, d, left in later:
        slots, *rest = rest
        if not rest:
            far = [(s, core) for s in range(SIZES[axis]) for core in range(CORES) if s or core]
            waits = [place.copy(axis, s, lambda s=s, core=core: (view(first, names, dict(pick, **only(place.shifted(axis, s), d))), slots.at[PAIR * s + core]), core) for s, core in far]
            yield
            for w in waits:
                w()
            pick = dict(pick, **only(me, d))
            rows = pl.ds((me['l'] * PAIR + me['c']) * PAIR, PAIR)
            mine, away = first[tuple(pick.get(n, ALL) for n in names) + (rows,)], 0
            for s in range(SIZES[axis]):
                mine = mine + slots.at[PAIR * s][..., rows, :] if s else mine
                away = away + slots.at[PAIR * s + 1][..., rows, :]
            finish(own(me), mine)
            finish(other(me), away)
            return
        waits = [place.copy(axis, s, lambda s=s: (view(first, names, dict(pick, **only(place.shifted(axis, s), d))), slots.at[s - 1])) for s in place.peers(axis)]
        yield
        for w in waits:
            w()
        pick = dict(pick, **only(me, d))
        accumulate([slots.at[s] for s in range(SIZES[axis] - 1)], pick, first)
    away, = rest
    last = lambda core: dict(pick, c=core(me))
    wait = place.copy('c', 1, lambda: (view(first, names, last(other)), away))
    yield
    wait()
    finish(own(me), first[tuple(last(own).get(n, ALL) for n in names)])
    finish(other(me), away[...])


def blocks(n):
    return range(0, n, BLOCK)


def lane(i):
    return slice(WIDE * i, WIDE * i + WIDE)


def dot(a, b, ca=1, cb=0):
    return lax.dot_general(a, b, (((ca,), (cb,)), ((), ())), preferred_element_type=F32)


def rotary_tables():
    half_dim = HEAD_DIM // PAIR
    inv = (1.0 / (THETA ** (np.arange(half_dim, dtype=np.float32) * np.float32(2.0 / HEAD_DIM)))).astype(np.float32)
    ang = np.arange(SEQ, dtype=np.float32)[:, None] * inv[None, :]
    cos, sin = np.cos(ang), np.sin(ang)
    return np.tile(cos, (1, QUAD)), np.concatenate([-sin, sin] * PAIR, axis=1)


def swap_halves(t):
    n = HEAD_DIM // PAIR
    lanes = lax.broadcasted_iota(jnp.int32, t.shape, 1)
    return jnp.where(lax.rem(lanes, HEAD_DIM) < n, pltpu.roll(t, WIDE - n, 1), pltpu.roll(t, n, 1))


def normed(t):
    cent = t - jnp.mean(t, axis=-1, keepdims=True)
    rstd = lax.rsqrt(jnp.mean(cent * cent, axis=-1, keepdims=True) + EPS)
    return cent * rstd, rstd


def norm_back(dh, gain, xhat, rstd):
    dn = dh * gain
    return rstd * (dn - jnp.mean(dn, axis=-1, keepdims=True) - xhat * jnp.mean(dn * xhat, axis=-1, keepdims=True))


def row(ref, i):
    return ref[i:i + 1]


def half_mask(shape, axis, h):
    i = lax.broadcasted_iota(jnp.int32, shape, axis)
    return i >= HEAD_DIM if h else i < HEAD_DIM


def any_space(n):
    return [pl.BlockSpec(memory_space=pl.ANY)] * n


def in_vmem(n):
    return [pl.BlockSpec(memory_space=pltpu.VMEM)] * n


def semaphores(n):
    return [pltpu.SemaphoreType.DMA((n,))] * PAIR


def whole(shape, **kw):
    return pl.BlockSpec(shape, lambda *_: (0,) * len(shape), **kw)


def tiles_to_rows(t):
    *lead, r, n, s, w = t.shape
    return t.swapaxes(-3, -2).reshape(*lead, r * s, n * w)


def natural(kind, full):
    n = full.shape[FINE[kind].index('t')]
    lead = (MATRICES,) if kind == 'attn' else ()
    return tiles_to_rows(full.reshape(*lead, -1, n, *TILE))


def fine_shape(kind):
    n = LANE_TILES[kind] if kind == 'attn' else PAIR * LANE_TILES[kind]
    dims = dict(SIZES, t=n, k=MATRICES)
    return tuple(dims[d] for d in FINE[kind]) + ((WIDE,) if 'r' in FINE[kind] else TILE)


ATTN0, ATTN1 = ((('attn', l, 0, 'zxy'), ('attn', l, 1, 'zyx')) for l in range(LAYERS))
MLP0, MLP1 = ((('up', l, 0, 'zxy'), ('down', l, 0, 'zyx')) for l in range(LAYERS))
JOBS = dict(gather=[(gather_whole, g) for g in ATTN0] + [(gather_early, g) for g in MLP0 + ATTN1 + MLP1],
            attn0=[(gather_late, g) for g in MLP0 + ATTN1], attn1=[(gather_late, g) for g in MLP1])
HOST_STEPS = dict(attn0=((5, '0101'), (6, '01')), attn1=((5, '0101'), (6, '01')))
KINDS = tuple(FINE)


def keys(name):
    return sorted({g[:2] for _, g in JOBS[name]})


def units_of(name, place, full, shards):
    units = []
    for make, (kind, layer, part, order) in JOBS[name]:
        args = [place, kind, part, order, full[kind, layer]]
        units.append(make(*args) if make is gather_late else make(*args, shards[kind, layer]))
    return units


def host(name, place, t, full, shards):
    units, said = [], []

    @pl.when(t == 0)
    def _():
        said.append(place.hello())

    def start():
        place.greet(*said)
        units.extend(units_of(name, place, full, shards))
        for u in units:
            next(u)

    def proceed():
        for step, digits in HOST_STEPS[name]:
            @pl.when(t == step)
            def _():
                for i in digits:
                    next(units[int(i)], 0)

        @pl.when(t == pl.num_programs(0) - 1)
        def _():
            run(units)
    return start, proceed


def gather_kernel(sa, su, sd, b_attn, ln, b_up, b_down, *refs):
    n = len(keys('gather'))
    full, total, value, slots, sems = refs[:n], refs[n], refs[n + 1], refs[n + 2:-2], refs[-2:]
    place = Place(*sems)
    place.greet()
    shards = {(kind, l): ref.at[l] for kind, ref in zip(KINDS, (sa, su, sd)) for l in range(LAYERS)}
    me = place.me
    index = ((me['z'] * SIZES['y'] + me['y']) * SIZES['x'] + me['x']) * CORES + me['c']

    def spread(v, rows):
        n = v.shape[1]
        at = lax.broadcasted_iota(jnp.int32, (rows, DIM), 1) - n * index
        if v.shape[0] < rows:
            at = at + DIM * lax.broadcasted_iota(jnp.int32, (rows, DIM), 0)
        return sum(jnp.where(at == i, v[:, i:i + 1], 0.0) for i in range(n))
    value[...] = jnp.zeros_like(value)
    shape = (PAIR, DIM)
    two = (lax.broadcasted_iota(jnp.int32, shape, 1) == PAIR * index + lax.broadcasted_iota(jnp.int32, shape, 0)).astype(F32).astype(BF)
    for l in range(LAYERS):
        value[l, :GAIN1] = dot(b_attn[l], two, 0, 0)
        value[l, GAIN1:BIAS_UP] = dot(ln[l], two, 0, 0)
        value[l, BIAS_UP:BIAS_DOWN] = spread(b_up[l:l + 1].astype(F32), QUAD)
        value[l, BIAS_DOWN:BIAS_DOWN + 1] = spread(b_down[l:l + 1].astype(F32), 1)
    units = units_of('gather', place, dict(zip(keys('gather'), full)), shards)
    units.insert(PAIR, total_unit(place, value, total, slots))
    run(units)


def tiled_shards(attn, up, down):
    return (attn.reshape(LAYERS, MATRICES, PAIR, -1, WIDE).swapaxes(-3, -2), up.reshape(LAYERS, PAIR, -1, WIDE).swapaxes(-3, -2),
            down.reshape(LAYERS, OCT, -1, WIDE).swapaxes(-3, -2))


def gather(shards, *small):
    names = keys('gather')
    *full, total = pl.pallas_call(
        gather_kernel, name='gather',
        in_specs=in_vmem(len(shards) + len(small)), out_specs=any_space(len(names)) + in_vmem(1),
        out_shape=[SD(fine_shape(k), BF) for k, _ in names] + [SD((LAYERS, SMALL, DIM), F32)],
        scratch_shapes=[pltpu.VMEM((LAYERS, SMALL, DIM), F32)] + total_buffers(SMALL) + semaphores(200),
        compiler_params=pltpu.CompilerParams(collective_id=1, has_side_effects=True),
    )(*shards, *small)
    return dict(zip(names, full)), total


def attn_fwd_kernel(name, len_ref, x_ref, w_ref, s_ref, cos_ref, sin_ref, *refs):
    h_ref, q_ref, k_ref, v_ref, ctx_ref, x1_ref, p_ref, *full = refs[:-2]
    t = pl.program_id(0)
    seq, j = lax.div(t, QUAD), lax.rem(t, QUAD)
    start, proceed = host(name, Place(*refs[-2:]), t, dict(zip(keys(name), full)), {})

    @pl.when(j == 0)
    def _():
        for r in blocks(SEQ):
            rows = pl.ds(r, BLOCK)
            xhat, _ = normed(x_ref[0, rows].astype(F32))
            h_ref[0, rows] = (xhat * row(s_ref, GAIN1) + row(s_ref, SHIFT1)).astype(BF)
            h = h_ref[0, rows]
            cos, sin = cos_ref[rows], sin_ref[rows]
            for c in blocks(DIM):
                cols = slice(c, c + BLOCK)
                for kind, dst in enumerate((q_ref, k_ref, v_ref)):
                    u = dot(h, w_ref[kind, :, cols]) + s_ref[kind:kind + 1, cols]
                    if dst is q_ref:
                        u = u * (HEAD_DIM ** -0.5)
                    for i in range(PAIR):
                        e = u[:, lane(i)]
                        if dst is not v_ref:
                            e = e * cos + swap_halves(e) * sin
                        dst[0, rows, c + WIDE * i:c + WIDE * i + WIDE] = e.astype(BF)

    pl.when(t == 0)(start)
    valid = lax.broadcasted_iota(jnp.int32, (1, SEQ), 1) < len_ref[seq]
    lanes = pl.ds(pl.multiple_of(j * WIDE, WIDE), WIDE)
    masks = [half_mask((SEQ, WIDE), 1, h) for h in range(PAIR)]
    ks = [jnp.where(m, k_ref[0, :, lanes], 0) for m in masks]
    vs = [jnp.where(m, v_ref[0, :, lanes], 0) for m in masks]
    chains = [(r, h) for r in blocks(SEQ) for h in range(PAIR)]

    def score(r, h):
        return dot(q_ref[0, pl.ds(r, BLOCK), lanes], ks[h], 1, 1)
    ahead, ctx = score(*chains[0]), 0
    for i, (r, h) in enumerate(chains):
        s = jnp.where(valid, ahead, NEG_BIG)
        if i + 1 < len(chains):
            ahead = score(*chains[i + 1])
        e = jnp.exp(s - jnp.max(s, axis=-1, keepdims=True))
        p = (e * (1.0 / jnp.sum(e, axis=-1, keepdims=True))).astype(BF)
        p_ref[0, h, pl.ds(r, BLOCK)] = p
        ctx = ctx + dot(p, vs[h]) if h else dot(p, vs[h])
        if h:
            ctx_ref[0, pl.ds(r, BLOCK), lanes] = ctx.astype(BF)

    @pl.when(j == QUAD - 1)
    def _():
        for r in blocks(SEQ):
            rows = pl.ds(r, BLOCK)
            x1_ref[0, rows] = (x_ref[0, rows].astype(F32) + dot(ctx_ref[0, rows], w_ref[BIAS_OUT]) + row(s_ref, BIAS_OUT)).astype(BF)

    proceed()


def mlp_fwd_kernel(x_ref, w1_ref, w2_ref, s_ref, h_ref, a_ref, g_ref, *y_ref):
    x = x_ref[0].astype(F32)
    xhat, _ = normed(x)
    h = (xhat * row(s_ref, GAIN2) + row(s_ref, SHIFT2)).astype(BF)
    h_ref[0] = h
    acc = x + row(s_ref, BIAS_DOWN)
    for j in range(CHUNKS):
        cols = slice(CHUNK * j, CHUNK * j + CHUNK)
        pre = dot(h, w1_ref[:, cols]) + row(s_ref, BIAS_UP + j)
        z = pre * math.sqrt(0.5)
        cdf = 0.5 + 0.5 * lax.erf(z)
        g_ref[0, :, cols] = cdf + pre * math.sqrt(0.5 / math.pi) * jnp.exp2(z * z * -math.log2(math.e))
        a = (pre * cdf).astype(BF)
        a_ref[0, :, cols] = a
        if y_ref:
            acc = acc + dot(a, w2_ref[cols, :])
    for ref in y_ref:
        ref[0] = acc.astype(BF)


def layer_small(layer):
    return pl.BlockSpec((None, SMALL, DIM), lambda *_: (layer, 0, 0))


def attn_fwd(layer, lengths, x, w, s, cos, sin, prev, late):
    seq = lambda t: (lax.div(t, QUAD), 0, 0)
    t = pl.BlockSpec((1, SEQ, DIM), seq)
    saved = [pl.BlockSpec((None, 1, SEQ, DIM), lambda t: (layer,) + seq(t))] * 6
    saved.append(pl.BlockSpec((None, 1, PAIR, SEQ, SEQ), lambda t: (layer, lax.div(t, QUAD), lax.rem(t, QUAD), 0, 0)))
    inputs = [lengths, x, w, s, cos, sin]
    n, m = len(inputs), len(prev)
    res = pl.pallas_call(
        lambda *refs: attn_fwd_kernel('attn%d' % layer, *refs[:n], *refs[n + m + len(late):]), name='attn_fwd', grid=(OCT,),
        in_specs=[pl.BlockSpec(memory_space=pltpu.SMEM), t, whole((MATRICES, DIM, DIM)), layer_small(layer), whole((SEQ, WIDE)), whole((SEQ, WIDE))] + any_space(m + len(late)),
        out_specs=saved + any_space(len(late)),
        out_shape=[SD((LAYERS, SEQS, SEQ, DIM), BF)] * 6 + [SD((LAYERS, SEQS, HEADS, SEQ, SEQ), BF)] + [SD(e.shape, BF) for e in late],
        input_output_aliases=dict([(n + i, i) for i in range(m)] + [(n + m + i, len(saved) + i) for i in range(len(late))]),
        scratch_shapes=semaphores(40),
        compiler_params=pltpu.CompilerParams(collective_id=PAIR + layer, has_side_effects=True, vmem_limit_bytes=VM),
    )(*inputs, *prev, *late)
    return res[:len(saved)], res[len(saved):]


def mlp_fwd(layer, x1, w1, w2, s, prev):
    place = lambda t: (layer, lax.div(t, PAIR), lax.rem(t, PAIR), 0)
    block = lambda n: pl.BlockSpec((None, 1, BLOCK, n), place)
    widths = [(DIM, BF), (FFN, BF), (FFN, F32)]
    outs = [block(w) for w, _ in widths] + [pl.BlockSpec((1, BLOCK, DIM), lambda t: place(t)[1:])] * (1 - layer)
    inputs = [x1, w1, w2, s]
    n, m = len(inputs), len(prev)
    return pl.pallas_call(
        lambda *refs: mlp_fwd_kernel(*refs[:n], *refs[n + m:]), name='mlp_fwd', grid=(QUAD,),
        in_specs=[block(DIM), whole((DIM, FFN)), whole((FFN, DIM)), layer_small(layer)] + any_space(m), out_specs=outs,
        out_shape=[SD((LAYERS, SEQS, SEQ, w), d) for w, d in widths] + [SD((SEQS, SEQ, DIM), BF)] * (1 - layer),
        input_output_aliases={n + i: i for i in range(m)},
        compiler_params=pltpu.CompilerParams(vmem_limit_bytes=VM),
    )(*inputs, *prev)


def backward_kernel(dy, a, g, q, k, v, p, s, cos_ref, sin_ref, h2, x1, h1, ctx, x0, y0, w1_0, w1_1, w2_0, w2_1, wa_0, wa_1,
                    d_x, *refs):
    (g_attn, g_up, g_down, gb_attn, g_ln, gb_up, gb_down), outs, refs = refs[RESULTS:RESULTS + RESULTS], refs[:RESULTS], refs[RESULTS + RESULTS:]
    made = (g_attn, g_up, g_down, gb_attn, g_ln, gb_up, gb_down)
    (dx, dmid, dproj, dpre, acc, value, total, w1, w2, wa, h2s, h1s, late, *refs) = refs
    credits, fetched, written, *sems = refs[-5:]
    t = pl.program_id(0)
    layer, r = 1 - lax.div(t, LAYER_STEPS), lax.rem(t, LAYER_STEPS)
    place = Place(*sems)
    me = place.me
    n = len(total_buffers(1))
    slots, last_slots, refs = refs[:n], refs[n:n + n], refs[n + n:-5]

    def finish_of(name, l):
        def finish(core, part):
            if name == 'down':
                for i in range(PAIR):
                    g_down[l, :, pl.ds(pl.multiple_of((PAIR * core + i) * WIDE, WIDE), WIDE)] = part[i]
            elif name == 'up':
                for i in range(OCT):
                    at = i // PAIR * QUAD + PAIR * core + i % PAIR
                    g_up[l, :, pl.ds(pl.multiple_of(at * WIDE, WIDE), WIDE)] = part[i]
            elif name == 'first':
                for i in range(QUAD):
                    g_attn[l, PAIR * core + i // PAIR, :, lane(i % PAIR)] = part[i // PAIR, i % PAIR]
            else:
                for i in range(PAIR):
                    g_attn[l, PAIR * core + (name == 'third'), :, lane(PAIR + i)] = part[i]
        return finish

    gens, grads = {(1, 'small'): total_unit(place, value.at[1], total.at[1], slots)}, {}
    for i, (name, kind, pieces) in enumerate(SETS):
        shared, refs = refs[:QUAD], refs[QUAD:]
        m = len(unit_buffers(kind)[1][0])
        later, refs = (refs[:m], refs[m:m + m]), refs[m + m:]
        grads[name] = shared[0]
        axis = UNITS[kind][0][0]
        groups = [[('c', 1)], [(axis, e) for e in place.peers(axis)]]

        def give(which, groups=groups, i=i):
            for e in groups[which]:
                place.signal(credits.at[PAIR * i + which], *e)

        def take(which, groups=groups, i=i):
            pl.semaphore_wait(credits.at[PAIR * i + which], len(groups[which]))
        nothing = lambda which: None
        for l in (1, 0):
            gens[l, name] = reduce_unit(place, kind, l, [*shared, *later[l]], finish_of(name, l), pieces, give if l else nothing, nothing if l else take)

    loads = dict(w2=(w2_0, w2_1, w2), w1=(w1_0, w1_1, w1), h2=(h2.at[0], h2.at[1], h2s), x1=(x1.at[0], x1.at[1], late), h1=(h1.at[0], h1.at[1], h1s),
                 wa=(wa_0, wa_1, wa), ctx=(ctx.at[0], ctx.at[1], late), xin=(x0, y0, late))
    starts = {(1, 'w2'): 'A', (1, 'w1'): 'A', (1, 'h2'): 'A', (1, 'x1'): 'A', (1, 'h1'): 'B', (1, 'wa'): 'B', (1, 'ctx'): 'E', (1, 'xin'): 'I',
              (0, 'w2'): 'E', (0, 'w1'): 'E', (0, 'h2'): 'E', (0, 'x1'): 'M', (0, 'h1'): 'M', (0, 'wa'): 'M', (0, 'ctx'): 'Q', (0, 'xin'): 'U'}

    def load(name, l):
        return pltpu.make_async_copy(loads[name][l], loads[name][-1], fetched.at[list(loads).index(name)])

    said = []

    @pl.when(t == 0)
    def _():
        said.append(place.hello('xl'))
        dx[...] = dy[...]
        value[...] = jnp.zeros_like(value)

    for step in range(STEPS):
        due = [key for key, letter in starts.items() if ord(letter) - ord('A') == step]
        if due:
            @pl.when(t == step)
            def _():
                for l, name in due:
                    load(name, l).start()

    def put(ref, where, part, shape):
        ref[where] = part.reshape(shape + TILE)

    def add_sums(rows, terms):
        for i, e in zip(rows, terms):
            value[layer, i // OCT, i % OCT:i % OCT + 1] += jnp.sum(e, axis=0, keepdims=True)

    @pl.when(r < MLP_STEPS)
    def _():
        gw = dot(a[...], dx[...], 0, 0)
        for i in range(QUAD):
            put(grads['down'], (i // PAIR, pl.ds(PAIR * r, PAIR), ALL, ALL, ALL, i % PAIR), gw[:, lane(i)], (PAIR, QUAD, QUAD, CORES))

        @pl.when(r == 0)
        def _():
            for name in ('w2', 'w1', 'h2'):
                load(name, 0).wait()
        chunk = pl.ds(pl.multiple_of(r * CHUNK, CHUNK), CHUNK)
        bias = jnp.zeros((1, DIM), F32)
        for e in blocks(TOKENS):
            rows = pl.ds(e, BLOCK)
            d = dot(dx[rows], w2[chunk], 1, 1) * g[rows]
            bias = bias + jnp.sum(d, axis=0, keepdims=True)
            dpre[rows] = d.astype(BF)
            part = dot(dpre[rows], w1[:, chunk], 1, 1)

            @pl.when(r == 0)
            def _():
                acc[rows] = part

            @pl.when(r > 0)
            def _():
                acc[rows] = acc[rows] + part
        value[layer, 1, pl.ds(r, 1)] = bias
        gw = dot(h2s[...], dpre[...], 0, 0)
        for i in range(QUAD):
            put(grads['up'], (i // PAIR, ALL, ALL, ALL, PAIR * r + i % PAIR), gw[:, lane(i)], (OCT, QUAD, PAIR))

    @pl.when(r == MLP_STEPS - 1)
    def _():
        load('x1', 0).wait()
        for e in blocks(TOKENS):
            rows = pl.ds(e, BLOCK)
            dh = acc[rows]
            xhat, rstd = normed(late[rows].astype(F32))
            d = dx[rows].astype(F32)
            dmid[rows] = (d + norm_back(dh, row(s, GAIN2), xhat, rstd)).astype(BF)
            add_sums((BIAS_DOWN, GAIN2, SHIFT2, BIAS_OUT), (d, dh * xhat, dh, dmid[rows].astype(F32)))

    @pl.when(r == MLP_STEPS)
    def _():
        load('wa', 0).wait()

    @pl.when(r >= MLP_STEPS)
    def _():
        e = r - MLP_STEPS
        rows = pl.ds(pl.multiple_of(lax.rem(e, SEQS) * SEQ, SEQ), SEQ)
        lanes = pl.ds(pl.multiple_of(lax.div(e, SEQS) * WIDE, WIDE), WIDE)
        qv, kv, vv = q[...], k[...], v[...]
        dc = dot(dmid[rows], wa[BIAS_OUT, lanes], 1, 1).astype(BF)
        qt, dct = qv.T, dc.T
        dq, dkt, dvt = 0, 0, 0
        for h in range(PAIR):
            m = half_mask((SEQ, WIDE), 1, h)
            mt = half_mask((WIDE, SEQ), 0, h)
            kh, vh = jnp.where(m, kv, 0), jnp.where(m, vv, 0)
            dvt = dvt + dot(jnp.where(mt, dct, 0), p[h])
            ds = []
            for b in blocks(SEQ):
                pf = p[h, pl.ds(b, BLOCK)].astype(F32)
                dp = dot(dc[b:b + BLOCK], vh, 1, 1)
                ds.append((pf * (dp - jnp.sum(dp * pf, axis=-1, keepdims=True))).astype(BF))
            ds = jnp.concatenate(ds, axis=0)
            dq = dq + dot(ds, kh)
            dkt = dkt + dot(jnp.where(mt, qt, 0), ds)
        cos, sin = cos_ref[...], sin_ref[...]
        dk = dkt.T
        dproj[0, rows, lanes] = ((dq * cos - swap_halves(dq) * sin) * (HEAD_DIM ** -0.5)).astype(BF)
        dproj[1, rows, lanes] = (dk * cos - swap_halves(dk) * sin).astype(BF)
        dproj[PAIR, rows, lanes] = dvt.T.astype(BF)

    for which in range(PAIR):
        @pl.when(r == MLP_STEPS + ATTN_STEPS // PAIR * (1 + which) - 1)
        def _():
            if which == 0:
                load('h1', 0).wait()
                load('ctx', 0).wait()
                gw_out = dot(late[...], dmid[...], 0, 0)
                for j in range(QUAD):
                    name, at = (('third', (1, ALL, ALL, ALL, j % PAIR)) if j >= PAIR else ('first', (1, 1, ALL, ALL, ALL, j)))
                    put(grads[name], at, gw_out[:, lane(j)], (OCT, QUAD, PAIR))
            cols = slice(BLOCK * which, BLOCK * which + BLOCK)
            for i in range(MATRICES - 1):
                gw = dot(h1s[...], dproj[i, :, cols], 0, 0)
                for j in range(PAIR):
                    name, at = (('second', 'third')[i % PAIR], (i // PAIR,)) if which else ('first', (i // PAIR, i % PAIR))
                    put(grads[name], at + (ALL, ALL, ALL, j), gw[:, lane(j)], (OCT, QUAD, PAIR))

    def advance(when, cond):
        due = [gens[key] for key, letters in SCHEDULE.items() if when in letters]
        if due:
            @pl.when(cond)
            def _():
                for gen in due:
                    next(gen, 0)

    @pl.when(t == 0)
    def _():
        place.greet(*said)

    for step in range(STEPS):
        advance(chr(ord('A') + step), t == step)

    def result(i):
        e = pl.ds(i * BLOCK, BLOCK)
        return pltpu.make_async_copy(dx.at[e], d_x.at[e], fetched.at[len(loads) + i])

    @pl.when(r == LAYER_STEPS - 1)
    def _():
        load('xin', 0).wait()
        for i, e in enumerate(blocks(TOKENS)):
            rows = pl.ds(e, BLOCK)
            parts = [dproj[j, rows] for j in range(MATRICES - 1)]
            dh = sum(dot(part, wa[j], 1, 1) for j, part in enumerate(parts))
            xhat, rstd = normed(late[rows].astype(F32))
            add_sums((0, 1, PAIR, GAIN1, SHIFT1), [part.astype(F32) for part in parts] + [dh * xhat, dh])
            dx[rows] = (dmid[rows].astype(F32) + norm_back(dh, row(s, GAIN1), xhat, rstd)).astype(BF)
            advance('abcd'[i], layer == 0)

    @pl.when(t == STEPS - 1)
    def _():
        for i in range(QUAD):
            result(i).start()
        left = {name[0]: gens[0, name] for name, _, _ in SETS}
        left['l'] = total_unit(place, value.at[0], total.at[0], last_slots, 'zyx')
        for letter in ENDING:
            next(left[letter], 0)
        run(left.values())
        index = ((me['z'] * SIZES['y'] + me['y']) * SIZES['x'] + me['x']) * CORES + me['c']
        shape = (OCT, DIM)
        lanes, rows = lax.broadcasted_iota(jnp.int32, shape, 1), lax.broadcasted_iota(jnp.int32, shape, 0)
        diagonal = lax.broadcasted_iota(jnp.int32, (OCT, OCT), 0) == lax.broadcasted_iota(jnp.int32, (OCT, OCT), 1)

        def across(e):
            return jnp.sum(jnp.where(diagonal, jnp.sum(e, axis=-1, keepdims=True), 0.0), axis=0, keepdims=True)
        for l in range(LAYERS):
            for i in range(PAIR):
                here = lanes == PAIR * index + i
                e = across(jnp.where(here, total[l, 0], 0.0))
                gb_attn[l, i:i + 1], g_ln[l, i:i + 1] = e[:, :QUAD], e[:, QUAD:]
                gb_down[l:l + 1, i:i + 1] = across(jnp.where(here, total[l, 1], 0.0))[:, QUAD:QUAD + 1]
            gb_up[l:l + 1] = across(sum(jnp.where(lanes + DIM * n == OCT * index + rows, total[l, 1, n:n + 1], 0.0) for n in range(QUAD)))
        copies = [pltpu.make_async_copy(src, dst, written.at[i]) for i, (src, dst) in enumerate(zip(made, outs))]
        for e in copies:
            e.start()
        for e in copies + [result(i) for i in range(QUAD)]:
            e.wait()


RESULTS = 7


def backward(dy, saved, x0, y0, wts, s, cos, sin):
    h1, q, k, v, ctx, x1, p, h2, a, g = saved
    once = dict(pipeline_mode=pl.Buffered(1))
    layer = lambda t: 1 - lax.div(t, LAYER_STEPS)
    chunk = lambda t: jnp.minimum(lax.rem(t, LAYER_STEPS), CHUNKS - 1)
    head_of = lambda t: jnp.maximum(lax.rem(t, LAYER_STEPS) - MLP_STEPS, 0)
    seq = lambda t: lax.rem(head_of(t), SEQS)
    pair = lambda t: lax.div(head_of(t), SEQS)
    flat = lambda e: e.reshape(*e.shape[:-3], TOKENS, e.shape[-1])
    cols = pl.BlockSpec((None, TOKENS, CHUNK), lambda t: (layer(t), 0, chunk(t)))
    head = pl.BlockSpec((None, None, SEQ, WIDE), lambda t: (layer(t), seq(t), 0, pair(t)))
    late = [flat(e) for e in (h2, x1, h1, ctx, x0, y0)] + [w for pair_of in wts for w in pair_of]
    act, small = pltpu.VMEM((TOKENS, DIM), BF), pltpu.VMEM((LAYERS, CORES, OCT, DIM), F32)
    bufs = [e for _, kind, _ in SETS for group in (unit_buffers(kind)[0], *unit_buffers(kind)[1]) for e in group]
    shapes = [(LAYERS, MATRICES, PAIR, DIM), (LAYERS, PAIR, FFN), (LAYERS, OCT, DIM), (LAYERS, PAIR, QUAD), (LAYERS, PAIR, QUAD), (LAYERS, OCT), (LAYERS, PAIR)]
    return pl.pallas_call(
        backward_kernel, name='backward', grid=(STEPS,),
        in_specs=[whole((TOKENS, DIM), **once), cols, cols, head, head, head,
                  pl.BlockSpec((None, None, PAIR, SEQ, SEQ), lambda t: (layer(t), seq(t), pair(t), 0, 0)),
                  pl.BlockSpec((None, SMALL, DIM), lambda t: (layer(t), 0, 0)), whole((SEQ, WIDE), **once), whole((SEQ, WIDE), **once)] + any_space(len(late)),
        out_specs=any_space(1 + len(shapes)),
        out_shape=[SD((TOKENS, DIM), BF)] + [SD(e, F32) for e in shapes],
        scratch_shapes=[pltpu.VMEM(e, F32) for e in shapes] + [act, act, pltpu.VMEM((MATRICES - 1, TOKENS, DIM), BF), act, pltpu.VMEM((TOKENS, DIM), F32), small, small,
                        pltpu.VMEM((DIM, FFN), BF), pltpu.VMEM((FFN, DIM), BF), pltpu.VMEM((MATRICES, DIM, DIM), BF), act, act, act]
        + total_buffers(OCT) * LAYERS + bufs + [pltpu.SemaphoreType.REGULAR((PAIR * len(SETS),)), pltpu.SemaphoreType.DMA((SMALL,)), pltpu.SemaphoreType.DMA((RESULTS,))] + semaphores(260),
        compiler_params=pltpu.CompilerParams(collective_id=SMALL, has_side_effects=True, vmem_limit_bytes=67043328),
    )(flat(dy), flat(a), flat(g), q, k, v, p, s, cos, sin, *late)


def deliver(*results):
    n = len(results)

    def body(*refs):
        for src, dst in zip(refs[:n], refs[n:]):
            dst[...] = src[...]
    return pl.pallas_call(body, name='deliver', in_specs=in_vmem(n), out_specs=in_vmem(n), out_shape=[SD(e.shape, e.dtype) for e in results])(*results)


def solution(mesh):
    grid = Mesh(mesh.devices.reshape([SIZES[a] for a in AXES]), AXES)
    first, second, third = P(AXES), P(None, AXES), P(None, None, AXES)
    weight_specs = (third, third, third, second, second, second, second)

    def device_step(x, lengths, d_y, w_attn, b_attn, ln_par, w_up, b_up, w_down, b_down):
        shards = tiled_shards(w_attn, w_up, w_down)
        full, small = gather(shards, b_attn.swapaxes(1, PAIR), ln_par.swapaxes(1, PAIR), b_up, b_down)
        cos, sin = (jnp.asarray(t) for t in rotary_tables())
        attn_saved, mlp_saved, y, wts = [], [], x, {}
        for layer in range(LAYERS):
            inner = y
            late = keys('attn%d' % layer)
            wts['attn', layer] = natural('attn', full['attn', layer])
            attn_saved, done = attn_fwd(layer, lengths, inner, wts['attn', layer], small, cos, sin, attn_saved, [full[e] for e in late])
            full.update(zip(late, done))
            for kind in ('up', 'down'):
                wts[kind, layer] = natural(kind, full[kind, layer])
            *mlp_saved, y = list(mlp_fwd(layer, attn_saved[5], wts['up', layer], wts['down', layer], small, mlp_saved)) + [x] * layer
        by_layer = [[wts[kind, layer] for layer in range(LAYERS)] for kind in ('up', 'down', 'attn')]
        d_x, *grads = backward(d_y, list(attn_saved) + mlp_saved, x, inner, by_layer, small, cos, sin)
        d_x, g_attn, g_up, g_down, gb_attn, g_ln, gb_up, gb_down = deliver(d_x, *grads)
        return d_x.reshape(x.shape), g_attn, gb_attn.swapaxes(1, PAIR), g_ln.swapaxes(1, PAIR), g_up, gb_up, g_down, gb_down

    return jax.shard_map(device_step, mesh=grid, in_specs=(first,) * 3 + weight_specs, out_specs=(first,) + weight_specs, check_vma=False)
```

```python
import math
import jax
import jax.numpy as jnp
import numpy as np
from jax import lax
from jax.experimental import pallas as pl
from jax.experimental.pallas import tpu as pltpu
from jax.sharding import Mesh, PartitionSpec as P

HEAD_DIM, EPS, THETA, NEG_BIG = 64, 1e-5, 10000.0, -1e30
SEQ, DIM, FFN, TOKENS, CHUNK, BLOCK, WIDE = 512, 512, 2048, 1024, 512, 256, 128
LAYERS = CORES = SEQS = PAIR = 2
MATRICES = CHUNKS = QUAD = 4
HEADS = OCT = 8
SMALL = 16
F32, BF = jnp.float32, jnp.bfloat16
SD = jax.ShapeDtypeStruct
AXES = ('z', 'y', 'x', 'c')
SIZES = dict(z=OCT, y=QUAD, x=QUAD, c=PAIR, k=PAIR, h=PAIR, l=PAIR, r=PAIR)
TILE = (OCT, WIDE)
ALL = slice(None)
BIAS_OUT, GAIN1, SHIFT1, GAIN2, SHIFT2, BIAS_UP, BIAS_DOWN = 3, 4, 5, 6, 7, 8, 12
TILED = dict(part='kzyht', slim='zyht', pair='zyht', up='zyht', down='zyxct')
FINE = dict(attn='kzyhtlcr', up='zyhtlcr', down='zyxct')
LANE_TILES = dict(attn=QUAD, part=PAIR, slim=PAIR, pair=PAIR, up=OCT, down=PAIR)
OWNER = dict(x='xhl', y='y', z='z')
UNITS = dict(up=('yzx', 'yzx'), down=('xyz', 'xyz'), part=('hyzl', 'hzyl'), slim=('yzx', 'yzx'), pair=('hyzl', 'hzyl'))
MLP_STEPS, ATTN_STEPS = CHUNKS, 8
LAYER_STEPS = MLP_STEPS + ATTN_STEPS
STEPS = LAYERS * LAYER_STEPS
SETS = (('up', 'up', ('t', PAIR, CHUNKS)), ('down', 'down', ('z', PAIR, CHUNKS)), ('first', 'part', ('z', OCT, 1)), ('second', 'slim', ('z', OCT, 1)), ('third', 'pair', ('z', OCT, 1)))
SCHEDULE = {(1, 'small'): 'MNOPTU', (1, 'second'): 'LMQUb', (1, 'third'): 'LMPUX', (1, 'first'): 'HJNSUX', (1, 'up'): 'ABCDEJNU', (1, 'down'): 'ABCDEJMOP',
            (0, 'up'): 'MNOPQV', (0, 'down'): 'MNOPQW', (0, 'first'): 'TVc', (0, 'second'): 'Xa', (0, 'third'): 'Xa'}
ENDING = 'lduls3tfldtsufltdsftlftl'
VM = 56 << 20


def spot(at):
    return dict(at, h=lax.div(at['x'], SIZES['l']), l=lax.rem(at['x'], SIZES['l']))


def only(at, names):
    return {n: at[n] for n in names if n in at}


def view(ref, names, pick):
    return ref.at[tuple(pick.get(n, ALL) for n in names)]


class Place:
    def __init__(self, send, recv):
        self.me = spot({a: lax.axis_index(a) for a in AXES})
        self.send, self.recv, self.used = send, recv, 0

    def shifted(self, axis, s):
        at = dict(self.me, **{axis: lax.rem(self.me[axis] + s, SIZES[axis])})
        if axis in 'hl':
            at['x'] = SIZES['l'] * at['h'] + at['l']
        return spot(at)

    def device(self, axis, s, core=0):
        at = self.shifted(axis, s)
        if core:
            at['c'] = other(at)
        return tuple(at[a] for a in AXES)

    def peers(self, axis):
        n = SIZES[axis]
        return sorted(range(1, n), key=lambda s: min(s, n - s))

    def signal(self, sem, *to):
        pl.semaphore_signal(sem, inc=1, device_id=self.device(*to), device_id_type=pl.DeviceIdType.MESH)

    def hello(self, partners=()):
        everyone = [(a, s, 0) for a in AXES for s in self.peers(a)] + [(a, s, 1) for a in partners for s in self.peers(a)]
        for e in everyone:
            self.signal(pltpu.get_barrier_semaphore(), *e)
        return len(everyone)

    def greet(self, said=None):
        n = self.hello() if said is None else said
        pl.semaphore_wait(pltpu.get_barrier_semaphore(), n)

    def begin(self, build):
        self.used += 1
        assert self.used <= self.send.shape[0]
        build().start()
        return lambda: build().wait()

    def copy(self, axis, s, refs, core=0):
        i = self.used

        def build():
            src, dst = refs()
            return pltpu.make_async_remote_copy(src, dst, self.send.at[i], self.recv.at[i], device_id=self.device(axis, s, core), device_id_type=pl.DeviceIdType.MESH)
        return self.begin(build)

    def local(self, refs):
        i = self.used
        return self.begin(lambda: pltpu.make_async_copy(*refs(), self.send.at[i]))


def half(kind, core, part):
    if kind == 'attn':
        return dict(k=pl.ds(core * CORES + part, 1))
    return dict(t=pl.ds(core * LANE_TILES[kind], LANE_TILES[kind]))


def gathered(kind, full, part):
    names = FINE[kind]
    return lambda core, fixed, at: view(full, names, dict(half(kind, core(at), part), **only(at, fixed)))


def own(at):
    return at['c']


def other(at):
    return 1 - at['c']


def gather_early(place, kind, part, order, full, shard):
    block = gathered(kind, full, part)
    names = FINE[kind]
    mine = [n for n in names if n not in 'tkr']
    rows = [n for n in names if n in 'tk'] + ['r', 'r']

    def piece(core):
        return view(shard, rows, half(kind, core(place.me), part))
    waits = [place.local(lambda: (piece(own), block(own, mine, place.me))),
             place.copy('c', 1, lambda: (piece(other), block(other, mine, place.me)))]
    for i in range(len(order) - 1):
        yield
        for w in waits:
            w()
        fixed = ''.join(OWNER[a] for a in order[i:])
        waits = [place.copy(order[i], s, lambda: (block(own, fixed, place.me),) * PAIR) for s in place.peers(order[i])]
    yield
    for w in waits:
        w()


def gather_late(place, kind, part, order, full):
    block = gathered(kind, full, part)
    axis = order[-1]
    fixed = OWNER[axis]
    same = lambda at: (block(own, fixed, at),) * PAIR
    waits = [(s, place.copy(axis, s, lambda: same(place.me))) for s in place.peers(axis)]
    last = [place.copy('c', 1, lambda: same(place.me))]
    for s, w in waits:
        yield
        w()
        last.append(place.copy('c', 1, lambda s=s: same(place.shifted(axis, SIZES[axis] - s))))
    yield
    for w in last:
        w()


def gather_whole(*args):
    yield from gather_early(*args)
    yield from gather_late(*args[:-1])


def unravel(i, shape):
    idx = []
    for n in reversed(shape):
        idx.append(lax.rem(i, n))
        i = lax.div(i, n)
    return tuple(reversed(idx))


def each(shape, body):
    def step(i, carry):
        body(unravel(i, shape))
        return carry
    lax.fori_loop(0, math.prod(shape), step, 0)


def total_unit(place, value, out, slots, axes='xyz'):
    me = place.me
    keep, slot, *slots = slots
    wait = place.copy('c', 1, lambda: (value.at[other(me)], slot.at[0]))
    yield
    wait()
    keep[...] = value[me['c']] + slot[0]
    for axis, slot in zip(axes, slots):
        last = SIZES[axis] - 1
        slot[last] = keep[...]
        waits = [place.copy(axis, s, lambda s=s: (slot.at[last], slot.at[s - 1])) for s in place.peers(axis)]
        yield
        for w in waits:
            w()
        v = slot[0]
        for s in range(1, SIZES[axis]):
            v = v + slot[s]
        keep[...] = v
    out[me['c']] = keep[...]
    wait = place.copy('c', 1, lambda: (keep, out.at[me['c']]))
    yield
    wait()


def total_buffers(n):
    return [pltpu.VMEM((n, DIM), F32)] + [pltpu.VMEM((OCT, n, DIM), F32)] * QUAD


def run(units):
    units = list(units)
    while units:
        units = [u for u in units if next(u, units) is not units]


def free_sizes(kind, names):
    return tuple(LANE_TILES[kind] if n == 't' else SIZES[n] for n in names) + TILE


def plan(kind, layer=0):
    left = TILED[kind]
    for axis in UNITS[kind][layer]:
        d = axis if axis in left else 'h' if axis == 'x' else ''
        left = left.replace(d, '')
        yield axis, d, left


def unit_buffers(kind):
    _, _, first = next(plan(kind))
    shapes = [(PAIR,) + free_sizes(kind, TILED[kind]), free_sizes(kind, TILED[kind]), free_sizes(kind, first)]
    later = []
    for layer in range(LAYERS):
        slots = [(SIZES[axis] - 1,) + free_sizes(kind, left) for axis, _, left in plan(kind, layer)]
        *_, (axis, _, left) = plan(kind, layer)
        if kind == 'down':
            slots.append(free_sizes(kind, left.replace('c', '')))
        else:
            slots[-1] = (PAIR * SIZES[axis],) + free_sizes(kind, left)
        later.append([pltpu.VMEM(s, F32) for s in slots[1:]])
    return [pltpu.VMEM(s, F32) for s in shapes + slots[:1]], later


def reduce_unit(place, kind, layer, bufs, finish, pieces, give, take):
    grad, got, first, slots, *rest = bufs
    me = place.me
    whole_grad, whole_names = grad, 'g' + TILED[kind]
    names, pick = whole_names, dict(g=me['c'])
    dim, size, count = pieces

    def cut(i):
        return {dim: pl.ds(size * i, size)}

    def accumulate(terms, fixed, into, piece=None):
        left = [n for n in names if n not in fixed]
        lead = left[:-3]
        sizes_of = dict(SIZES, t=LANE_TILES[kind])
        if piece is not None:
            sizes_of[dim] = size

        def body(idx):
            loop = dict(zip(lead, idx))
            if piece is not None:
                loop[dim] = loop[dim] + size * piece if dim in loop else pl.ds(size * piece, size)
            mine = tuple(fixed.get(n, loop.get(n, ALL)) for n in names)
            at = tuple(loop.get(n, ALL) for n in left)
            v = grad[mine]
            for ref in terms:
                v = v + ref[at]
            into[mine if into is grad else at] = v
        if lead:
            each([sizes_of[n] for n in lead], body)
        else:
            body(())

    (axis, d, left), *later = plan(kind, layer)
    arrived, waits = [], []

    def begin(i):
        if i == 0:
            take(1)
        arrived[i]()
        accumulate([got], pick, grad, i)
        for s in place.peers(axis):
            waits.append(place.copy(axis, s, lambda s=s: (view(whole_grad, whole_names, dict(only(place.shifted(axis, s), d), g=me['c'], **cut(i))),
                                                          view(slots, 's' + TILED[kind].replace(d, ''), dict(cut(i), s=s - 1)))))
    take(0)
    for i in range(count):
        arrived.append(place.copy('c', 1, lambda i=i: (view(whole_grad, whole_names, dict(cut(i), g=other(me))), view(got, TILED[kind], cut(i)))))
        if i:
            begin(i - 1)
        yield
    begin(count - 1)
    give(0)
    yield
    for w in waits:
        w()
    pick = dict(pick, **only(me, d))
    accumulate([slots.at[s] for s in range(SIZES[axis] - 1)], pick, first)
    give(1)
    grad, names, pick = first, left, {}
    for axis, d, left in later:
        slots, *rest = rest
        if not rest:
            far = [(s, core) for s in range(SIZES[axis]) for core in range(CORES) if s or core]
            waits = [place.copy(axis, s, lambda s=s, core=core: (view(first, names, dict(pick, **only(place.shifted(axis, s), d))), slots.at[PAIR * s + core]), core) for s, core in far]
            yield
            for w in waits:
                w()
            pick = dict(pick, **only(me, d))
            rows = pl.ds((me['l'] * PAIR + me['c']) * PAIR, PAIR)
            mine, away = first[tuple(pick.get(n, ALL) for n in names) + (rows,)], 0
            for s in range(SIZES[axis]):
                mine = mine + slots.at[PAIR * s][..., rows, :] if s else mine
                away = away + slots.at[PAIR * s + 1][..., rows, :]
            finish(own(me), mine)
            finish(other(me), away)
            return
        waits = [place.copy(axis, s, lambda s=s: (view(first, names, dict(pick, **only(place.shifted(axis, s), d))), slots.at[s - 1])) for s in place.peers(axis)]
        yield
        for w in waits:
            w()
        pick = dict(pick, **only(me, d))
        accumulate([slots.at[s] for s in range(SIZES[axis] - 1)], pick, first)
    away, = rest
    last = lambda core: dict(pick, c=core(me))
    wait = place.copy('c', 1, lambda: (view(first, names, last(other)), away))
    yield
    wait()
    finish(own(me), first[tuple(last(own).get(n, ALL) for n in names)])
    finish(other(me), away[...])


def blocks(n):
    return range(0, n, BLOCK)


def lane(i):
    return slice(WIDE * i, WIDE * i + WIDE)


def dot(a, b, ca=1, cb=0):
    return lax.dot_general(a, b, (((ca,), (cb,)), ((), ())), preferred_element_type=F32)


def rotary_tables():
    half_dim = HEAD_DIM // PAIR
    inv = (1.0 / (THETA ** (np.arange(half_dim, dtype=np.float32) * np.float32(2.0 / HEAD_DIM)))).astype(np.float32)
    ang = np.arange(SEQ, dtype=np.float32)[:, None] * inv[None, :]
    cos, sin = np.cos(ang), np.sin(ang)
    return np.tile(cos, (1, QUAD)), np.concatenate([-sin, sin] * PAIR, axis=1)


def swap_halves(t):
    n = HEAD_DIM // PAIR
    lanes = lax.broadcasted_iota(jnp.int32, t.shape, 1)
    return jnp.where(lax.rem(lanes, HEAD_DIM) < n, pltpu.roll(t, WIDE - n, 1), pltpu.roll(t, n, 1))


def normed(t):
    cent = t - jnp.mean(t, axis=-1, keepdims=True)
    rstd = lax.rsqrt(jnp.mean(cent * cent, axis=-1, keepdims=True) + EPS)
    return cent * rstd, rstd


def norm_back(dh, gain, xhat, rstd):
    dn = dh * gain
    return rstd * (dn - jnp.mean(dn, axis=-1, keepdims=True) - xhat * jnp.mean(dn * xhat, axis=-1, keepdims=True))


def row(ref, i):
    return ref[i:i + 1]


def half_mask(shape, axis, h):
    i = lax.broadcasted_iota(jnp.int32, shape, axis)
    return i >= HEAD_DIM if h else i < HEAD_DIM


def any_space(n):
    return [pl.BlockSpec(memory_space=pl.ANY)] * n


def in_vmem(n):
    return [pl.BlockSpec(memory_space=pltpu.VMEM)] * n


def semaphores(n):
    return [pltpu.SemaphoreType.DMA((n,))] * PAIR


def whole(shape, **kw):
    return pl.BlockSpec(shape, lambda *_: (0,) * len(shape), **kw)


def tiles_to_rows(t):
    *lead, r, n, s, w = t.shape
    return t.swapaxes(-3, -2).reshape(*lead, r * s, n * w)


def natural(kind, full):
    n = full.shape[FINE[kind].index('t')]
    lead = (MATRICES,) if kind == 'attn' else ()
    return tiles_to_rows(full.reshape(*lead, -1, n, *TILE))


def fine_shape(kind):
    n = LANE_TILES[kind] if kind == 'attn' else PAIR * LANE_TILES[kind]
    dims = dict(SIZES, t=n, k=MATRICES)
    return tuple(dims[d] for d in FINE[kind]) + ((WIDE,) if 'r' in FINE[kind] else TILE)


ATTN0, ATTN1 = ((('attn', l, 0, 'zxy'), ('attn', l, 1, 'zyx')) for l in range(LAYERS))
MLP0, MLP1 = ((('up', l, 0, 'zxy'), ('down', l, 0, 'zyx')) for l in range(LAYERS))
JOBS = dict(gather=[(gather_whole, g) for g in ATTN0] + [(gather_early, g) for g in MLP0 + ATTN1 + MLP1],
            attn0=[(gather_late, g) for g in MLP0 + ATTN1], attn1=[(gather_late, g) for g in MLP1])
HOST_STEPS = dict(attn0=((5, '0101'), (6, '01')), attn1=((5, '0101'), (6, '01')))
KINDS = tuple(FINE)


def keys(name):
    return sorted({g[:2] for _, g in JOBS[name]})


def units_of(name, place, full, shards):
    units = []
    for make, (kind, layer, part, order) in JOBS[name]:
        args = [place, kind, part, order, full[kind, layer]]
        units.append(make(*args) if make is gather_late else make(*args, shards[kind, layer]))
    return units


def host(name, place, t, full, shards):
    units, said = [], []

    @pl.when(t == 0)
    def _():
        said.append(place.hello())

    def start():
        place.greet(*said)
        units.extend(units_of(name, place, full, shards))
        for u in units:
            next(u)

    def proceed():
        for step, digits in HOST_STEPS[name]:
            @pl.when(t == step)
            def _():
                for i in digits:
                    next(units[int(i)], 0)

        @pl.when(t == OCT - 1)
        def _():
            run(units)
    return start, proceed


def gather_kernel(sa, su, sd, b_attn, ln, b_up, b_down, *refs):
    n = len(keys('gather'))
    full, total, value, slots, sems = refs[:n], refs[n], refs[n + 1], refs[n + 2:-2], refs[-2:]
    place = Place(*sems)
    place.greet()
    shards = {(kind, l): ref.at[l] for kind, ref in zip(KINDS, (sa, su, sd)) for l in range(LAYERS)}
    me = place.me
    index = ((me['z'] * SIZES['y'] + me['y']) * SIZES['x'] + me['x']) * CORES + me['c']

    def spread(v, rows):
        n = v.shape[1]
        at = lax.broadcasted_iota(jnp.int32, (rows, DIM), 1) - n * index
        if v.shape[0] < rows:
            at = at + DIM * lax.broadcasted_iota(jnp.int32, (rows, DIM), 0)
        return sum(jnp.where(at == i, v[:, i:i + 1], 0.0) for i in range(n))
    value[...] = jnp.zeros_like(value)
    shape = (PAIR, DIM)
    two = (lax.broadcasted_iota(jnp.int32, shape, 1) == PAIR * index + lax.broadcasted_iota(jnp.int32, shape, 0)).astype(F32).astype(BF)
    for l in range(LAYERS):
        value[l, :GAIN1] = dot(b_attn[l], two, 0, 0)
        value[l, GAIN1:BIAS_UP] = dot(ln[l], two, 0, 0)
        value[l, BIAS_UP:BIAS_DOWN] = spread(b_up[l:l + 1].astype(F32), QUAD)
        value[l, BIAS_DOWN:BIAS_DOWN + 1] = spread(b_down[l:l + 1].astype(F32), 1)
    units = units_of('gather', place, dict(zip(keys('gather'), full)), shards)
    units.insert(PAIR, total_unit(place, value, total, slots))
    run(units)


def tiled_shards(attn, up, down):
    return (attn.reshape(LAYERS, MATRICES, PAIR, -1, WIDE).swapaxes(-3, -2), up.reshape(LAYERS, PAIR, -1, WIDE).swapaxes(-3, -2),
            down.reshape(LAYERS, OCT, -1, WIDE).swapaxes(-3, -2))


def gather(shards, *small):
    names = keys('gather')
    *full, total = pl.pallas_call(
        gather_kernel, name='gather',
        in_specs=in_vmem(len(shards) + len(small)), out_specs=any_space(len(names)) + in_vmem(1),
        out_shape=[SD(fine_shape(k), BF) for k, _ in names] + [SD((LAYERS, SMALL, DIM), F32)],
        scratch_shapes=[pltpu.VMEM((LAYERS, SMALL, DIM), F32)] + total_buffers(SMALL) + semaphores(200),
        compiler_params=pltpu.CompilerParams(collective_id=1, has_side_effects=True),
    )(*shards, *small)
    return dict(zip(names, full)), total


def attn_fwd_kernel(name, len_ref, x_ref, w_ref, s_ref, cos_ref, sin_ref, *refs):
    h_ref, q_ref, k_ref, v_ref, ctx_ref, x1_ref, p_ref, *full = refs[:-2]
    seq, j = pl.program_id(0), pl.program_id(1)
    t = seq * QUAD + j
    start, proceed = host(name, Place(*refs[-2:]), t, dict(zip(keys(name), full)), {})

    @pl.when(j == 0)
    def _():
        for r in blocks(SEQ):
            rows = pl.ds(r, BLOCK)
            xhat, _ = normed(x_ref[0, rows].astype(F32))
            h_ref[0, rows] = (xhat * row(s_ref, GAIN1) + row(s_ref, SHIFT1)).astype(BF)
            h = h_ref[0, rows]
            cos, sin = cos_ref[rows], sin_ref[rows]
            for c in blocks(DIM):
                cols = slice(c, c + BLOCK)
                for kind, dst in enumerate((q_ref, k_ref, v_ref)):
                    u = dot(h, w_ref[kind, :, cols]) + s_ref[kind:kind + 1, cols]
                    if dst is q_ref:
                        u = u * (HEAD_DIM ** -0.5)
                    for i in range(PAIR):
                        e = u[:, lane(i)]
                        if dst is not v_ref:
                            e = e * cos + swap_halves(e) * sin
                        dst[0, rows, c + WIDE * i:c + WIDE * i + WIDE] = e.astype(BF)

    pl.when(t == 0)(start)
    valid = lax.broadcasted_iota(jnp.int32, (1, SEQ), 1) < len_ref[seq]
    lanes = pl.ds(pl.multiple_of(j * WIDE, WIDE), WIDE)
    masks = [half_mask((SEQ, WIDE), 1, h) for h in range(PAIR)]
    ks = [jnp.where(m, k_ref[0, :, lanes], 0) for m in masks]
    vs = [jnp.where(m, v_ref[0, :, lanes], 0) for m in masks]
    chains = [(r, h) for r in blocks(SEQ) for h in range(PAIR)]

    def score(r, h):
        return dot(q_ref[0, pl.ds(r, BLOCK), lanes], ks[h], 1, 1)
    ahead, ctx = [score(*c) for c in chains[:PAIR]], 0
    for i, (r, h) in enumerate(chains):
        s = jnp.where(valid, ahead.pop(0), NEG_BIG)
        if i + PAIR < len(chains):
            ahead.append(score(*chains[i + PAIR]))
        e = jnp.exp(s - jnp.max(s, axis=-1, keepdims=True))
        p = (e * (1.0 / jnp.sum(e, axis=-1, keepdims=True))).astype(BF)
        p_ref[0, h, pl.ds(r, BLOCK)] = p
        ctx = ctx + dot(p, vs[h]) if h else dot(p, vs[h])
        if h:
            ctx_ref[0, pl.ds(r, BLOCK), lanes] = ctx.astype(BF)

    @pl.when(j == QUAD - 1)
    def _():
        for r in blocks(SEQ):
            rows = pl.ds(r, BLOCK)
            x1_ref[0, rows] = (x_ref[0, rows].astype(F32) + dot(ctx_ref[0, rows], w_ref[BIAS_OUT]) + row(s_ref, BIAS_OUT)).astype(BF)

    proceed()


def mlp_fwd_kernel(x_ref, w1_ref, w2_ref, s_ref, h_ref, a_ref, g_ref, *y_ref):
    x = x_ref[0].astype(F32)
    xhat, _ = normed(x)
    h = (xhat * row(s_ref, GAIN2) + row(s_ref, SHIFT2)).astype(BF)
    h_ref[0] = h
    acc = x + row(s_ref, BIAS_DOWN)
    for j in range(CHUNKS):
        cols = slice(CHUNK * j, CHUNK * j + CHUNK)
        pre = dot(h, w1_ref[:, cols]) + row(s_ref, BIAS_UP + j)
        z = pre * math.sqrt(0.5)
        cdf = 0.5 + 0.5 * lax.erf(z)
        g_ref[0, :, cols] = cdf + pre * math.sqrt(0.5 / math.pi) * jnp.exp2(z * z * -math.log2(math.e))
        a = (pre * cdf).astype(BF)
        a_ref[0, :, cols] = a
        if y_ref:
            acc = acc + dot(a, w2_ref[cols, :])
    for ref in y_ref:
        ref[0] = acc.astype(BF)


def layer_small(layer):
    return pl.BlockSpec((None, SMALL, DIM), lambda *_: (layer, 0, 0))


def attn_fwd(layer, lengths, x, w, s, cos, sin, prev, late):
    t = pl.BlockSpec((1, SEQ, DIM), lambda i, j: (i, 0, 0))
    saved = [pl.BlockSpec((None, 1, SEQ, DIM), lambda i, j: (layer, i, 0, 0))] * 6
    saved.append(pl.BlockSpec((None, 1, PAIR, SEQ, SEQ), lambda i, j: (layer, i, j, 0, 0)))
    inputs = [lengths, x, w, s, cos, sin]
    n, m = len(inputs), len(prev)
    res = pl.pallas_call(
        lambda *refs: attn_fwd_kernel('attn%d' % layer, *refs[:n], *refs[n + m + len(late):]), name='attn_fwd', grid=(SEQS, QUAD),
        in_specs=[pl.BlockSpec(memory_space=pltpu.SMEM), t, whole((MATRICES, DIM, DIM)), layer_small(layer), whole((SEQ, WIDE)), whole((SEQ, WIDE))] + any_space(m + len(late)),
        out_specs=saved + any_space(len(late)),
        out_shape=[SD((LAYERS, SEQS, SEQ, DIM), BF)] * 6 + [SD((LAYERS, SEQS, HEADS, SEQ, SEQ), BF)] + [SD(e.shape, BF) for e in late],
        input_output_aliases=dict([(n + i, i) for i in range(m)] + [(n + m + i, len(saved) + i) for i in range(len(late))]),
        scratch_shapes=semaphores(40),
        compiler_params=pltpu.CompilerParams(collective_id=PAIR + layer, has_side_effects=True, vmem_limit_bytes=VM),
    )(*inputs, *prev, *late)
    return res[:len(saved)], res[len(saved):]


def mlp_fwd(layer, x1, w1, w2, s, prev):
    block = lambda n: pl.BlockSpec((None, 1, BLOCK, n), lambda i, j: (layer, i, j, 0))
    widths = [(DIM, BF), (FFN, BF), (FFN, F32)]
    outs = [block(w) for w, _ in widths] + [pl.BlockSpec((1, BLOCK, DIM), lambda i, j: (i, j, 0))] * (1 - layer)
    inputs = [x1, w1, w2, s]
    n, m = len(inputs), len(prev)
    return pl.pallas_call(
        lambda *refs: mlp_fwd_kernel(*refs[:n], *refs[n + m:]), name='mlp_fwd', grid=(SEQS, PAIR),
        in_specs=[block(DIM), whole((DIM, FFN)), whole((FFN, DIM)), layer_small(layer)] + any_space(m), out_specs=outs,
        out_shape=[SD((LAYERS, SEQS, SEQ, w), d) for w, d in widths] + [SD((SEQS, SEQ, DIM), BF)] * (1 - layer),
        input_output_aliases={n + i: i for i in range(m)},
        compiler_params=pltpu.CompilerParams(vmem_limit_bytes=VM),
    )(*inputs, *prev)


def backward_kernel(dy, a, g, q, k, v, p, s, cos_ref, sin_ref, h2, x1, h1, ctx, x0, y0, w1_0, w1_1, w2_0, w2_1, wa_0, wa_1,
                    d_x, *refs):
    (g_attn, g_up, g_down, gb_attn, g_ln, gb_up, gb_down), outs, refs = refs[RESULTS:RESULTS + RESULTS], refs[:RESULTS], refs[RESULTS + RESULTS:]
    made = (g_attn, g_up, g_down, gb_attn, g_ln, gb_up, gb_down)
    (dx, dmid, dproj, dpre, acc, value, total, w1, w2, wa, h2s, h1s, late, *refs) = refs
    credits, fetched, written, *sems = refs[-5:]
    layer, r = 1 - pl.program_id(0), pl.program_id(1)
    t = (1 - layer) * LAYER_STEPS + r
    place = Place(*sems)
    me = place.me
    n = len(total_buffers(1))
    slots, last_slots, refs = refs[:n], refs[n:n + n], refs[n + n:-5]

    def finish_of(name, l):
        def finish(core, part):
            if name == 'down':
                for i in range(PAIR):
                    g_down[l, :, pl.ds(pl.multiple_of((PAIR * core + i) * WIDE, WIDE), WIDE)] = part[i]
            elif name == 'up':
                for i in range(OCT):
                    at = i // PAIR * QUAD + PAIR * core + i % PAIR
                    g_up[l, :, pl.ds(pl.multiple_of(at * WIDE, WIDE), WIDE)] = part[i]
            elif name == 'first':
                for i in range(QUAD):
                    g_attn[l, PAIR * core + i // PAIR, :, lane(i % PAIR)] = part[i // PAIR, i % PAIR]
            else:
                for i in range(PAIR):
                    g_attn[l, PAIR * core + (name == 'third'), :, lane(PAIR + i)] = part[i]
        return finish

    gens, grads = {(1, 'small'): total_unit(place, value.at[1], total.at[1], slots)}, {}
    for i, (name, kind, pieces) in enumerate(SETS):
        shared, refs = refs[:QUAD], refs[QUAD:]
        m = len(unit_buffers(kind)[1][0])
        later, refs = (refs[:m], refs[m:m + m]), refs[m + m:]
        grads[name] = shared[0]
        axis = UNITS[kind][0][0]
        groups = [[('c', 1)], [(axis, e) for e in place.peers(axis)]]

        def give(which, groups=groups, i=i):
            for e in groups[which]:
                place.signal(credits.at[PAIR * i + which], *e)

        def take(which, groups=groups, i=i):
            pl.semaphore_wait(credits.at[PAIR * i + which], len(groups[which]))
        nothing = lambda which: None
        for l in (1, 0):
            gens[l, name] = reduce_unit(place, kind, l, [*shared, *later[l]], finish_of(name, l), pieces, give if l else nothing, nothing if l else take)

    loads = dict(w2=(w2_0, w2_1, w2), w1=(w1_0, w1_1, w1), h2=(h2.at[0], h2.at[1], h2s), x1=(x1.at[0], x1.at[1], late), h1=(h1.at[0], h1.at[1], h1s),
                 wa=(wa_0, wa_1, wa), ctx=(ctx.at[0], ctx.at[1], late), xin=(x0, y0, late))
    starts = {(1, 'w2'): 'A', (1, 'w1'): 'A', (1, 'h2'): 'A', (1, 'x1'): 'A', (1, 'h1'): 'B', (1, 'wa'): 'B', (1, 'ctx'): 'E', (1, 'xin'): 'I',
              (0, 'w2'): 'E', (0, 'w1'): 'E', (0, 'h2'): 'E', (0, 'x1'): 'M', (0, 'h1'): 'M', (0, 'wa'): 'M', (0, 'ctx'): 'Q', (0, 'xin'): 'U'}

    def load(name, l):
        return pltpu.make_async_copy(loads[name][l], loads[name][-1], fetched.at[list(loads).index(name)])

    said = []

    @pl.when(t == 0)
    def _():
        said.append(place.hello('xl'))
        dx[...] = dy[...]
        value[...] = jnp.zeros_like(value)

    for step in range(STEPS):
        due = [key for key, letter in starts.items() if ord(letter) - ord('A') == step]
        if due:
            @pl.when(t == step)
            def _():
                for l, name in due:
                    load(name, l).start()

    def put(ref, where, part, shape):
        ref[where] = part.reshape(shape + TILE)

    def add_sums(rows, terms):
        for i, e in zip(rows, terms):
            value[layer, i // OCT, i % OCT:i % OCT + 1] += jnp.sum(e, axis=0, keepdims=True)

    @pl.when(r < MLP_STEPS)
    def _():
        gw = dot(a[...], dx[...], 0, 0)
        for i in range(QUAD):
            put(grads['down'], (i // PAIR, pl.ds(PAIR * r, PAIR), ALL, ALL, ALL, i % PAIR), gw[:, lane(i)], (PAIR, QUAD, QUAD, CORES))

        @pl.when(r == 0)
        def _():
            for name in ('w2', 'w1', 'h2'):
                load(name, 0).wait()
        chunk = pl.ds(pl.multiple_of(r * CHUNK, CHUNK), CHUNK)
        bias = jnp.zeros((1, DIM), F32)
        for e in blocks(TOKENS):
            rows = pl.ds(e, BLOCK)
            d = dot(dx[rows], w2[chunk], 1, 1) * g[rows]
            bias = bias + jnp.sum(d, axis=0, keepdims=True)
            dpre[rows] = d.astype(BF)
            part = dot(dpre[rows], w1[:, chunk], 1, 1)

            @pl.when(r == 0)
            def _():
                acc[rows] = part

            @pl.when(r > 0)
            def _():
                acc[rows] = acc[rows] + part
        value[layer, 1, pl.ds(r, 1)] = bias
        gw = dot(h2s[...], dpre[...], 0, 0)
        for i in range(QUAD):
            put(grads['up'], (i // PAIR, ALL, ALL, ALL, PAIR * r + i % PAIR), gw[:, lane(i)], (OCT, QUAD, PAIR))

    @pl.when(r == MLP_STEPS - 1)
    def _():
        load('x1', 0).wait()
        for e in blocks(TOKENS):
            rows = pl.ds(e, BLOCK)
            dh = acc[rows]
            xhat, rstd = normed(late[rows].astype(F32))
            d = dx[rows].astype(F32)
            dmid[rows] = (d + norm_back(dh, row(s, GAIN2), xhat, rstd)).astype(BF)
            add_sums((BIAS_DOWN, GAIN2, SHIFT2, BIAS_OUT), (d, dh * xhat, dh, dmid[rows].astype(F32)))

    @pl.when(r == MLP_STEPS)
    def _():
        load('wa', 0).wait()

    @pl.when(r >= MLP_STEPS)
    def _():
        e = r - MLP_STEPS
        rows = pl.ds(pl.multiple_of(lax.rem(e, SEQS) * SEQ, SEQ), SEQ)
        lanes = pl.ds(pl.multiple_of(lax.div(e, SEQS) * WIDE, WIDE), WIDE)
        qv, kv, vv = q[...], k[...], v[...]
        dc = dot(dmid[rows], wa[BIAS_OUT, lanes], 1, 1).astype(BF)
        qt, dct = qv.T, dc.T
        dq, dkt, dvt = 0, 0, 0
        masks = [half_mask((SEQ, WIDE), 1, h) for h in range(PAIR)]
        ks, vs = ([jnp.where(m, e, 0) for m in masks] for e in (kv, vv))
        chains = [(h, b) for h in range(PAIR) for b in blocks(SEQ)]

        def slope(h, b):
            return dot(dc[b:b + BLOCK], vs[h], 1, 1)
        ahead, ds = [slope(*c) for c in chains[:PAIR]], []
        for i, (h, b) in enumerate(chains):
            dp = ahead.pop(0)
            if i + PAIR < len(chains):
                ahead.append(slope(*chains[i + PAIR]))
            pf = p[h, pl.ds(b, BLOCK)].astype(F32)
            ds.append((pf * (dp - jnp.sum(dp * pf, axis=-1, keepdims=True))).astype(BF))
            if len(ds) == SEQ // BLOCK:
                mt = half_mask((WIDE, SEQ), 0, h)
                dvt = dvt + dot(jnp.where(mt, dct, 0), p[h])
                whole_ds = jnp.concatenate(ds, axis=0)
                dq = dq + dot(whole_ds, ks[h])
                dkt = dkt + dot(jnp.where(mt, qt, 0), whole_ds)
                ds = []
        cos, sin = cos_ref[...], sin_ref[...]
        dk = dkt.T
        dproj[0, rows, lanes] = ((dq * cos - swap_halves(dq) * sin) * (HEAD_DIM ** -0.5)).astype(BF)
        dproj[1, rows, lanes] = (dk * cos - swap_halves(dk) * sin).astype(BF)
        dproj[PAIR, rows, lanes] = dvt.T.astype(BF)

    for which in range(PAIR):
        @pl.when(r == MLP_STEPS + ATTN_STEPS // PAIR * (1 + which) - 1)
        def _():
            if which == 0:
                load('h1', 0).wait()
                load('ctx', 0).wait()
                gw_out = dot(late[...], dmid[...], 0, 0)
                for j in range(QUAD):
                    name, at = (('third', (1, ALL, ALL, ALL, j % PAIR)) if j >= PAIR else ('first', (1, 1, ALL, ALL, ALL, j)))
                    put(grads[name], at, gw_out[:, lane(j)], (OCT, QUAD, PAIR))
            cols = slice(BLOCK * which, BLOCK * which + BLOCK)
            for i in range(MATRICES - 1):
                gw = dot(h1s[...], dproj[i, :, cols], 0, 0)
                for j in range(PAIR):
                    name, at = (('second', 'third')[i % PAIR], (i // PAIR,)) if which else ('first', (i // PAIR, i % PAIR))
                    put(grads[name], at + (ALL, ALL, ALL, j), gw[:, lane(j)], (OCT, QUAD, PAIR))

    def advance(when, cond):
        due = [gens[key] for key, letters in SCHEDULE.items() if when in letters]
        if due:
            @pl.when(cond)
            def _():
                for gen in due:
                    next(gen, 0)

    @pl.when(t == 0)
    def _():
        place.greet(*said)

    for step in range(STEPS):
        advance(chr(ord('A') + step), t == step)

    def result(i):
        e = pl.ds(i * BLOCK, BLOCK)
        return pltpu.make_async_copy(dx.at[e], d_x.at[e], fetched.at[len(loads) + i])

    @pl.when(r == LAYER_STEPS - 1)
    def _():
        load('xin', 0).wait()
        for i, e in enumerate(blocks(TOKENS)):
            rows = pl.ds(e, BLOCK)
            parts = [dproj[j, rows] for j in range(MATRICES - 1)]
            dh = sum(dot(part, wa[j], 1, 1) for j, part in enumerate(parts))
            xhat, rstd = normed(late[rows].astype(F32))
            add_sums((0, 1, PAIR, GAIN1, SHIFT1), [part.astype(F32) for part in parts] + [dh * xhat, dh])
            dx[rows] = (dmid[rows].astype(F32) + norm_back(dh, row(s, GAIN1), xhat, rstd)).astype(BF)
            advance('abcd'[i], layer == 0)

    @pl.when(t == STEPS - 1)
    def _():
        for i in range(QUAD):
            result(i).start()
        left = {name[0]: gens[0, name] for name, _, _ in SETS}
        left['3'] = gens[1, 'third']
        left['l'] = total_unit(place, value.at[0], total.at[0], last_slots, 'zyx')
        for letter in ENDING:
            next(left[letter], 0)
        run(left.values())
        index = ((me['z'] * SIZES['y'] + me['y']) * SIZES['x'] + me['x']) * CORES + me['c']
        shape = (OCT, DIM)
        lanes, rows = lax.broadcasted_iota(jnp.int32, shape, 1), lax.broadcasted_iota(jnp.int32, shape, 0)
        diagonal = lax.broadcasted_iota(jnp.int32, (OCT, OCT), 0) == lax.broadcasted_iota(jnp.int32, (OCT, OCT), 1)

        def across(e):
            return jnp.sum(jnp.where(diagonal, jnp.sum(e, axis=-1, keepdims=True), 0.0), axis=0, keepdims=True)
        for l in range(LAYERS):
            for i in range(PAIR):
                here = lanes == PAIR * index + i
                e = across(jnp.where(here, total[l, 0], 0.0))
                gb_attn[l, i:i + 1], g_ln[l, i:i + 1] = e[:, :QUAD], e[:, QUAD:]
                gb_down[l:l + 1, i:i + 1] = across(jnp.where(here, total[l, 1], 0.0))[:, QUAD:QUAD + 1]
            gb_up[l:l + 1] = across(sum(jnp.where(lanes + DIM * n == OCT * index + rows, total[l, 1, n:n + 1], 0.0) for n in range(QUAD)))
        copies = [pltpu.make_async_copy(src, dst, written.at[i]) for i, (src, dst) in enumerate(zip(made, outs))]
        for e in copies:
            e.start()
        for e in copies + [result(i) for i in range(QUAD)]:
            e.wait()


RESULTS = 7


def backward(dy, saved, x0, y0, wts, s, cos, sin):
    h1, q, k, v, ctx, x1, p, h2, a, g = saved
    once = dict(pipeline_mode=pl.Buffered(1))
    chunk = lambda r: jnp.minimum(r, CHUNKS - 1)
    seq = lambda r: lax.rem(jnp.maximum(r - MLP_STEPS, 0), SEQS)
    pair = lambda r: lax.div(jnp.maximum(r - MLP_STEPS, 0), SEQS)
    flat = lambda e: e.reshape(*e.shape[:-3], TOKENS, e.shape[-1])
    cols = pl.BlockSpec((None, TOKENS, CHUNK), lambda i, r: (1 - i, 0, chunk(r)))
    head = pl.BlockSpec((None, None, SEQ, WIDE), lambda i, r: (1 - i, seq(r), 0, pair(r)))
    late = [flat(e) for e in (h2, x1, h1, ctx, x0, y0)] + [w for pair_of in wts for w in pair_of]
    act, small = pltpu.VMEM((TOKENS, DIM), BF), pltpu.VMEM((LAYERS, CORES, OCT, DIM), F32)
    bufs = [e for _, kind, _ in SETS for group in (unit_buffers(kind)[0], *unit_buffers(kind)[1]) for e in group]
    shapes = [(LAYERS, MATRICES, PAIR, DIM), (LAYERS, PAIR, FFN), (LAYERS, OCT, DIM), (LAYERS, PAIR, QUAD), (LAYERS, PAIR, QUAD), (LAYERS, OCT), (LAYERS, PAIR)]
    return pl.pallas_call(
        backward_kernel, name='backward', grid=(LAYERS, LAYER_STEPS),
        in_specs=[whole((TOKENS, DIM), **once), cols, cols, head, head, head,
                  pl.BlockSpec((None, None, PAIR, SEQ, SEQ), lambda i, r: (1 - i, seq(r), pair(r), 0, 0)),
                  pl.BlockSpec((None, SMALL, DIM), lambda i, r: (1 - i, 0, 0)), whole((SEQ, WIDE), **once), whole((SEQ, WIDE), **once)] + any_space(len(late)),
        out_specs=any_space(1 + len(shapes)),
        out_shape=[SD((TOKENS, DIM), BF)] + [SD(e, F32) for e in shapes],
        scratch_shapes=[pltpu.VMEM(e, F32) for e in shapes] + [act, act, pltpu.VMEM((MATRICES - 1, TOKENS, DIM), BF), act, pltpu.VMEM((TOKENS, DIM), F32), small, small,
                        pltpu.VMEM((DIM, FFN), BF), pltpu.VMEM((FFN, DIM), BF), pltpu.VMEM((MATRICES, DIM, DIM), BF), act, act, act]
        + total_buffers(OCT) * LAYERS + bufs + [pltpu.SemaphoreType.REGULAR((PAIR * len(SETS),)), pltpu.SemaphoreType.DMA((SMALL,)), pltpu.SemaphoreType.DMA((RESULTS,))] + semaphores(260),
        compiler_params=pltpu.CompilerParams(collective_id=SMALL, has_side_effects=True, vmem_limit_bytes=67043328),
    )(flat(dy), flat(a), flat(g), q, k, v, p, s, cos, sin, *late)


def deliver(*results):
    n = len(results)

    def body(*refs):
        for src, dst in zip(refs[:n], refs[n:]):
            dst[...] = src[...]
    return pl.pallas_call(body, name='deliver', in_specs=in_vmem(n), out_specs=in_vmem(n), out_shape=[SD(e.shape, e.dtype) for e in results])(*results)


def solution(mesh):
    grid = Mesh(mesh.devices.reshape([SIZES[a] for a in AXES]), AXES)
    first, second, third = P(AXES), P(None, AXES), P(None, None, AXES)
    weight_specs = (third, third, third, second, second, second, second)

    def device_step(x, lengths, d_y, w_attn, b_attn, ln_par, w_up, b_up, w_down, b_down):
        shards = tiled_shards(w_attn, w_up, w_down)
        full, small = gather(shards, b_attn.swapaxes(1, PAIR), ln_par.swapaxes(1, PAIR), b_up, b_down)
        cos, sin = (jnp.asarray(t) for t in rotary_tables())
        attn_saved, mlp_saved, y, wts = [], [], x, {}
        for layer in range(LAYERS):
            inner = y
            late = keys('attn%d' % layer)
            wts['attn', layer] = natural('attn', full['attn', layer])
            attn_saved, done = attn_fwd(layer, lengths, inner, wts['attn', layer], small, cos, sin, attn_saved, [full[e] for e in late])
            full.update(zip(late, done))
            for kind in ('up', 'down'):
                wts[kind, layer] = natural(kind, full[kind, layer])
            *mlp_saved, y = list(mlp_fwd(layer, attn_saved[5], wts['up', layer], wts['down', layer], small, mlp_saved)) + [x] * layer
        by_layer = [[wts[kind, layer] for layer in range(LAYERS)] for kind in ('up', 'down', 'attn')]
        d_x, *grads = backward(d_y, list(attn_saved) + mlp_saved, x, inner, by_layer, small, cos, sin)
        d_x, g_attn, g_up, g_down, gb_attn, g_ln, gb_up, gb_down = deliver(d_x, *grads)
        return d_x.reshape(x.shape), g_attn, gb_attn.swapaxes(1, PAIR), g_ln.swapaxes(1, PAIR), g_up, gb_up, g_down, gb_down

    return jax.shard_map(device_step, mesh=grid, in_specs=(first,) * 3 + weight_specs, out_specs=(first,) + weight_specs, check_vma=False)
```
